8 devices in a mesh: dp: 8 (over z, y, x, core).
Axes of the slice: x: 2, y: 2, z: 1, core: 2. Of those that a mesh axis runs over, the one named last changes fastest.
Arguments:
- weights: float32 [12596224], P('dp')
- moment_one: float32 [12596224], P('dp')
- moment_two: float32 [12596224], P('dp')
- x_qkv: bfloat16 [32768, 1024], P('dp')
- dy_qkv: bfloat16 [32768, 3072], P('dp')
- x_proj: bfloat16 [32768, 1024], P('dp')
- dy_proj: bfloat16 [32768, 1024], P('dp')
- x_inter: bfloat16 [32768, 1024], P('dp')
- dy_inter: bfloat16 [32768, 4096], P('dp')
- x_out: bfloat16 [32768, 4096], P('dp')
- dy_out: bfloat16 [32768, 1024], P('dp')
- ln_grad: float32 [8, 4, 1024], P('dp')
Outputs:
- output 1: float32 [12596224], P('dp')
- output 2: float32 [12596224], P('dp')
- output 3: float32 [12596224], P('dp')
- output 4: bfloat16 [12596224], replicated
All inputs are finite; a program needn't handle non-finite values.
Results may differ from the reference program's by a relative error of at most 0.00574614.
Values sent between devices are 32-bit elements.
A program may use at most 1 GiB of HBM per device.

```python
import jax
import jax.numpy as jnp

D = 1024
REPLICAS = 8
TOKENS = 4096
NPAD = 12596224
STEP = 10

LEARN_RATE = 0.5
BETA_ONE = 0.9
BETA_TWO = 0.999
EPSILON = 1e-6
DECAY = 0.01
CORR_ONE = 1.0 - BETA_ONE ** STEP
CORR_TWO = 1.0 - BETA_TWO ** STEP
TENSOR_SIZES = [3 * D * D, 3 * D, D * D, D, D, D, 4 * D * D, 4 * D, 4 * D * D, D, D, D]
NPARAM = sum(TENSOR_SIZES)
NUM_SEGS = len(TENSOR_SIZES) + 1
TENSOR_STARTS = [sum(TENSOR_SIZES[:tensor_index]) for tensor_index in range(len(TENSOR_SIZES))]
DECAY_FLAGS = [1.0, 0.0, 1.0, 0.0, 0.0, 0.0, 1.0, 0.0, 1.0, 0.0, 0.0, 0.0, 0.0]
WEIGHT_SCALES = [1.0, 0.1, 0.4, 0.2, 3.0, 0.3, 0.7, 0.15, 0.35, 0.25, 2.0, 0.5]
LN_BOOST = 30.0
GRAD_VAR = [1.0, 1.0, 1.0, 1.0, LN_BOOST ** 2, LN_BOOST ** 2, 1.0, 1.0, 1.0, 1.0, LN_BOOST ** 2, LN_BOOST ** 2]
GRAD_VAR_TOTAL = sum(tensor_size * var_factor for tensor_size, var_factor in zip(TENSOR_SIZES, GRAD_VAR))


def segment_ids():
    pieces = [jnp.full((tensor_size,), tensor_index, jnp.int32) for tensor_index, tensor_size in enumerate(TENSOR_SIZES)]
    pieces.append(jnp.full((NPAD - NPARAM,), NUM_SEGS - 1, jnp.int32))
    return jnp.concatenate(pieces)


def setup_inputs(seed: int = 0) -> dict:
    key_list = jax.random.split(jax.random.key(seed), 12)
    seg_ids = segment_ids()
    row_count = REPLICAS * TOKENS
    starts = jnp.asarray(TENSOR_STARTS + [NPARAM], jnp.float32)[seg_ids]
    lengths = jnp.asarray(TENSOR_SIZES + [1], jnp.float32)[seg_ids]
    position_frac = jnp.clip((jnp.arange(NPAD, dtype=jnp.float32) - starts) / lengths, 0.0, 1.0)
    weight_ramp = 0.25 + 3.0 * position_frac * position_frac
    weight_scale = jnp.asarray(WEIGHT_SCALES + [0.0], jnp.float32)[seg_ids] * weight_ramp * D ** -0.5
    grad_var = jnp.asarray(GRAD_VAR + [0.0], jnp.float32)[seg_ids] / GRAD_VAR_TOTAL
    weights = weight_scale * jax.random.normal(key_list[0], (NPAD,), jnp.float32)
    moment_one = 0.2 * jnp.sqrt(grad_var) * jax.random.normal(key_list[1], (NPAD,), jnp.float32)
    moment_two = 0.001 * grad_var * (0.5 + jax.random.uniform(key_list[2], (NPAD,), jnp.float32))
    act_widths = [D, 3 * D, D, D, D, 4 * D, 4 * D, D]
    act_list = [jax.random.normal(key_list[3 + act_index], (row_count, act_width), jnp.float32).astype(jnp.bfloat16) for act_index, act_width in enumerate(act_widths)]
    ln_grad = LN_BOOST * TOKENS ** 0.5 * jax.random.normal(key_list[11], (REPLICAS, 4, D), jnp.float32)
    return {'weights': weights, 'moment_one': moment_one, 'moment_two': moment_two,
            'x_qkv': act_list[0], 'dy_qkv': act_list[1], 'x_proj': act_list[2], 'dy_proj': act_list[3],
            'x_inter': act_list[4], 'dy_inter': act_list[5], 'x_out': act_list[6], 'dy_out': act_list[7],
            'ln_grad': ln_grad}


def weight_grad(x_rows, dy_rows):
    return jnp.dot(x_rows.T, dy_rows, preferred_element_type=jnp.float32)


def bias_grad(dy_rows):
    return jnp.sum(dy_rows.astype(jnp.float32), axis=0)


def reference(weights, moment_one, moment_two, x_qkv, dy_qkv, x_proj, dy_proj, x_inter, dy_inter, x_out, dy_out, ln_grad):
    ln_sum = jnp.sum(ln_grad, axis=0)
    pieces = [weight_grad(x_qkv, dy_qkv), bias_grad(dy_qkv), weight_grad(x_proj, dy_proj), bias_grad(dy_proj),
              ln_sum[0], ln_sum[1], weight_grad(x_inter, dy_inter), bias_grad(dy_inter),
              weight_grad(x_out, dy_out), bias_grad(dy_out), ln_sum[2], ln_sum[3]]
    flat_grad = jnp.concatenate([grad_piece.reshape(-1) for grad_piece in pieces] + [jnp.zeros((NPAD - NPARAM,), jnp.float32)])
    mean_grad = flat_grad / REPLICAS
    grad_norm = jnp.sqrt(jnp.sum(mean_grad * mean_grad))
    grad_hat = mean_grad / jnp.maximum(1.0, grad_norm)
    new_m = BETA_ONE * moment_one + (1.0 - BETA_ONE) * grad_hat
    new_v = BETA_TWO * moment_two + (1.0 - BETA_TWO) * grad_hat * grad_hat
    seg_ids = segment_ids()
    decay_mask = jnp.asarray(DECAY_FLAGS, jnp.float32)[seg_ids]
    update = (new_m / CORR_ONE) / (jnp.sqrt(new_v / CORR_TWO) + EPSILON) + DECAY * decay_mask * weights
    w_norm = jnp.sqrt(jax.ops.segment_sum(weights * weights, seg_ids, num_segments=NUM_SEGS))
    u_norm = jnp.sqrt(jax.ops.segment_sum(update * update, seg_ids, num_segments=NUM_SEGS))
    both_pos = (w_norm > 0) & (u_norm > 0)
    trust_vec = jnp.where(both_pos, w_norm / jnp.where(u_norm > 0, u_norm, 1.0), 1.0)
    new_w = weights - LEARN_RATE * trust_vec[seg_ids] * update
    return new_w, new_m, new_v, new_w.astype(jnp.bfloat16)
```

```python
import jax
import jax.numpy as jnp
from jax import lax
from jax.experimental import pallas as pl
from jax.experimental.pallas import tpu as pltpu
from jax.sharding import PartitionSpec as P

STEP = 10
LEARN_RATE = 0.5
BETA_ONE = 0.9
BETA_TWO = 0.999
EPSILON = 1e-6
DECAY = 0.01
CORR_ONE = 1.0 - BETA_ONE ** STEP
CORR_TWO = 1.0 - BETA_TWO ** STEP

D = 1024
N_DEV = 8
TOKENS = 4096
LANES = 128
SHARD_ROWS = 12301
TOTAL_ROWS = N_DEV * SHARD_ROWS
KC = 1024
CHUNKS = TOKENS // KC
BLOCK = 512
TASKS = 24
STEPS = TASKS * CHUNKS
UR = 128
UNITS = 12
HALF = UNITS // 2
F32 = jnp.float32
BF16 = jnp.bfloat16
MIB = 1024 * 1024

SIZES = [24576, 24, 8192, 8, 8, 8, 32768, 32, 32768, 8, 8, 8]
STARTS = [sum(SIZES[:pos]) for pos in range(len(SIZES) + 1)]
SHARE = UNITS * D
NOMINAL = [0, 12288, 24600, 36912, 49200, 61488, 73808, 86096]
FIRST_TENSOR = [max(t for t, at in enumerate(STARTS[:-1]) if at <= SHARD_ROWS * dev) for dev in range(N_DEV)]
PAST_TENSOR = [1 + max(t for t, at in enumerate(STARTS[:-1]) if at < SHARD_ROWS * (dev + 1)) for dev in range(N_DEV)]
EDGE = 48
WIN = 12416
UP, DOWN = 24, 16
FEW = [0, 1, 5, 6, 7, 11]
MANY = [0, 3, 3, 6, 9, 9]
WIDE = [0, 0, 1, 2, 0, 3]
B1, Y1, X1 = range(1, 4)


def pick(index, values):
    out = jnp.int32(values[-1])
    for pos in reversed(range(len(values) - 1)):
        out = jnp.where(index == pos, jnp.int32(values[pos]), out)
    return out


def tile(index, size):
    return pl.ds(pl.multiple_of(index * size, size), size)


def each(lo, hi, body):
    def step(pos, carry):
        body(pos)
        return carry
    lax.fori_loop(lo, hi, step, lo)


def other(bit):
    return 1 - bit


def device(y, x, core):
    return 4 * y + 2 * x + core


def neighbours():
    me = lax.axis_index('dp')
    chip, core = me // 2, me % 2
    x, y = chip % 2, chip // 2
    return me, chip, core, device(y, x, other(core)), device(y, other(x), core), device(other(y), x, core)


def local(src, dst, sem):
    return pltpu.make_async_copy(src, dst, sem)


def remote(src, dst, send_sem, recv_sem, dev):
    return pltpu.make_async_remote_copy(src_ref=src, dst_ref=dst, send_sem=send_sem, recv_sem=recv_sem,
                                        device_id=(dev,), device_id_type=pl.DeviceIdType.MESH)


def act_on(copy, act):
    if act == 'start':
        copy.start()
    elif act == 'sent':
        copy.wait_send()
    else:
        copy.wait()


def enter(devices):
    barrier = pltpu.get_barrier_semaphore()
    for dev in devices:
        pl.semaphore_signal(barrier, inc=1, device_id=(dev,), device_id_type=pl.DeviceIdType.MESH)
    pl.semaphore_wait(barrier, len(devices))


def task_of(n):
    six = HALF
    mid = n - six
    first, last = n < six, n >= 3 * six
    t = jnp.where(first, 0, jnp.where(last, X1, B1 + mid % 2))
    i = jnp.where(first, n, jnp.where(last, n - 3 * six, mid // 2))
    return t, i


def chip_of(t, chip):
    x, y = chip % 2, chip // 2
    return 2 * ((y + other(t % 2)) % 2) + (x + other(t // 2)) % 2


def is_square(i):
    return i % 3 == 1


def is_edge(q):
    return q % 3 == 0


def operands_of(q, i):
    square, odd, pair = is_square(i), i % 2, i // 2
    kind = jnp.where(is_edge(q), q, jnp.where(square, 2 * q - 1, 2))
    rb = jnp.where(q == 0, odd, jnp.where(is_edge(q), 2 + 3 * odd + pair, jnp.where(square, i // 4, q - 1)))
    cb = jnp.where(q == 0, pair, jnp.where(is_edge(q) | square, 0, pick(i, WIDE)))
    return kind, rb, cb


def units_of(q, i, par):
    square = is_square(i)
    few = q - 1 == par
    cnt = jnp.where(few, jnp.where(square, 4, 1), jnp.where(square, 0, 3))
    s0 = jnp.where(square | (par == 0), 0, 2 * q - 1)
    u0 = jnp.where(few, pick(i, FEW), pick(i, MANY))
    edge = is_edge(q)
    return (jnp.where(edge, 0, s0), jnp.where(edge, jnp.where(i % 2 == par, 4, 0), cnt),
            jnp.where(edge, 4 * (i // 2), u0))


def bias_of(q, i):
    square = is_square(i)
    need = jnp.where(is_edge(q), jnp.where(q == 0, i % 2, i) == 0, jnp.where(q == 1, i == 1, ~square))
    return need, jnp.where(q == 0, i // 2, jnp.where(q == 2, pick(i, WIDE), 0))


def reduce_kernel(xq, dyq, xp, dyp, xi, dyi, xo, dyo, ln,
                  g_a, g_b, g_c, v_out, ss_out, sib_land, x_land, y_land,
                  xbuf, dybuf, acc, part, stage, stage_r, flat, vec, vsum, vflat, vland, lnbuf, ss, ss_small,
                  x_sem, dy_sem, sib_send, sib_recv, out_send, x_recv, y_recv,
                  v_send, v_recv, st_sem, sr_sem, fl_sem, misc_sem):
    me, chip, core, sib, xn, yn = neighbours()
    kinds = ((xq, dyq), (xp, dyp), (xi, dyi), (xo, dyo))
    here = X1

    def arrived(ref, sem):
        remote(ref, ref, misc_sem.at[0], sem, sib).wait_recv()

    def issue(j):
        n, slot = j // CHUNKS, j % CHUNKS
        t, i = task_of(n)
        kind, rb, cb = operands_of(chip_of(t, chip), i)
        for which, (x_ref, dy_ref) in enumerate(kinds):
            @pl.when(kind == which)
            def _():
                local(x_ref.at[tile(slot, KC), tile(rb, BLOCK)], xbuf.at[slot], x_sem.at[slot]).start()
                local(dy_ref.at[tile(slot, KC), tile(cb, D)], dybuf.at[slot], dy_sem.at[slot]).start()

    for j in range(CHUNKS - 1):
        issue(jnp.int32(j))
    ln_copy = local(ln, lnbuf, misc_sem.at[0])
    ln_copy.start()
    enter((sib, xn, yn))
    ln_copy.wait()
    ss[...] = jnp.zeros_like(ss)
    vec[...] = jnp.zeros_like(vec)
    for t in range(4):
        for q in (1, 3):
            @pl.when(chip_of(jnp.int32(t), chip) == q)
            def _():
                vec[t, 1:3, :] = lnbuf[q - 1:q + 1, :]

    def own_units(n, par, body):
        t, i = task_of(n)
        s0, cnt, u0 = units_of(chip_of(t, chip), i, par)
        each(s0, s0 + cnt, lambda s: body(t, u0 + s - s0, s, t * UNITS + u0 + s - s0))

    def relayed(t, u, do):
        @pl.when((t == B1) & (u % 2 == 1))
        def _():
            do(y_land, y_recv)

        @pl.when((t == Y1) & (u % 2 == 0))
        def _():
            do(x_land, x_recv)

    def prefetch(n):
        def body(t, u, s, e):
            arrived(sib_land.at[e], sib_recv.at[e])
            local(sib_land.at[e], stage.at[s], st_sem.at[s]).start()

            def more(land, recv):
                arrived(land.at[u // 2], recv.at[u // 2])
                local(land.at[u // 2], stage_r.at[s], sr_sem.at[s]).start()
            relayed(t, u, more)
        own_units(n, core, body)

    def combine(n):
        def body(t, u, s, e):
            local(sib_land.at[e], stage.at[s], st_sem.at[s]).wait()
            part[e] = acc[n % 3, tile(s, UR), :] + stage[s]

            def more(land, recv):
                local(land.at[u // 2], stage_r.at[s], sr_sem.at[s]).wait()
                part[e] = part[e] + stage_r[s]
            relayed(t, u, more)
        own_units(n, core, body)
        t, i = task_of(n)

        @pl.when(i == HALF - 1)
        def _():
            remote(vec.at[t], vland.at[t], v_send.at[t], v_recv.at[t], sib).wait()
            vsum[t] = vec[t] + vland[t]

            @pl.when(t == Y1)
            def _():
                arrived(vland.at[4], v_recv.at[4])
                vsum[t] = vsum[t] + vland[4]

    def send_own(n):
        def body(t, u, s, e):
            def go(land, recv, slot, dev):
                remote(part.at[e], land.at[slot], out_send.at[e], recv.at[slot], dev).start()

            @pl.when((t == 0) & (u % 2 == 0))
            def _():
                go(x_land, x_recv, u // 2, xn)

            @pl.when((t == 0) & (u % 2 == 1))
            def _():
                go(y_land, y_recv, u // 2, yn)

            @pl.when(t == B1)
            def _():
                go(x_land, x_recv, HALF + u, xn)

            @pl.when(t == Y1)
            def _():
                go(y_land, y_recv, HALF + u, yn)
        own_units(n, core, body)
        t, i = task_of(n)
        for way, dev in enumerate((xn, xn, yn)):
            @pl.when((i == HALF - 1) & (t == way))
            def _():
                remote(vsum.at[t], vland.at[4 + way], v_send.at[4 + way], v_recv.at[4 + way], dev).start()

    def sib_units(n, act):
        def body(t, u, s, e):
            act_on(remote(acc.at[n % 3, tile(s, UR)], sib_land.at[e], sib_send.at[e], sib_recv.at[e], sib), act)
        own_units(n, other(core), body)

    def task(n):
        t, i = task_of(n)
        need, row = bias_of(chip_of(t, chip), i)
        a = n % 3

        @pl.when(n >= 3)
        def _():
            sib_units(n - 3, 'sent')

        def chunk(slot):
            j = n * CHUNKS + slot

            @pl.when(j + CHUNKS - 1 < STEPS)
            def _():
                issue(j + CHUNKS - 1)
            local(xq.at[tile(0, KC), tile(0, BLOCK)], xbuf.at[slot], x_sem.at[slot]).wait()
            local(dyq.at[tile(0, KC), tile(0, D)], dybuf.at[slot], dy_sem.at[slot]).wait()

            def dot():
                return lax.dot_general(xbuf[slot], dybuf[slot], (((0,), (0,)), ((), ())),
                                       preferred_element_type=F32)

            @pl.when(slot == 0)
            def _():
                acc[a] = dot()

            @pl.when(slot > 0)
            def _():
                acc[a] += dot()

            @pl.when(need)
            def _():
                def add(r, total):
                    block = dybuf[slot, tile(r, LANES), :].astype(F32)
                    return total + jnp.sum(block.reshape(-1, 8, D), axis=0)
                total = lax.fori_loop(0, KC // LANES, add, jnp.zeros_like(ss))
                vec[t, pl.ds(row, 1), :] += jnp.sum(total, axis=0, keepdims=True)

            @pl.when((slot == 1) & (n > 0))
            def _():
                prefetch(n - 1)

            @pl.when((slot == 2) & (n > 0))
            def _():
                combine(n - 1)
                send_own(n - 1)
        each(0, CHUNKS, chunk)
        sib_units(n, 'start')

        @pl.when(i == HALF - 1)
        def _():
            remote(vec.at[t], vland.at[t], v_send.at[t], v_recv.at[t], sib).start()

    each(0, TASKS, task)
    prefetch(jnp.int32(TASKS - 1))
    combine(jnp.int32(TASKS - 1))
    each(TASKS - 3, TASKS, lambda n: sib_units(n, 'sent'))

    few = chip - 1 == core
    mid = jnp.logical_not(is_edge(chip))
    past = chip == 2

    def write_unit(u, slot):
        def go(dst):
            local(flat.at[slot], dst, fl_sem.at[slot]).start()

        @pl.when(chip == 0)
        def _():
            go(g_a.at[tile(u % 4, UR), tile(u // 4, 8)])

        @pl.when(chip == 3)
        def _():
            go(g_c.at[tile(u, UR)])
        square = jnp.where((u >= FEW[1]) & (u < FEW[2]), u - FEW[1],
                           jnp.where((u >= FEW[4]) & (u < FEW[-1]), u - 3, -1))
        col = jnp.where(u < FEW[2], 0, jnp.where(u < FEW[4], u - 4, 3))

        @pl.when(mid & few & (square < 0))
        def _():
            go(g_b.at[tile(jnp.where(past, 0, 2), UR), tile(col, 8)])

        @pl.when(mid & few & (square >= 0))
        def _():
            go(g_c.at[tile(jnp.where(past, 4, 0) + square, UR)])

        @pl.when(mid & jnp.logical_not(few))
        def _():
            go(g_b.at[tile(u % 3, UR), tile(u // 3, 8)])

    def written(slot):
        local(flat.at[slot], g_c.at[tile(0, UR)], fl_sem.at[slot]).wait()

    def finish(u):
        copies = []
        for e, (land, recv) in enumerate(((x_land, x_recv), (y_land, y_recv))):
            arrived(land.at[HALF + u], recv.at[HALF + u])
            copies.append(local(land.at[HALF + u], stage.at[e], st_sem.at[e]))
            copies[e].start()
        slot = u % 2

        @pl.when(u >= 2)
        def _():
            written(slot)
        for c in copies:
            c.wait()

        def add(r, total):
            rows = tile(r, 16)
            val = part[here * UNITS + u, rows, :] + stage[0, rows, :] + stage[1, rows, :]
            flat[slot, rows] = val.reshape(16, 8, LANES)
            return total + val[0:8] * val[0:8] + val[8:16] * val[8:16]
        ss[...] += lax.fori_loop(0, UR // 16, add, jnp.zeros_like(ss))
        write_unit(u, slot)

    each(0, UNITS, finish)
    arrived(vland.at[5], v_recv.at[5])
    arrived(vland.at[6], v_recv.at[6])
    val = vsum[here] + vland[5] + vland[6]
    vflat[...] = val.reshape(8, 8, LANES)
    total = ss[...] + jnp.where(core == 0, 1.0, 0.0).astype(F32) * (val * val)
    ss_small[...] = sum(total[:, LANES * c:LANES * (c + 1)] for c in range(8))
    tail = [local(vflat, v_out, misc_sem.at[0]), local(ss_small, ss_out, misc_sem.at[1])]
    for c in tail:
        c.start()
    written(0)
    written(1)
    for c in tail:
        c.wait()
    each(0, here * UNITS, lambda e: remote(part.at[e], x_land.at[0], out_send.at[e], x_recv.at[0], xn).wait_send())
    for way in range(3):
        remote(vsum.at[way], vland.at[4], v_send.at[4 + way], v_recv.at[4], xn).wait_send()


def shape(*dims, dtype=F32):
    return jax.ShapeDtypeStruct(dims, dtype)


def vmem(*dims, dtype=F32):
    return pltpu.VMEM(dims, dtype)


def dmas(*counts):
    return [pltpu.SemaphoreType.DMA(c if isinstance(c, tuple) else (c,)) for c in counts]


def any_space(count):
    return [pl.BlockSpec(memory_space=pltpu.HBM)] * count


def params_of(collective_id, mib):
    return pltpu.CompilerParams(collective_id=collective_id, has_side_effects=True, vmem_limit_bytes=mib * MIB)


def reduce_call(acts, ln_rows):
    lands = UNITS + HALF
    outs = [shape(512, 24, LANES), shape(384, 32, LANES), shape(1536, 8, LANES), shape(8, 8, LANES), shape(8, LANES),
            shape(4 * UNITS, UR, D), shape(lands, UR, D), shape(lands, UR, D)]
    return pl.pallas_call(
        reduce_kernel,
        out_shape=outs,
        in_specs=any_space(len(acts) + 1),
        out_specs=any_space(len(outs)),
        scratch_shapes=[
            vmem(CHUNKS, KC, BLOCK, dtype=BF16), vmem(CHUNKS, KC, D, dtype=BF16), vmem(3, BLOCK, D),
            vmem(4 * UNITS, UR, D), vmem(4, UR, D), vmem(4, UR, D), vmem(2, UR, 8, LANES),
            vmem(4, 8, D), vmem(4, 8, D), vmem(8, 8, LANES), vmem(7, 8, D), vmem(4, D), vmem(8, D), vmem(8, LANES),
            *dmas(CHUNKS, CHUNKS, 4 * UNITS, 4 * UNITS, 3 * UNITS, lands, lands, 7, 7, 4, 4, 2, 2)],
        compiler_params=params_of(0, 62),
        name='grad_reduce',
    )(*acts, ln_rows)


PARTS = 16
SEG = SHARE // PARTS
CUTS = [SEG * j for j in range(PARTS)] + [SHARD_ROWS]
BLK = 64
FULL = SHARE // BLK
LOADS = 8
LOAD = SHARE // LOADS
GB = FULL // LOADS


def update_kernel(w_in, m_in, v_in, ga, gb, gc, vg, ss_in,
                  wbuf, mbuf, vbuf, params, full,
                  gbuf, cin, ssl, sums, rates,
                  load_sem, g_sem, edge_send, edge_recv, ss_send, ss_recv, sum_send, sum_recv,
                  own_send, own_copy, x_recv, y_recv, d_recv, s_recv, fwd_send, sib_fwd, cin_sem):
    me, chip, core, sib, xn, yn = neighbours()

    def floor_of(dev):
        return DOWN * (SHARD_ROWS * dev // DOWN)

    def in_window(dev, row):
        return row - SHARD_ROWS * dev + EDGE

    def load_rows(k):
        return pl.ds(LOAD * k, LOAD if k < LOADS - 1 else SHARD_ROWS - LOAD * k)

    loads = [[local(src.at[load_rows(k)], dst.at[load_rows(k)], load_sem.at[e, k])
              for e, (src, dst) in enumerate(((w_in, wbuf), (m_in, mbuf), (v_in, vbuf)))] for k in range(LOADS)]

    def when_in(lo, hi, do, *args):
        @pl.when((me >= lo) & (me <= hi))
        def _():
            do(*args)

    def g_loads(act):
        start = in_window(me, pick(me, NOMINAL))

        def go(*copies):
            for e, (src, lo, size, at) in enumerate(copies):
                act_on(local(src.at[pl.ds(lo, size)], gbuf.at[pl.ds(start + at, size)], g_sem.at[e]), act)
        two, one = SIZES[2], SHARE - SIZES[2]
        tail = (vg, 0, UP, SHARE)
        when_in(0, 0, go, (ga, 0, SHARE, 0))
        when_in(1, 1, go, (ga, 0, SHARE, 0), tail)
        when_in(2, 2, go, (gc, 0, two, 0), (vg, 0, UP, two), (gb, two, one, two + UP))
        when_in(3, 4, go, (gb, 0, SHARE, 0))
        when_in(5, 5, go, (gb, 0, one, 0), (vg, 0, SIZES[7], one), (gc, one, two, one + SIZES[7]))
        when_in(6, 6, go, (gc, 0, SHARE, 0))
        when_in(7, 7, go, (gc, 0, SHARE, 0), tail)

    ss_copy = local(ss_in, ssl.at[me], cin_sem.at[0])
    ss_copy.start()
    g_loads('start')
    for group in loads:
        for c in group:
            c.start()
    sums[...] = jnp.zeros_like(sums)
    ss_copy.wait()
    others = [lax.rem(me + e, N_DEV) for e in range(1, N_DEV)]
    enter(others)

    def share(buf, send, recv, act):
        for e, dev in enumerate(others):
            if act == 'get':
                remote(buf.at[dev], buf.at[dev], send.at[e], recv.at[dev], dev).wait_recv()
            else:
                act_on(remote(buf.at[me], buf.at[me], send.at[e], recv.at[me], dev), act)

    share(ssl, ss_send, ss_recv, 'start')

    def edges(act):
        def go(src, lo, size, dev, row, e):
            act_on(remote(src.at[pl.ds(lo, size)], gbuf.at[pl.ds(in_window(dev, row), size)],
                          edge_send.at[e], edge_recv.at[e], dev), act)

        def up(src):
            go(src, 0, UP, me - 1, pick(me, NOMINAL), 0)

        def down(src):
            go(src, SHARE - DOWN, DOWN, me + 1, pick(me + 1, NOMINAL) - DOWN, 1)
        when_in(1, 1, up, ga)
        when_in(2, 2, up, gc)
        when_in(3, 5, up, gb)
        when_in(6, 7, up, gc)
        when_in(0, 1, down, ga)
        when_in(2, 4, down, gb)
        when_in(5, 6, down, gc)

    edges('start')
    share(ssl, ss_send, ss_recv, 'get')
    grad_sq = jnp.sum(sum(ssl[e] for e in range(N_DEV)))
    grad_sq = grad_sq * (1.0 / (N_DEV * N_DEV))
    norm = jnp.sqrt(jnp.full((8, LANES), grad_sq, F32))
    scale = (1.0 / N_DEV) / jnp.maximum(1.0, norm)
    scale = jnp.concatenate([scale] * (BLK // 8), axis=0)
    for e, (has, size) in enumerate(((me < N_DEV - 1, UP), (me > 0, DOWN))):
        @pl.when(has)
        def _():
            rows = gbuf.at[pl.ds(0, size)]
            remote(rows, rows, edge_send.at[e], edge_recv.at[e], sib).wait_recv()
    g_loads('wait')
    first_t, past_t = pick(me, FIRST_TENSOR), pick(me, PAST_TENSOR)

    def over(first, past, body):
        def tensor(t):
            lo = pick(t, STARTS[:-1]) - SHARD_ROWS * me
            hi = pick(t, STARTS[1:]) - SHARD_ROWS * me
            from_b = jnp.maximum(lo // BLK, first)
            to_b = jnp.maximum(from_b, jnp.minimum((hi + BLK - 1) // BLK, min(past, FULL)))

            def keep(b, size):
                ids = lax.broadcasted_iota(jnp.int32, (size, LANES), 0) + b * BLK
                return (ids >= lo) & (ids < hi)
            body(t, from_b, to_b, keep, past > FULL)
        each(first_t, past_t, tensor)

    REST = SHARD_ROWS - FULL * BLK

    def direction(t, first, past, keep_of, with_rest):
        decay = jnp.where((t % 2 == 0) & (t != 4) & (t < 9), DECAY, 0.0).astype(F32)

        def rows(at, g_at, keep, rate):
            g, w, m, v = gbuf[g_at, :], wbuf[at, :], mbuf[at, :], vbuf[at, :]
            h = g * rate
            new_m = BETA_ONE * m + (1.0 - BETA_ONE) * h
            new_v = BETA_TWO * v + (1.0 - BETA_TWO) * h * h
            u = (new_m * (1.0 / CORR_ONE)) / (jnp.sqrt(new_v * (1.0 / CORR_TWO)) + EPSILON) + decay * w
            mbuf[at, :] = jnp.where(keep, new_m, m)
            vbuf[at, :] = jnp.where(keep, new_v, v)
            gbuf[g_at, :] = jnp.where(keep, u, g)
            return jnp.where(keep, u * u, 0.0), jnp.where(keep, w * w, 0.0)

        def block(b, carry):
            found = rows(tile(b, BLK), pl.ds(pl.multiple_of(b * BLK + EDGE, DOWN), BLK), keep_of(b, BLK), scale)
            return tuple(total + jnp.sum(sq.reshape(-1, 8, LANES), axis=0) for total, sq in zip(carry, found))

        def note(at, sq):
            sums[me, pl.ds(at, 1), :] += jnp.sum(sq, axis=0, keepdims=True)
        zero = jnp.zeros((8, LANES), F32)
        found = lax.fori_loop(first, past, block, (zero, zero))
        note(t, found[0])
        note(DOWN + t, found[1])
        if with_rest:
            found = rows(pl.ds(FULL * BLK, REST), pl.ds(FULL * BLK + EDGE, REST), keep_of(FULL, REST), scale[:REST])
            note(t, found[0])
            note(DOWN + t, found[1])

    for k in range(LOADS):
        for c in loads[k]:
            c.wait()
        over(GB * k, GB * (k + 1) + (k == LOADS - 1), direction)
    share(sums, sum_send, sum_recv, 'start')
    share(sums, sum_send, sum_recv, 'get')
    total = jnp.sum(sum(sums[e] for e in range(N_DEV)), axis=1, keepdims=True)
    u_n, w_n = jnp.sqrt(total[:DOWN]), jnp.sqrt(total[DOWN:])
    both = (u_n > 0) & (w_n > 0)
    ratio = jnp.where(both, w_n / jnp.where(u_n > 0, u_n, 1.0), 1.0)
    rates[...] = jnp.broadcast_to(LEARN_RATE * ratio, rates.shape)

    def apply(t, first, past, keep_of, with_rest):
        def rows(at, g_at, keep):
            w = wbuf[at, :]
            rate = jnp.broadcast_to(rates[pl.ds(t, 1), :], w.shape)
            wbuf[at, :] = jnp.where(keep, w - rate * gbuf[g_at, :], w)

        def block(b):
            rows(tile(b, BLK), pl.ds(pl.multiple_of(b * BLK + EDGE, DOWN), BLK), keep_of(b, BLK))
        each(first, past, block)
        if with_rest:
            rows(pl.ds(FULL * BLK, REST), pl.ds(FULL * BLK + EDGE, REST), keep_of(FULL, REST))

    def cut(dev, j):
        return pl.ds(SHARD_ROWS * dev + CUTS[j], CUTS[j + 1] - CUTS[j])

    def twin(dev):
        return dev + other(2 * core)

    dg = N_DEV - 2 * (chip + 1) + core

    def own_part(j, e, sem, dev):
        return remote(wbuf.at[cut(0, j)], full.at[cut(me, j)], own_send.at[e, j], sem, dev)

    PB = SEG // BLK
    for j in range(PARTS):
        over(PB * j, PB * (j + 1) + (j == PARTS - 1), apply)
        for e, (sem, dev) in enumerate(((x_recv.at[j], xn), (y_recv.at[j], yn), (s_recv.at[0, j], sib))):
            own_part(j, e, sem, dev).start()
        local(wbuf.at[cut(0, j)], full.at[cut(me, j)], own_copy.at[j]).start()

    def wait_from(dev, j, sem):
        rows = full.at[cut(dev, j)]
        remote(rows, rows, cin_sem.at[0], sem, sib).wait_recv()

    def forward(dev, j, send_sem, recv_sem, to):
        rows = full.at[cut(dev, j)]
        remote(rows, rows, send_sem, recv_sem, to).start()

    def convert(*parts):
        todo = []
        for slot, (dev, j) in enumerate(parts):
            skip = DOWN if j == 0 else 0
            lo, size = pl.multiple_of(floor_of(dev) + skip + SEG * j, DOWN), SEG - skip
            cp = local(full.at[pl.ds(lo, size)], cin.at[slot, pl.ds(0, size)], cin_sem.at[slot])
            cp.start()
            todo.append((cp, slot, lo, size))
        for cp, slot, lo, size in todo:
            cp.wait()

            def body(b):
                params[pl.ds(pl.multiple_of(lo + b * DOWN, DOWN), DOWN), :] = cin[slot, tile(b, DOWN), :].astype(BF16)
            lax.fori_loop(0, size // DOWN, lambda b, c: (body(b), c)[1], 0, unroll=8)

    for j in range(PARTS):
        local(wbuf.at[cut(0, j)], full.at[cut(me, j)], own_copy.at[j]).wait()
        wait_from(sib, j, s_recv.at[0, j])
        convert((me, j), (sib, j))
        wait_from(xn, j, x_recv.at[j])
        forward(xn, j, sib_fwd.at[0, j], s_recv.at[1, j], sib)
        if j % 2 == 0:
            forward(xn, j, fwd_send.at[j], d_recv.at[j], yn)
        wait_from(yn, j, y_recv.at[j])
        forward(yn, j, sib_fwd.at[1, j], s_recv.at[2, j], sib)
        if j % 2 == 1:
            forward(yn, j, fwd_send.at[j], d_recv.at[j], xn)
        convert((xn, j), (yn, j))
        wait_from(twin(xn), j, s_recv.at[1, j])
        wait_from(twin(yn), j, s_recv.at[2, j])
        convert((twin(xn), j), (twin(yn), j))
    for j in range(0, PARTS, 2):
        both_parts = (j, j + 1)
        for e in both_parts:
            wait_from(dg, e, d_recv.at[e])
            forward(dg, e, sib_fwd.at[2, e], s_recv.at[3, e], sib)
        convert(*[(dg, e) for e in both_parts])
        for e in both_parts:
            wait_from(twin(dg), e, s_recv.at[3, e])
        if e == PARTS - 1:
            low = DOWN * (SHARD_ROWS * (N_DEV - 1) // DOWN) + SHARE
            pieces = ([(0, DOWN)] + [(DOWN * (SHARD_ROWS * s // DOWN) - DOWN, 2 * DOWN) for s in range(1, N_DEV)]
                      + [(low, TOTAL_ROWS - low)])
            ends = [local(full.at[pl.ds(lo, size)], cin.at[2, pl.ds(2 * DOWN * p, size)], cin_sem.at[2 + p])
                    for p, (lo, size) in enumerate(pieces)]
            for c in ends:
                c.start()
        convert(*[(twin(dg), e) for e in both_parts])
    for p, (c, (lo, size)) in enumerate(zip(ends, pieces)):
        c.wait()
        params[lo:lo + size, :] = cin[2, 2 * DOWN * p:2 * DOWN * p + size, :].astype(BF16)
    edges('sent')
    share(ssl, ss_send, ss_recv, 'sent')
    share(sums, sum_send, sum_recv, 'sent')
    for j in range(PARTS):
        sems = [fwd_send.at[j]] + [s.at[e, j] for s in (own_send, sib_fwd) for e in range(3)]
        for sem in sems:
            remote(wbuf.at[cut(0, j)], full.at[cut(me, j)], sem, x_recv.at[j], xn).wait_send()


def update_call(w, m, v, ga, gb, gc, vg, ss):
    shard = pltpu.VMEM((SHARD_ROWS, LANES), F32)
    outs = [shard, shard, shard, pltpu.VMEM((TOTAL_ROWS, LANES), BF16), shape(TOTAL_ROWS, LANES)]
    in_vmem = pl.BlockSpec(memory_space=pltpu.VMEM)
    return pl.pallas_call(
        update_kernel,
        out_shape=outs,
        in_specs=any_space(8),
        out_specs=[in_vmem] * 4 + any_space(1),
        scratch_shapes=[
            vmem(WIN, LANES), vmem(3, SEG, LANES),
            vmem(N_DEV, 8, LANES), vmem(N_DEV, 2 * DOWN, LANES), vmem(DOWN, LANES),
            *dmas((3, LOADS), 3, 2, 2, 7, N_DEV, 7, N_DEV, (3, PARTS), PARTS, PARTS, PARTS, PARTS, (4, PARTS),
                  PARTS, (3, PARTS), 11)],
        compiler_params=params_of(1, 14),
        name='lamb_gather',
    )(w, m, v, ga, gb, gc, vg, ss)


def write_kernel(*refs):
    *pairs, sem = refs
    half = len(pairs) // 2
    copies = [local(src, dst, sem.at[e]) for e, (src, dst) in enumerate(zip(pairs[:half], pairs[half:]))]
    for c in copies:
        c.start()
    for c in copies:
        c.wait()


def write_call(arrays):
    return pl.pallas_call(
        write_kernel,
        out_shape=[jax.ShapeDtypeStruct(a.shape, a.dtype) for a in arrays],
        in_specs=[pl.BlockSpec(memory_space=pltpu.VMEM)] * len(arrays),
        out_specs=any_space(len(arrays)),
        scratch_shapes=dmas(len(arrays)),
        compiler_params=pltpu.CompilerParams(vmem_limit_bytes=MIB),
        name='write_out',
    )(*arrays)


def solution(mesh):
    def local_step(weights, moment_one, moment_two, *rest):
        *acts, ln_grad = rest
        ga, gb, gc, vg, ss, *_ = reduce_call(acts, ln_grad[0])
        rows = [a.reshape(SHARD_ROWS, LANES) for a in (weights, moment_one, moment_two)]
        out = update_call(*rows, *(g.reshape(-1, LANES) for g in (ga, gb, gc, vg)), ss)
        return tuple(a.reshape(-1) for a in write_call(out[:-1]))

    row_spec = P('dp', None)
    flat_spec = P('dp')
    in_specs = (flat_spec,) * 3 + (row_spec,) * 8 + (P('dp', None, None),)
    return jax.shard_map(local_step, mesh=mesh, in_specs=in_specs, out_specs=(flat_spec,) * 3 + (P(),), check_vma=False)
```

```python
import jax
import jax.numpy as jnp
from jax import lax
from jax.experimental import pallas as pl
from jax.experimental.pallas import tpu as pltpu
from jax.sharding import PartitionSpec as P

STEP = 10
LEARN_RATE = 0.5
BETA_ONE = 0.9
BETA_TWO = 0.999
EPSILON = 1e-6
DECAY = 0.01
CORR_ONE = 1.0 - BETA_ONE ** STEP
CORR_TWO = 1.0 - BETA_TWO ** STEP

D = 1024
N_DEV = 8
TOKENS = 4096
LANES = 128
SHARD_ROWS = 12301
TOTAL_ROWS = N_DEV * SHARD_ROWS
KC = 1024
CHUNKS = TOKENS // KC
BLOCK = 512
TASKS = 24
STEPS = TASKS * CHUNKS
UR = 128
UNITS = 12
HALF = UNITS // 2
F32 = jnp.float32
BF16 = jnp.bfloat16
MIB = 1024 * 1024

SIZES = [24576, 24, 8192, 8, 8, 8, 32768, 32, 32768, 8, 8, 8]
STARTS = [sum(SIZES[:pos]) for pos in range(len(SIZES) + 1)]
SHARE = UNITS * D
NOMINAL = [0, 12288, 24600, 36912, 49200, 61488, 73808, 86096]
FIRST_TENSOR = [max(t for t, at in enumerate(STARTS[:-1]) if at <= SHARD_ROWS * dev) for dev in range(N_DEV)]
PAST_TENSOR = [1 + max(t for t, at in enumerate(STARTS[:-1]) if at < SHARD_ROWS * (dev + 1)) for dev in range(N_DEV)]
EDGE = 48
WIN = 12416
UP, DOWN = 24, 16
FEW = [0, 1, 5, 6, 7, 11]
MANY = [0, 3, 3, 6, 9, 9]
WIDE = [0, 0, 1, 2, 0, 3]
B1, Y1, X1 = range(1, 4)


def pick(index, values):
    out = jnp.int32(values[-1])
    for pos in reversed(range(len(values) - 1)):
        out = jnp.where(index == pos, jnp.int32(values[pos]), out)
    return out


def tile(index, size):
    return pl.ds(pl.multiple_of(index * size, size), size)


def each(lo, hi, body):
    def step(pos, carry):
        body(pos)
        return carry
    lax.fori_loop(lo, hi, step, lo)


def other(bit):
    return 1 - bit


def device(y, x, core):
    return 4 * y + 2 * x + core


def neighbours():
    me = lax.axis_index('dp')
    chip, core = me // 2, me % 2
    x, y = chip % 2, chip // 2
    return me, chip, core, device(y, x, other(core)), device(y, other(x), core), device(other(y), x, core)


def local(src, dst, sem):
    return pltpu.make_async_copy(src, dst, sem)


def remote(src, dst, send_sem, recv_sem, dev):
    return pltpu.make_async_remote_copy(src_ref=src, dst_ref=dst, send_sem=send_sem, recv_sem=recv_sem,
                                        device_id=(dev,), device_id_type=pl.DeviceIdType.MESH)


def act_on(copy, act):
    if act == 'start':
        copy.start()
    elif act == 'sent':
        copy.wait_send()
    else:
        copy.wait()


def enter(devices):
    barrier = pltpu.get_barrier_semaphore()
    for dev in devices:
        pl.semaphore_signal(barrier, inc=1, device_id=(dev,), device_id_type=pl.DeviceIdType.MESH)
    pl.semaphore_wait(barrier, len(devices))


def task_of(n):
    six = HALF
    mid = n - six
    first, last = n < six, n >= 3 * six
    t = jnp.where(first, 0, jnp.where(last, X1, B1 + mid % 2))
    i = jnp.where(first, n, jnp.where(last, n - 3 * six, mid // 2))
    return t, i


def chip_of(t, chip):
    x, y = chip % 2, chip // 2
    return 2 * ((y + other(t % 2)) % 2) + (x + other(t // 2)) % 2


def is_square(i):
    return i % 3 == 1


def is_edge(q):
    return q % 3 == 0


def operands_of(q, i):
    square, odd, pair = is_square(i), i % 2, i // 2
    kind = jnp.where(is_edge(q), q, jnp.where(square, 2 * q - 1, 2))
    rb = jnp.where(q == 0, odd, jnp.where(is_edge(q), 2 + 3 * odd + pair, jnp.where(square, i // 4, q - 1)))
    cb = jnp.where(q == 0, pair, jnp.where(is_edge(q) | square, 0, pick(i, WIDE)))
    return kind, rb, cb


def units_of(q, i, par):
    square = is_square(i)
    few = q - 1 == par
    cnt = jnp.where(few, jnp.where(square, 4, 1), jnp.where(square, 0, 3))
    s0 = jnp.where(square | (par == 0), 0, 2 * q - 1)
    u0 = jnp.where(few, pick(i, FEW), pick(i, MANY))
    edge = is_edge(q)
    return (jnp.where(edge, 0, s0), jnp.where(edge, jnp.where(i % 2 == par, 4, 0), cnt),
            jnp.where(edge, 4 * (i // 2), u0))


def bias_of(q, i):
    square = is_square(i)
    need = jnp.where(is_edge(q), jnp.where(q == 0, i % 2, i) == 0, jnp.where(q == 1, i == 1, ~square))
    return need, jnp.where(q == 0, i // 2, jnp.where(q == 2, pick(i, WIDE), 0))


def reduce_kernel(xq, dyq, xp, dyp, xi, dyi, xo, dyo, ln,
                  g_a, g_b, g_c, v_out, ss_out, sib_land, x_land, y_land,
                  xbuf, dybuf, acc, part, stage, stage_r, flat, vec, vsum, vflat, vland, lnbuf, ss, ss_small,
                  x_sem, dy_sem, sib_send, sib_recv, out_send, x_recv, y_recv,
                  v_send, v_recv, st_sem, sr_sem, fl_sem, misc_sem):
    me, chip, core, sib, xn, yn = neighbours()
    kinds = ((xq, dyq), (xp, dyp), (xi, dyi), (xo, dyo))
    here = X1

    def arrived(ref, sem):
        remote(ref, ref, misc_sem.at[0], sem, sib).wait_recv()

    def issue(j):
        n, slot = j // CHUNKS, j % CHUNKS
        t, i = task_of(n)
        kind, rb, cb = operands_of(chip_of(t, chip), i)
        for which, (x_ref, dy_ref) in enumerate(kinds):
            @pl.when(kind == which)
            def _():
                local(x_ref.at[tile(slot, KC), tile(rb, BLOCK)], xbuf.at[slot], x_sem.at[slot]).start()
                local(dy_ref.at[tile(slot, KC), tile(cb, D)], dybuf.at[slot], dy_sem.at[slot]).start()

    for j in range(CHUNKS - 1):
        issue(jnp.int32(j))
    ln_copy = local(ln, lnbuf, misc_sem.at[0])
    ln_copy.start()
    enter((sib, xn, yn))
    ln_copy.wait()
    ss[...] = jnp.zeros_like(ss)
    vec[...] = jnp.zeros_like(vec)
    for t in range(4):
        for q in (1, 3):
            @pl.when(chip_of(jnp.int32(t), chip) == q)
            def _():
                vec[t, 1:3, :] = lnbuf[q - 1:q + 1, :]

    def own_units(n, par, body):
        t, i = task_of(n)
        s0, cnt, u0 = units_of(chip_of(t, chip), i, par)
        each(s0, s0 + cnt, lambda s: body(t, u0 + s - s0, s, t * UNITS + u0 + s - s0))

    def relayed(t, u, do):
        @pl.when((t == B1) & (u % 2 == 1))
        def _():
            do(y_land, y_recv)

        @pl.when((t == Y1) & (u % 2 == 0))
        def _():
            do(x_land, x_recv)

    def prefetch(n):
        def body(t, u, s, e):
            arrived(sib_land.at[e], sib_recv.at[e])
            local(sib_land.at[e], stage.at[s], st_sem.at[s]).start()

            def more(land, recv):
                arrived(land.at[u // 2], recv.at[u // 2])
                local(land.at[u // 2], stage_r.at[s], sr_sem.at[s]).start()
            relayed(t, u, more)
        own_units(n, core, body)

    def combine(n):
        def body(t, u, s, e):
            local(sib_land.at[e], stage.at[s], st_sem.at[s]).wait()
            part[e] = acc[n % 3, tile(s, UR), :] + stage[s]

            def more(land, recv):
                local(land.at[u // 2], stage_r.at[s], sr_sem.at[s]).wait()
                part[e] = part[e] + stage_r[s]
            relayed(t, u, more)
        own_units(n, core, body)
        t, i = task_of(n)

        @pl.when(i == HALF - 1)
        def _():
            remote(vec.at[t], vland.at[t], v_send.at[t], v_recv.at[t], sib).wait()
            vsum[t] = vec[t] + vland[t]

            @pl.when(t == Y1)
            def _():
                arrived(vland.at[4], v_recv.at[4])
                vsum[t] = vsum[t] + vland[4]

    def send_own(n):
        def body(t, u, s, e):
            def go(land, recv, slot, dev):
                remote(part.at[e], land.at[slot], out_send.at[e], recv.at[slot], dev).start()

            @pl.when((t == 0) & (u % 2 == 0))
            def _():
                go(x_land, x_recv, u // 2, xn)

            @pl.when((t == 0) & (u % 2 == 1))
            def _():
                go(y_land, y_recv, u // 2, yn)

            @pl.when(t == B1)
            def _():
                go(x_land, x_recv, HALF + u, xn)

            @pl.when(t == Y1)
            def _():
                go(y_land, y_recv, HALF + u, yn)
        own_units(n, core, body)
        t, i = task_of(n)
        for way, dev in enumerate((xn, xn, yn)):
            @pl.when((i == HALF - 1) & (t == way))
            def _():
                remote(vsum.at[t], vland.at[4 + way], v_send.at[4 + way], v_recv.at[4 + way], dev).start()

    def sib_units(n, act):
        def body(t, u, s, e):
            act_on(remote(acc.at[n % 3, tile(s, UR)], sib_land.at[e], sib_send.at[e], sib_recv.at[e], sib), act)
        own_units(n, other(core), body)

    def task(n):
        t, i = task_of(n)
        need, row = bias_of(chip_of(t, chip), i)
        a = n % 3

        @pl.when(n >= 3)
        def _():
            sib_units(n - 3, 'sent')

        def chunk(slot):
            j = n * CHUNKS + slot

            @pl.when(j + CHUNKS - 1 < STEPS)
            def _():
                issue(j + CHUNKS - 1)
            local(xq.at[tile(0, KC), tile(0, BLOCK)], xbuf.at[slot], x_sem.at[slot]).wait()
            local(dyq.at[tile(0, KC), tile(0, D)], dybuf.at[slot], dy_sem.at[slot]).wait()

            def dot():
                return lax.dot_general(xbuf[slot], dybuf[slot], (((0,), (0,)), ((), ())),
                                       preferred_element_type=F32)

            @pl.when(slot == 0)
            def _():
                acc[a] = dot()

            @pl.when(slot > 0)
            def _():
                acc[a] += dot()

            @pl.when(need)
            def _():
                def add(r, total):
                    block = dybuf[slot, tile(r, LANES), :].astype(F32)
                    return total + jnp.sum(block.reshape(-1, 8, D), axis=0)
                total = lax.fori_loop(0, KC // LANES, add, jnp.zeros_like(ss))
                vec[t, pl.ds(row, 1), :] += jnp.sum(total, axis=0, keepdims=True)

            @pl.when((slot == 0) & (n > 0))
            def _():
                prefetch(n - 1)

            @pl.when((slot == 1) & (n > 0))
            def _():
                combine(n - 1)
                send_own(n - 1)
        each(0, CHUNKS, chunk)
        sib_units(n, 'start')

        @pl.when(i == HALF - 1)
        def _():
            remote(vec.at[t], vland.at[t], v_send.at[t], v_recv.at[t], sib).start()

    each(0, TASKS, task)
    prefetch(jnp.int32(TASKS - 1))
    combine(jnp.int32(TASKS - 1))
    each(TASKS - 3, TASKS, lambda n: sib_units(n, 'sent'))

    few = chip - 1 == core
    mid = jnp.logical_not(is_edge(chip))
    past = chip == 2

    def write_unit(u, slot):
        def go(dst):
            local(flat.at[slot], dst, fl_sem.at[slot]).start()

        @pl.when(chip == 0)
        def _():
            go(g_a.at[tile(u % 4, UR), tile(u // 4, 8)])

        @pl.when(chip == 3)
        def _():
            go(g_c.at[tile(u, UR)])
        square = jnp.where((u >= FEW[1]) & (u < FEW[2]), u - FEW[1],
                           jnp.where((u >= FEW[4]) & (u < FEW[-1]), u - 3, -1))
        col = jnp.where(u < FEW[2], 0, jnp.where(u < FEW[4], u - 4, 3))

        @pl.when(mid & few & (square < 0))
        def _():
            go(g_b.at[tile(jnp.where(past, 0, 2), UR), tile(col, 8)])

        @pl.when(mid & few & (square >= 0))
        def _():
            go(g_c.at[tile(jnp.where(past, 4, 0) + square, UR)])

        @pl.when(mid & jnp.logical_not(few))
        def _():
            go(g_b.at[tile(u % 3, UR), tile(u // 3, 8)])

    def written(slot):
        local(flat.at[slot], g_c.at[tile(0, UR)], fl_sem.at[slot]).wait()

    def finish(u):
        copies = []
        for e, (land, recv) in enumerate(((x_land, x_recv), (y_land, y_recv))):
            arrived(land.at[HALF + u], recv.at[HALF + u])
            copies.append(local(land.at[HALF + u], stage.at[e], st_sem.at[e]))
            copies[e].start()
        slot = u % 2

        @pl.when(u >= 2)
        def _():
            written(slot)
        for c in copies:
            c.wait()

        def add(r, total):
            rows = tile(r, 16)
            val = part[here * UNITS + u, rows, :] + stage[0, rows, :] + stage[1, rows, :]
            flat[slot, rows] = val.reshape(16, 8, LANES)
            return total + val[0:8] * val[0:8] + val[8:16] * val[8:16]
        ss[...] += lax.fori_loop(0, UR // 16, add, jnp.zeros_like(ss))
        write_unit(u, slot)

    each(0, UNITS, finish)
    arrived(vland.at[5], v_recv.at[5])
    arrived(vland.at[6], v_recv.at[6])
    val = vsum[here] + vland[5] + vland[6]
    vflat[...] = val.reshape(8, 8, LANES)
    total = ss[...] + jnp.where(core == 0, 1.0, 0.0).astype(F32) * (val * val)
    ss_small[...] = sum(total[:, LANES * c:LANES * (c + 1)] for c in range(8))
    tail = [local(vflat, v_out, misc_sem.at[0]), local(ss_small, ss_out, misc_sem.at[1])]
    for c in tail:
        c.start()
    written(0)
    written(1)
    for c in tail:
        c.wait()
    each(0, here * UNITS, lambda e: remote(part.at[e], x_land.at[0], out_send.at[e], x_recv.at[0], xn).wait_send())
    for way in range(3):
        remote(vsum.at[way], vland.at[4], v_send.at[4 + way], v_recv.at[4], xn).wait_send()


def shape(*dims, dtype=F32):
    return jax.ShapeDtypeStruct(dims, dtype)


def vmem(*dims, dtype=F32):
    return pltpu.VMEM(dims, dtype)


def dmas(*counts):
    return [pltpu.SemaphoreType.DMA(c if isinstance(c, tuple) else (c,)) for c in counts]


def any_space(count):
    return [pl.BlockSpec(memory_space=pltpu.HBM)] * count


def params_of(collective_id, mib):
    return pltpu.CompilerParams(collective_id=collective_id, has_side_effects=True, vmem_limit_bytes=mib * MIB)


def reduce_call(acts, ln_rows):
    lands = UNITS + HALF
    outs = [shape(512, 24, LANES), shape(384, 32, LANES), shape(1536, 8, LANES), shape(8, 8, LANES), shape(8, LANES),
            shape(CHUNKS * UNITS, UR, D), shape(lands, UR, D), shape(lands, UR, D)]
    return pl.pallas_call(
        reduce_kernel,
        out_shape=outs,
        in_specs=any_space(len(acts) + 1),
        out_specs=any_space(len(outs)),
        scratch_shapes=[
            vmem(CHUNKS, KC, BLOCK, dtype=BF16), vmem(CHUNKS, KC, D, dtype=BF16), vmem(3, BLOCK, D),
            vmem(CHUNKS * UNITS, UR, D), vmem(CHUNKS, UR, D), vmem(CHUNKS, UR, D), vmem(2, UR, 8, LANES),
            vmem(CHUNKS, 8, D), vmem(CHUNKS, 8, D), vmem(8, 8, LANES), vmem(7, 8, D), vmem(CHUNKS, D), vmem(8, D), vmem(8, LANES),
            *dmas(CHUNKS, CHUNKS, CHUNKS * UNITS, CHUNKS * UNITS, X1 * UNITS, lands, lands, 7, 7, CHUNKS, CHUNKS, 2, 2)],
        compiler_params=params_of(0, 62),
        name='grad_reduce',
    )(*acts, ln_rows)


PARTS = 16
SEG = SHARE // PARTS
CUTS = [SEG * j for j in range(PARTS)] + [SHARD_ROWS]
BLK = 128
FULL = SHARE // BLK
LOADS = 4
LOAD = SHARE // LOADS
GB = FULL // LOADS


def update_kernel(w_in, m_in, v_in, ga, gb, gc, vg, ss_in,
                  wbuf, mbuf, vbuf, params, full,
                  gbuf, cin, ssl, sums, rates,
                  load_sem, g_sem, edge_send, edge_recv, ss_send, ss_recv, sum_send, sum_recv,
                  own_send, own_copy, x_recv, y_recv, d_recv, s_recv, fwd_send, sib_fwd, cin_sem):
    me, chip, core, sib, xn, yn = neighbours()

    def floor_of(dev):
        return DOWN * (SHARD_ROWS * dev // DOWN)

    def in_window(dev, row):
        return row - SHARD_ROWS * dev + EDGE

    def load_rows(k):
        return pl.ds(LOAD * k, LOAD if k < LOADS - 1 else SHARD_ROWS - LOAD * k)

    loads = [[local(src.at[load_rows(k)], dst.at[load_rows(k)], load_sem.at[e, k])
              for e, (src, dst) in enumerate(((w_in, wbuf), (m_in, mbuf), (v_in, vbuf)))] for k in range(LOADS)]

    def when_in(lo, hi, do, *args):
        @pl.when((me >= lo) & (me <= hi))
        def _():
            do(*args)

    def g_loads(act):
        start = in_window(me, pick(me, NOMINAL))

        def go(*copies):
            for e, (src, lo, size, at) in enumerate(copies):
                act_on(local(src.at[pl.ds(lo, size)], gbuf.at[pl.ds(start + at, size)], g_sem.at[e]), act)
        two, one = SIZES[2], SHARE - SIZES[2]
        tail = (vg, 0, UP, SHARE)
        when_in(0, 0, go, (ga, 0, SHARE, 0))
        when_in(1, 1, go, (ga, 0, SHARE, 0), tail)
        when_in(2, 2, go, (gc, 0, two, 0), (vg, 0, UP, two), (gb, two, one, two + UP))
        when_in(3, 4, go, (gb, 0, SHARE, 0))
        when_in(5, 5, go, (gb, 0, one, 0), (vg, 0, SIZES[7], one), (gc, one, two, one + SIZES[7]))
        when_in(6, 6, go, (gc, 0, SHARE, 0))
        when_in(7, 7, go, (gc, 0, SHARE, 0), tail)

    ss_copy = local(ss_in, ssl.at[me], cin_sem.at[0])
    ss_copy.start()
    g_loads('start')
    for group in loads:
        for c in group:
            c.start()
    sums[...] = jnp.zeros_like(sums)
    ss_copy.wait()
    others = [lax.rem(me + e, N_DEV) for e in range(1, N_DEV)]
    enter(others)

    def share(buf, send, recv, act):
        for e, dev in enumerate(others):
            if act == 'get':
                remote(buf.at[dev], buf.at[dev], send.at[e], recv.at[dev], dev).wait_recv()
            else:
                act_on(remote(buf.at[me], buf.at[me], send.at[e], recv.at[me], dev), act)

    share(ssl, ss_send, ss_recv, 'start')

    def edges(act):
        def go(src, lo, size, dev, row, e):
            act_on(remote(src.at[pl.ds(lo, size)], gbuf.at[pl.ds(in_window(dev, row), size)],
                          edge_send.at[e], edge_recv.at[e], dev), act)

        def up(src):
            go(src, 0, UP, me - 1, pick(me, NOMINAL), 0)

        def down(src):
            go(src, SHARE - DOWN, DOWN, me + 1, pick(me + 1, NOMINAL) - DOWN, 1)
        when_in(1, 1, up, ga)
        when_in(2, 2, up, gc)
        when_in(3, 5, up, gb)
        when_in(6, 7, up, gc)
        when_in(0, 1, down, ga)
        when_in(2, 4, down, gb)
        when_in(5, 6, down, gc)

    edges('start')
    share(ssl, ss_send, ss_recv, 'get')
    grad_sq = jnp.sum(sum(ssl[e] for e in range(N_DEV)))
    grad_sq = grad_sq * (1.0 / (N_DEV * N_DEV))
    norm = jnp.sqrt(jnp.full((8, LANES), grad_sq, F32))
    scale = (1.0 / N_DEV) / jnp.maximum(1.0, norm)
    scale = jnp.concatenate([scale] * (BLK // 8), axis=0)
    for e, (has, size) in enumerate(((me < N_DEV - 1, UP), (me > 0, DOWN))):
        @pl.when(has)
        def _():
            rows = gbuf.at[pl.ds(0, size)]
            remote(rows, rows, edge_send.at[e], edge_recv.at[e], sib).wait_recv()
    g_loads('wait')
    first_t, past_t = pick(me, FIRST_TENSOR), pick(me, PAST_TENSOR)

    REST = SHARD_ROWS - FULL * BLK

    def over(first, past, whole, masked):
        top = min(past, FULL)

        def tensor(t):
            lo = pick(t, STARTS[:-1]) - SHARD_ROWS * me
            hi = pick(t, STARTS[1:]) - SHARD_ROWS * me
            head, tail = lo // BLK, hi // BLK
            from_b = jnp.maximum((lo + BLK - 1) // BLK, first)
            whole(t, from_b, jnp.maximum(from_b, jnp.minimum(tail, top)))

            def shared(b, size, at, g_at):
                ids = lax.broadcasted_iota(jnp.int32, (size, LANES), 0) + b * BLK
                masked(t, at, g_at, (ids >= lo) & (ids < hi))

            def end(e):
                b = jnp.where(e == 0, head, tail)
                cuts = jnp.where(e == 0, lo, hi) % BLK > 0
                again = (e > 0) & (head == tail) & (lo % BLK > 0)

                @pl.when(cuts & (b >= first) & (b < top) & jnp.logical_not(again))
                def _():
                    shared(b, BLK, *block_rows(b))
            each(0, 2, end)
            if past > FULL:
                shared(FULL, REST, pl.ds(FULL * BLK, REST), pl.ds(FULL * BLK + EDGE, REST))
        each(first_t, past_t, tensor)

    def block_rows(b):
        return tile(b, BLK), pl.ds(pl.multiple_of(b * BLK + EDGE, DOWN), BLK)

    def step_of(t, at, g_at):
        decay = jnp.where((t % 2 == 0) & (t != 4) & (t < 9), DECAY, 0.0).astype(F32)
        g, w, m, v = gbuf[g_at, :], wbuf[at, :], mbuf[at, :], vbuf[at, :]
        h = g * scale[:g.shape[0]]
        new_m = BETA_ONE * m + (1.0 - BETA_ONE) * h
        new_v = BETA_TWO * v + (1.0 - BETA_TWO) * (h * h)
        root = new_v * lax.rsqrt(jnp.maximum(new_v, jnp.finfo(F32).tiny))
        u = new_m / (root * (CORR_ONE / CORR_TWO ** 0.5) + EPSILON * CORR_ONE) + decay * w
        return (g, w, m, v), (u, w, new_m, new_v)

    def note(t, u_sq, w_sq):
        sums[me, pl.ds(t, 1), :] += jnp.sum(u_sq, axis=0, keepdims=True)
        sums[me, pl.ds(DOWN + t, 1), :] += jnp.sum(w_sq, axis=0, keepdims=True)

    def direction(t, first, past):
        def block(b, carry):
            at, g_at = block_rows(b)
            _, (u, w, new_m, new_v) = step_of(t, at, g_at)
            mbuf[at, :], vbuf[at, :], gbuf[g_at, :] = new_m, new_v, u
            return tuple(total + jnp.sum((x * x).reshape(-1, 8, LANES), axis=0) for total, x in zip(carry, (u, w)))
        zero = jnp.zeros((8, LANES), F32)
        note(t, *lax.fori_loop(first, past, block, (zero, zero)))

    def direction_shared(t, at, g_at, keep):
        (g, w, m, v), (u, _, new_m, new_v) = step_of(t, at, g_at)
        mbuf[at, :], vbuf[at, :] = jnp.where(keep, new_m, m), jnp.where(keep, new_v, v)
        gbuf[g_at, :] = jnp.where(keep, u, g)
        note(t, jnp.where(keep, u * u, 0.0), jnp.where(keep, w * w, 0.0))

    for k in range(LOADS):
        for c in loads[k]:
            c.wait()
        over(GB * k, GB * (k + 1) + (k == LOADS - 1), direction, direction_shared)
    share(sums, sum_send, sum_recv, 'start')
    share(sums, sum_send, sum_recv, 'get')
    total = jnp.sum(sum(sums[e] for e in range(N_DEV)), axis=1, keepdims=True)
    u_n, w_n = jnp.sqrt(total[:DOWN]), jnp.sqrt(total[DOWN:])
    both = (u_n > 0) & (w_n > 0)
    ratio = jnp.where(both, w_n / jnp.where(u_n > 0, u_n, 1.0), 1.0)
    rates[...] = jnp.broadcast_to(LEARN_RATE * ratio, rates.shape)

    def apply(t, first, past):
        rate = jnp.broadcast_to(rates[pl.ds(t, 1), :], (BLK, LANES))

        def block(b):
            at, g_at = block_rows(b)
            wbuf[at, :] = wbuf[at, :] - rate * gbuf[g_at, :]
        each(first, past, block)

    def apply_shared(t, at, g_at, keep):
        w = wbuf[at, :]
        wbuf[at, :] = jnp.where(keep, w - jnp.broadcast_to(rates[pl.ds(t, 1), :], w.shape) * gbuf[g_at, :], w)

    def cut(dev, j):
        return pl.ds(SHARD_ROWS * dev + CUTS[j], CUTS[j + 1] - CUTS[j])

    def twin(dev):
        return dev + other(2 * core)

    dg = N_DEV - 2 * (chip + 1) + core

    def own_part(j, e, sem, dev):
        return remote(wbuf.at[cut(0, j)], full.at[cut(me, j)], own_send.at[e, j], sem, dev)

    PB = SEG // BLK
    for j in range(PARTS):
        over(PB * j, PB * (j + 1) + (j == PARTS - 1), apply, apply_shared)
        for e, (sem, dev) in enumerate(((x_recv.at[j], xn), (y_recv.at[j], yn), (s_recv.at[0, j], sib))):
            own_part(j, e, sem, dev).start()
        local(wbuf.at[cut(0, j)], full.at[cut(me, j)], own_copy.at[j]).start()

    def wait_from(dev, j, sem):
        rows = full.at[cut(dev, j)]
        remote(rows, rows, cin_sem.at[0], sem, sib).wait_recv()

    def forward(dev, j, send_sem, recv_sem, to):
        rows = full.at[cut(dev, j)]
        remote(rows, rows, send_sem, recv_sem, to).start()

    def convert(*parts):
        todo = []
        for slot, (dev, j) in enumerate(parts):
            skip = DOWN if j == 0 else 0
            lo, size = pl.multiple_of(floor_of(dev) + skip + SEG * j, DOWN), SEG - skip
            cp = local(full.at[pl.ds(lo, size)], cin.at[slot, pl.ds(0, size)], cin_sem.at[slot])
            cp.start()
            todo.append((cp, slot, lo, size))
        for cp, slot, lo, size in todo:
            cp.wait()

            def body(b):
                params[pl.ds(pl.multiple_of(lo + b * DOWN, DOWN), DOWN), :] = cin[slot, tile(b, DOWN), :].astype(BF16)
            lax.fori_loop(0, size // DOWN, lambda b, c: (body(b), c)[1], 0, unroll=8)

    for j in range(PARTS):
        local(wbuf.at[cut(0, j)], full.at[cut(me, j)], own_copy.at[j]).wait()
        wait_from(sib, j, s_recv.at[0, j])
        convert((me, j), (sib, j))
        wait_from(xn, j, x_recv.at[j])
        forward(xn, j, sib_fwd.at[0, j], s_recv.at[1, j], sib)
        if j % 2 == 0:
            forward(xn, j, fwd_send.at[j], d_recv.at[j], yn)
        wait_from(yn, j, y_recv.at[j])
        forward(yn, j, sib_fwd.at[1, j], s_recv.at[2, j], sib)
        if j % 2 == 1:
            forward(yn, j, fwd_send.at[j], d_recv.at[j], xn)
        convert((xn, j), (yn, j))
        wait_from(twin(xn), j, s_recv.at[1, j])
        wait_from(twin(yn), j, s_recv.at[2, j])
        convert((twin(xn), j), (twin(yn), j))
    for j in range(0, PARTS, 2):
        both_parts = (j, j + 1)
        for e in both_parts:
            wait_from(dg, e, d_recv.at[e])
            forward(dg, e, sib_fwd.at[2, e], s_recv.at[3, e], sib)
        convert(*[(dg, e) for e in both_parts])
        for e in both_parts:
            wait_from(twin(dg), e, s_recv.at[3, e])
        if e == PARTS - 1:
            low = DOWN * (SHARD_ROWS * (N_DEV - 1) // DOWN) + SHARE
            pieces = ([(0, DOWN)] + [(DOWN * (SHARD_ROWS * s // DOWN) - DOWN, 2 * DOWN) for s in range(1, N_DEV)]
                      + [(low, TOTAL_ROWS - low)])
            ends = [local(full.at[pl.ds(lo, size)], cin.at[2, pl.ds(2 * DOWN * p, size)], cin_sem.at[2 + p])
                    for p, (lo, size) in enumerate(pieces)]
            for c in ends:
                c.start()
        convert(*[(twin(dg), e) for e in both_parts])
    for p, (c, (lo, size)) in enumerate(zip(ends, pieces)):
        c.wait()
        params[lo:lo + size, :] = cin[2, 2 * DOWN * p:2 * DOWN * p + size, :].astype(BF16)
    edges('sent')
    share(ssl, ss_send, ss_recv, 'sent')
    share(sums, sum_send, sum_recv, 'sent')
    for j in range(PARTS):
        sems = [fwd_send.at[j]] + [s.at[e, j] for s in (own_send, sib_fwd) for e in range(3)]
        for sem in sems:
            remote(wbuf.at[cut(0, j)], full.at[cut(me, j)], sem, x_recv.at[j], xn).wait_send()


def update_call(w, m, v, ga, gb, gc, vg, ss):
    shard = pltpu.VMEM((SHARD_ROWS, LANES), F32)
    outs = [shard, shard, shard, pltpu.VMEM((TOTAL_ROWS, LANES), BF16), shape(TOTAL_ROWS, LANES)]
    in_vmem = pl.BlockSpec(memory_space=pltpu.VMEM)
    return pl.pallas_call(
        update_kernel,
        out_shape=outs,
        in_specs=any_space(8),
        out_specs=[in_vmem] * 4 + any_space(1),
        scratch_shapes=[
            vmem(WIN, LANES), vmem(3, SEG, LANES),
            vmem(N_DEV, 8, LANES), vmem(N_DEV, 2 * DOWN, LANES), vmem(DOWN, LANES),
            *dmas((3, LOADS), 3, 2, 2, 7, N_DEV, 7, N_DEV, (3, PARTS), PARTS, PARTS, PARTS, PARTS, (4, PARTS),
                  PARTS, (3, PARTS), 11)],
        compiler_params=params_of(1, 14),
        name='lamb_gather',
    )(w, m, v, ga, gb, gc, vg, ss)


def cuts_of(rows):
    size, last = rows // CHUNKS // DOWN * DOWN, CHUNKS - 1
    return [(size * e, size) for e in range(last)] + [(size * last, rows - size * last)]


def write_kernel(*refs):
    *pairs, sem = refs
    half = len(pairs) // 2
    copies = [local(src.at[pl.ds(lo, size)], dst.at[pl.ds(lo, size)], sem.at[p, e])
              for p, (src, dst) in enumerate(zip(pairs[:half], pairs[half:]))
              for e, (lo, size) in enumerate(cuts_of(src.shape[0]))]
    for c in copies:
        c.start()
    for c in copies:
        c.wait()


def write_call(arrays):
    return pl.pallas_call(
        write_kernel,
        out_shape=[jax.ShapeDtypeStruct(a.shape, a.dtype) for a in arrays],
        in_specs=[pl.BlockSpec(memory_space=pltpu.VMEM)] * len(arrays),
        out_specs=any_space(len(arrays)),
        scratch_shapes=dmas((len(arrays), CHUNKS)),
        compiler_params=pltpu.CompilerParams(vmem_limit_bytes=MIB),
        name='write_out',
    )(*arrays)


def solution(mesh):
    def local_step(weights, moment_one, moment_two, *rest):
        *acts, ln_grad = rest
        ga, gb, gc, vg, ss, *_ = reduce_call(acts, ln_grad[0])
        rows = [a.reshape(SHARD_ROWS, LANES) for a in (weights, moment_one, moment_two)]
        out = update_call(*rows, *(g.reshape(-1, LANES) for g in (ga, gb, gc, vg)), ss)
        return tuple(a.reshape(-1) for a in write_call(out[:-1]))

    row_spec = P('dp', None)
    flat_spec = P('dp')
    in_specs = (flat_spec,) * 3 + (row_spec,) * 8 + (P('dp', None, None),)
    return jax.shard_map(local_step, mesh=mesh, in_specs=in_specs, out_specs=(flat_spec,) * 3 + (P(),), check_vma=False)
```

```python
import jax
import jax.numpy as jnp
from jax import lax
from jax.experimental import pallas as pl
from jax.experimental.pallas import tpu as pltpu
from jax.sharding import PartitionSpec as P

STEP = 10
LEARN_RATE = 0.5
BETA_ONE = 0.9
BETA_TWO = 0.999
EPSILON = 1e-6
DECAY = 0.01
CORR_ONE = 1.0 - BETA_ONE ** STEP
CORR_TWO = 1.0 - BETA_TWO ** STEP

D = 1024
N_DEV = 8
TOKENS = 4096
LANES = 128
SHARD_ROWS = 12301
TOTAL_ROWS = N_DEV * SHARD_ROWS
KC = 1024
CHUNKS = TOKENS // KC
BLOCK = 512
TASKS = 24
STEPS = TASKS * CHUNKS
UR = 128
UNITS = 12
HALF = UNITS // 2
F32 = jnp.float32
BF16 = jnp.bfloat16
MIB = 1024 * 1024

SIZES = [24576, 24, 8192, 8, 8, 8, 32768, 32, 32768, 8, 8, 8]
STARTS = [sum(SIZES[:pos]) for pos in range(len(SIZES) + 1)]
SHARE = UNITS * D
NOMINAL = [0, 12288, 24600, 36912, 49200, 61488, 73808, 86096]
FIRST_TENSOR = [max(t for t, at in enumerate(STARTS[:-1]) if at <= SHARD_ROWS * dev) for dev in range(N_DEV)]
PAST_TENSOR = [1 + max(t for t, at in enumerate(STARTS[:-1]) if at < SHARD_ROWS * (dev + 1)) for dev in range(N_DEV)]
EDGE = 48
WIN = 12416
UP, DOWN = 24, 16
FEW = [0, 1, 5, 6, 7, 11]
MANY = [0, 3, 3, 6, 9, 9]
WIDE = [0, 0, 1, 2, 0, 3]
B1, Y1, X1 = range(1, 4)


def pick(index, values):
    out = jnp.int32(values[-1])
    for pos in reversed(range(len(values) - 1)):
        out = jnp.where(index == pos, jnp.int32(values[pos]), out)
    return out


def tile(index, size):
    return pl.ds(pl.multiple_of(index * size, size), size)


def each(lo, hi, body):
    def step(pos, carry):
        body(pos)
        return carry
    lax.fori_loop(lo, hi, step, lo)


def other(bit):
    return 1 - bit


def device(y, x, core):
    return 4 * y + 2 * x + core


def neighbours():
    me = lax.axis_index('dp')
    chip, core = me // 2, me % 2
    x, y = chip % 2, chip // 2
    return me, chip, core, device(y, x, other(core)), device(y, other(x), core), device(other(y), x, core)


def local(src, dst, sem):
    return pltpu.make_async_copy(src, dst, sem)


def remote(src, dst, send_sem, recv_sem, dev):
    return pltpu.make_async_remote_copy(src_ref=src, dst_ref=dst, send_sem=send_sem, recv_sem=recv_sem,
                                        device_id=(dev,), device_id_type=pl.DeviceIdType.MESH)


def act_on(copy, act):
    if act == 'start':
        copy.start()
    elif act == 'sent':
        copy.wait_send()
    else:
        copy.wait()


def enter(devices):
    barrier = pltpu.get_barrier_semaphore()
    for dev in devices:
        pl.semaphore_signal(barrier, inc=1, device_id=(dev,), device_id_type=pl.DeviceIdType.MESH)
    pl.semaphore_wait(barrier, len(devices))


def task_of(n):
    six = HALF
    mid = n - six
    first, last = n < six, n >= 3 * six
    t = jnp.where(first, 0, jnp.where(last, X1, B1 + mid % 2))
    i = jnp.where(first, n, jnp.where(last, n - 3 * six, mid // 2))
    return t, i


def chip_of(t, chip):
    x, y = chip % 2, chip // 2
    return 2 * ((y + other(t % 2)) % 2) + (x + other(t // 2)) % 2


def is_square(i):
    return i % 3 == 1


def is_edge(q):
    return q % 3 == 0


def operands_of(q, i):
    square, odd, pair = is_square(i), i % 2, i // 2
    kind = jnp.where(is_edge(q), q, jnp.where(square, 2 * q - 1, 2))
    rb = jnp.where(q == 0, odd, jnp.where(is_edge(q), 2 + 3 * odd + pair, jnp.where(square, i // 4, q - 1)))
    cb = jnp.where(q == 0, pair, jnp.where(is_edge(q) | square, 0, pick(i, WIDE)))
    return kind, rb, cb


def units_of(q, i, par):
    square = is_square(i)
    few = q - 1 == par
    cnt = jnp.where(few, jnp.where(square, 4, 1), jnp.where(square, 0, 3))
    s0 = jnp.where(square | (par == 0), 0, 2 * q - 1)
    u0 = jnp.where(few, pick(i, FEW), pick(i, MANY))
    edge = is_edge(q)
    return (jnp.where(edge, 0, s0), jnp.where(edge, jnp.where(i % 2 == par, 4, 0), cnt),
            jnp.where(edge, 4 * (i // 2), u0))


def bias_of(q, i):
    square = is_square(i)
    need = jnp.where(q == 0, i % 2 > 0, jnp.where(q == 1, i == CHUNKS, jnp.where(q == 2, ~square, i == HALF - 1)))
    return need, jnp.where(q == 0, i // 2, jnp.where(q == 2, pick(i, WIDE), 0))


def reduce_kernel(xq, dyq, xp, dyp, xi, dyi, xo, dyo, ln,
                  g_a, g_b, g_c, v_out, ss_out, sib_land, x_land, y_land,
                  xbuf, dybuf, acc, part, x_fin, y_fin, stage, stage_r, flat, vec, vsum, vflat, vland, lnbuf, ss, ss_small,
                  x_sem, dy_sem, sib_send, sib_recv, out_send, x_recv, y_recv,
                  v_send, v_recv, st_sem, sr_sem, fl_sem, misc_sem):
    me, chip, core, sib, xn, yn = neighbours()
    kinds = ((xq, dyq), (xp, dyp), (xi, dyi), (xo, dyo))
    here = X1

    def arrived(ref, sem):
        remote(ref, ref, misc_sem.at[0], sem, sib).wait_recv()

    def issue(j):
        n, slot = j // CHUNKS, j % CHUNKS
        t, i = task_of(n)
        kind, rb, cb = operands_of(chip_of(t, chip), i)
        for which, (x_ref, dy_ref) in enumerate(kinds):
            @pl.when(kind == which)
            def _():
                local(x_ref.at[tile(slot, KC), tile(rb, BLOCK)], xbuf.at[slot], x_sem.at[slot]).start()
                local(dy_ref.at[tile(slot, KC), tile(cb, D)], dybuf.at[slot], dy_sem.at[slot]).start()

    for j in range(CHUNKS - 1):
        issue(jnp.int32(j))
    ln_copy = local(ln, lnbuf, misc_sem.at[0])
    ln_copy.start()
    enter((sib, xn, yn))
    ln_copy.wait()
    ss[...] = jnp.zeros_like(ss)
    vec[...] = jnp.zeros_like(vec)
    for t in range(4):
        for q in (1, 3):
            @pl.when(chip_of(jnp.int32(t), chip) == q)
            def _():
                vec[t, 1:3, :] = lnbuf[q - 1:q + 1, :]

    def own_units(n, par, body):
        t, i = task_of(n)
        s0, cnt, u0 = units_of(chip_of(t, chip), i, par)
        each(s0, s0 + cnt, lambda s: body(t, u0 + s - s0, s, t * UNITS + u0 + s - s0))

    def relayed(t, u, do):
        @pl.when((t == B1) & (u % 2 == 1))
        def _():
            do(y_land, y_recv)

        @pl.when((t == Y1) & (u % 2 == 0))
        def _():
            do(x_land, x_recv)

    def prefetch(n):
        def body(t, u, s, e):
            arrived(sib_land.at[e], sib_recv.at[e])
            local(sib_land.at[e], stage.at[s], st_sem.at[s]).start()

            def more(land, recv):
                arrived(land.at[u // 2], recv.at[u // 2])
                local(land.at[u // 2], stage_r.at[s], sr_sem.at[s]).start()
            relayed(t, u, more)
        own_units(n, core, body)

    def combine(n):
        def body(t, u, s, e):
            local(sib_land.at[e], stage.at[s], st_sem.at[s]).wait()
            part[e] = acc[n % 3, tile(s, UR), :] + stage[s]

            def more(land, recv):
                local(land.at[u // 2], stage_r.at[s], sr_sem.at[s]).wait()
                part[e] = part[e] + stage_r[s]
            relayed(t, u, more)
        own_units(n, core, body)
        t, i = task_of(n)

        @pl.when(i == HALF - 1)
        def _():
            remote(vec.at[t], vland.at[t], v_send.at[t], v_recv.at[t], sib).wait()
            vsum[t] = vec[t] + vland[t]

            @pl.when(t == Y1)
            def _():
                arrived(vland.at[CHUNKS], v_recv.at[CHUNKS])
                vsum[t] = vsum[t] + vland[4]

    def send_own(n):
        def body(t, u, s, e):
            def go(dst, recv, slot, dev):
                remote(part.at[e], dst, out_send.at[e], recv.at[slot], dev).start()

            @pl.when((t == 0) & (u % 2 == 0))
            def _():
                go(x_land.at[u // 2], x_recv, u // 2, xn)

            @pl.when((t == 0) & (u % 2 == 1))
            def _():
                go(y_land.at[u // 2], y_recv, u // 2, yn)

            @pl.when(t == B1)
            def _():
                go(x_fin.at[u], x_recv, HALF + u, xn)

            @pl.when(t == Y1)
            def _():
                go(y_fin.at[u], y_recv, HALF + u, yn)
        own_units(n, core, body)
        t, i = task_of(n)
        for way, dev in enumerate((xn, xn, yn)):
            @pl.when((i == HALF - 1) & (t == way))
            def _():
                remote(vsum.at[t], vland.at[CHUNKS + way], v_send.at[CHUNKS + way], v_recv.at[CHUNKS + way], dev).start()

    def sib_units(n, act):
        def body(t, u, s, e):
            act_on(remote(acc.at[n % 3, tile(s, UR)], sib_land.at[e], sib_send.at[e], sib_recv.at[e], sib), act)
        own_units(n, other(core), body)

    def task(n):
        t, i = task_of(n)
        need, row = bias_of(chip_of(t, chip), i)
        a = n % 3

        @pl.when(n >= 3)
        def _():
            sib_units(n - 3, 'sent')

        def chunk(slot):
            j = n * CHUNKS + slot

            @pl.when(j + CHUNKS - 1 < STEPS)
            def _():
                issue(j + CHUNKS - 1)
            local(xq.at[tile(0, KC), tile(0, BLOCK)], xbuf.at[slot], x_sem.at[slot]).wait()
            local(dyq.at[tile(0, KC), tile(0, D)], dybuf.at[slot], dy_sem.at[slot]).wait()

            def dot():
                return lax.dot_general(xbuf[slot], dybuf[slot], (((0,), (0,)), ((), ())),
                                       preferred_element_type=F32)

            @pl.when(slot == 0)
            def _():
                acc[a] = dot()

            @pl.when(slot > 0)
            def _():
                acc[a] += dot()

            @pl.when(need)
            def _():
                def add(r, total):
                    block = dybuf[slot, tile(r, LANES), :].astype(F32)
                    return total + jnp.sum(block.reshape(-1, 8, D), axis=0)
                total = lax.fori_loop(0, KC // LANES, add, jnp.zeros_like(ss))
                vec[t, pl.ds(row, 1), :] += jnp.sum(total, axis=0, keepdims=True)

            @pl.when((slot == 0) & (n > 0))
            def _():
                prefetch(n - 1)

            @pl.when((slot == 1) & (n > 0))
            def _():
                combine(n - 1)
                send_own(n - 1)
        each(0, CHUNKS, chunk)
        sib_units(n, 'start')

        @pl.when(i == HALF - 1)
        def _():
            remote(vec.at[t], vland.at[t], v_send.at[t], v_recv.at[t], sib).start()

    each(0, TASKS, task)
    prefetch(jnp.int32(TASKS - 1))
    combine(jnp.int32(TASKS - 1))
    each(TASKS - 3, TASKS, lambda n: sib_units(n, 'sent'))

    few = chip - 1 == core
    mid = jnp.logical_not(is_edge(chip))
    past = chip == 2

    def write_unit(u, slot):
        def go(dst):
            local(flat.at[slot], dst, fl_sem.at[slot]).start()

        @pl.when(chip == 0)
        def _():
            go(g_a.at[tile(u % 4, UR), tile(u // 4, 8)])

        @pl.when(chip == 3)
        def _():
            go(g_c.at[tile(u, UR)])
        square = jnp.where((u >= FEW[1]) & (u < FEW[2]), u - FEW[1],
                           jnp.where((u >= FEW[4]) & (u < FEW[-1]), u - 3, -1))
        col = jnp.where(u < FEW[2], 0, jnp.where(u < FEW[4], u - 4, 3))

        @pl.when(mid & few & (square < 0))
        def _():
            go(g_b.at[tile(jnp.where(past, 0, 2), UR), tile(col, 8)])

        @pl.when(mid & few & (square >= 0))
        def _():
            go(g_c.at[tile(jnp.where(past, 4, 0) + square, UR)])

        @pl.when(mid & jnp.logical_not(few))
        def _():
            go(g_b.at[tile(u % 3, UR), tile(u // 3, 8)])

    def written(slot):
        local(flat.at[slot], g_c.at[tile(0, UR)], fl_sem.at[slot]).wait()

    def finish(u):
        slot = u % 2

        @pl.when(u >= 2)
        def _():
            written(slot)
        arrived(x_fin.at[u], x_recv.at[HALF + u])
        arrived(y_fin.at[u], y_recv.at[HALF + u])

        def add(r, total):
            rows = tile(r, 16)
            val = part[here * UNITS + u, rows, :] + x_fin[u, rows, :] + y_fin[u, rows, :]
            flat[slot, rows] = val.reshape(16, 8, LANES)
            return total + val[0:8] * val[0:8] + val[8:16] * val[8:16]
        ss[...] += lax.fori_loop(0, UR // 16, add, jnp.zeros_like(ss))
        write_unit(u, slot)

    each(0, UNITS, finish)
    arrived(vland.at[5], v_recv.at[5])
    arrived(vland.at[6], v_recv.at[6])
    val = vsum[here] + vland[5] + vland[6]
    vflat[...] = val.reshape(8, 8, LANES)
    total = ss[...] + jnp.where(core == 0, 1.0, 0.0).astype(F32) * (val * val)
    ss_small[...] = sum(total[:, LANES * c:LANES * (c + 1)] for c in range(8))
    tail = [local(vflat, v_out, misc_sem.at[0]), local(ss_small, ss_out, misc_sem.at[1])]
    for c in tail:
        c.start()
    written(0)
    written(1)
    for c in tail:
        c.wait()
    each(0, here * UNITS, lambda e: remote(part.at[e], x_land.at[0], out_send.at[e], x_recv.at[0], xn).wait_send())
    for way in range(3):
        remote(vsum.at[way], vland.at[CHUNKS], v_send.at[CHUNKS + way], v_recv.at[CHUNKS], xn).wait_send()


def shape(*dims, dtype=F32):
    return jax.ShapeDtypeStruct(dims, dtype)


def vmem(*dims, dtype=F32):
    return pltpu.VMEM(dims, dtype)


def dmas(*counts):
    return [pltpu.SemaphoreType.DMA(c if isinstance(c, tuple) else (c,)) for c in counts]


def any_space(count):
    return [pl.BlockSpec(memory_space=pltpu.HBM)] * count


def params_of(collective_id, mib):
    return pltpu.CompilerParams(collective_id=collective_id, has_side_effects=True, vmem_limit_bytes=mib * MIB)


def reduce_call(acts, ln_rows):
    lands = UNITS + HALF
    outs = [shape(512, 24, LANES), shape(384, 32, LANES), shape(1536, 8, LANES), shape(8, 8, LANES), shape(8, LANES),
            shape(CHUNKS * UNITS, UR, D), shape(HALF, UR, D), shape(HALF, UR, D)]
    return pl.pallas_call(
        reduce_kernel,
        out_shape=outs,
        in_specs=any_space(len(acts) + 1),
        out_specs=any_space(len(outs)),
        scratch_shapes=[
            vmem(CHUNKS, KC, BLOCK, dtype=BF16), vmem(CHUNKS, KC, D, dtype=BF16), vmem(3, BLOCK, D),
            vmem(CHUNKS * UNITS, UR, D), vmem(UNITS, UR, D), vmem(UNITS, UR, D), vmem(CHUNKS, UR, D), vmem(CHUNKS, UR, D), vmem(2, UR, 8, LANES),
            vmem(CHUNKS, 8, D), vmem(CHUNKS, 8, D), vmem(8, 8, LANES), vmem(7, 8, D), vmem(CHUNKS, D), vmem(8, D), vmem(8, LANES),
            *dmas(CHUNKS, CHUNKS, CHUNKS * UNITS, CHUNKS * UNITS, X1 * UNITS, lands, lands, 7, 7, CHUNKS, CHUNKS, 2, 2)],
        compiler_params=params_of(0, 63),
        name='grad_reduce',
    )(*acts, ln_rows)


BLK = 128
PART_BLOCKS = [7] * UNITS + [4, 4, 2, 2]
PARTS = len(PART_BLOCKS)
SEG = max(PART_BLOCKS) * BLK
ENDS = [BLK * sum(PART_BLOCKS[:j]) for j in range(PARTS + 1)]
CUTS = ENDS[:-1] + [SHARD_ROWS]
FULL = SHARE // BLK
LOADS = 4
LOAD = SHARE // LOADS
GB = FULL // LOADS


def update_kernel(w_in, m_in, v_in, ga, gb, gc, vg, ss_in,
                  wbuf, mbuf, vbuf, params, full,
                  gbuf, cin, ssl, sums, rates,
                  load_sem, g_sem, edge_send, edge_recv, ss_send, ss_recv, sum_send, sum_recv,
                  own_send, own_copy, x_recv, y_recv, d_recv, s_recv, fwd_send, sib_fwd, cin_sem):
    me, chip, core, sib, xn, yn = neighbours()

    def floor_of(dev):
        return DOWN * (SHARD_ROWS * dev // DOWN)

    def in_window(dev, row):
        return row - SHARD_ROWS * dev + EDGE

    def load_rows(k):
        return pl.ds(LOAD * k, LOAD if k < LOADS - 1 else SHARD_ROWS - LOAD * k)

    loads = [[local(src.at[load_rows(k)], dst.at[load_rows(k)], load_sem.at[e, k])
              for e, (src, dst) in enumerate(((w_in, wbuf), (m_in, mbuf), (v_in, vbuf)))] for k in range(LOADS)]

    def when_in(lo, hi, do, *args):
        @pl.when((me >= lo) & (me <= hi))
        def _():
            do(*args)

    def g_loads(act):
        start = in_window(me, pick(me, NOMINAL))

        def go(*copies):
            for e, (src, lo, size, at) in enumerate(copies):
                act_on(local(src.at[pl.ds(lo, size)], gbuf.at[pl.ds(start + at, size)], g_sem.at[e]), act)
        two, one = SIZES[2], SHARE - SIZES[2]
        tail = (vg, 0, UP, SHARE)
        when_in(0, 0, go, (ga, 0, SHARE, 0))
        when_in(1, 1, go, (ga, 0, SHARE, 0), tail)
        when_in(2, 2, go, (gc, 0, two, 0), (vg, 0, UP, two), (gb, two, one, two + UP))
        when_in(3, 4, go, (gb, 0, SHARE, 0))
        when_in(5, 5, go, (gb, 0, one, 0), (vg, 0, SIZES[7], one), (gc, one, two, one + SIZES[7]))
        when_in(6, 6, go, (gc, 0, SHARE, 0))
        when_in(7, 7, go, (gc, 0, SHARE, 0), tail)

    ss_copy = local(ss_in, ssl.at[me], cin_sem.at[0])
    ss_copy.start()
    g_loads('start')
    for group in loads:
        for c in group:
            c.start()
    sums[...] = jnp.zeros_like(sums)
    others = [lax.rem(me + e, N_DEV) for e in range(1, N_DEV)]
    enter(others)
    ss_copy.wait()

    def share(buf, send, recv, act):
        for e, dev in enumerate(others):
            if act == 'get':
                remote(buf.at[dev], buf.at[dev], send.at[e], recv.at[dev], dev).wait_recv()
            else:
                act_on(remote(buf.at[me], buf.at[me], send.at[e], recv.at[me], dev), act)

    share(ssl, ss_send, ss_recv, 'start')

    def edges(act):
        def go(src, lo, size, dev, row, e):
            act_on(remote(src.at[pl.ds(lo, size)], gbuf.at[pl.ds(in_window(dev, row), size)],
                          edge_send.at[e], edge_recv.at[e], dev), act)

        def up(src):
            go(src, 0, UP, me - 1, pick(me, NOMINAL), 0)

        def down(src):
            go(src, SHARE - DOWN, DOWN, me + 1, pick(me + 1, NOMINAL) - DOWN, 1)
        when_in(1, 1, up, ga)
        when_in(2, 2, up, gc)
        when_in(3, 5, up, gb)
        when_in(6, 7, up, gc)
        when_in(0, 1, down, ga)
        when_in(2, 4, down, gb)
        when_in(5, 6, down, gc)

    edges('start')
    share(ssl, ss_send, ss_recv, 'get')
    grad_sq = jnp.sum(sum(ssl[e] for e in range(N_DEV)))
    grad_sq = grad_sq * (1.0 / (N_DEV * N_DEV))
    norm = jnp.sqrt(jnp.full((8, LANES), grad_sq, F32))
    scale = (1.0 / N_DEV) / jnp.maximum(1.0, norm)
    scale = jnp.concatenate([scale] * (BLK // 8), axis=0)
    for e, (has, size) in enumerate(((me < N_DEV - 1, UP), (me > 0, DOWN))):
        @pl.when(has)
        def _():
            rows = gbuf.at[pl.ds(0, size)]
            remote(rows, rows, edge_send.at[e], edge_recv.at[e], sib).wait_recv()
    g_loads('wait')
    first_t, past_t = pick(me, FIRST_TENSOR), pick(me, PAST_TENSOR)

    REST = SHARD_ROWS - FULL * BLK

    def over(first, past, whole, masked):
        top = min(past, FULL)

        def tensor(t):
            lo = pick(t, STARTS[:-1]) - SHARD_ROWS * me
            hi = pick(t, STARTS[1:]) - SHARD_ROWS * me
            head, tail = lo // BLK, hi // BLK
            from_b = jnp.maximum((lo + BLK - 1) // BLK, first)
            whole(t, from_b, jnp.maximum(from_b, jnp.minimum(tail, top)))

            def shared(b, size, at, g_at):
                ids = lax.broadcasted_iota(jnp.int32, (size, LANES), 0) + b * BLK
                masked(t, at, g_at, (ids >= lo) & (ids < hi))

            def end(e):
                b = jnp.where(e == 0, head, tail)
                cuts = jnp.where(e == 0, lo, hi) % BLK > 0
                again = (e > 0) & (head == tail) & (lo % BLK > 0)

                @pl.when(cuts & (b >= first) & (b < top) & jnp.logical_not(again))
                def _():
                    shared(b, BLK, *block_rows(b))
            each(0, 2, end)
            if past > FULL:
                shared(FULL, REST, pl.ds(FULL * BLK, REST), pl.ds(FULL * BLK + EDGE, REST))
        each(first_t, past_t, tensor)

    def block_rows(b):
        return tile(b, BLK), pl.ds(pl.multiple_of(b * BLK + EDGE, DOWN), BLK)

    def step_of(t, at, g_at):
        decay = jnp.where((t % 2 == 0) & (t != 4) & (t < 9), DECAY, 0.0).astype(F32)
        g, w, m, v = gbuf[g_at, :], wbuf[at, :], mbuf[at, :], vbuf[at, :]
        h = g * scale[:g.shape[0]]
        new_m = BETA_ONE * m + (1.0 - BETA_ONE) * h
        new_v = BETA_TWO * v + (1.0 - BETA_TWO) * (h * h)
        root = new_v * lax.rsqrt(jnp.maximum(new_v, jnp.finfo(F32).tiny))
        u = new_m / (root * (CORR_ONE / CORR_TWO ** 0.5) + EPSILON * CORR_ONE) + decay * w
        return (g, w, m, v), (u, w, new_m, new_v)

    def note(t, u_sq, w_sq):
        sums[me, pl.ds(t, 1), :] += jnp.sum(u_sq, axis=0, keepdims=True)
        sums[me, pl.ds(DOWN + t, 1), :] += jnp.sum(w_sq, axis=0, keepdims=True)

    def direction(t, first, past):
        def block(b, carry):
            at, g_at = block_rows(b)
            _, (u, w, new_m, new_v) = step_of(t, at, g_at)
            mbuf[at, :], vbuf[at, :], gbuf[g_at, :] = new_m, new_v, u
            return tuple(total + jnp.sum((x * x).reshape(-1, 8, LANES), axis=0) for total, x in zip(carry, (u, w)))
        zero = jnp.zeros((8, LANES), F32)
        note(t, *lax.fori_loop(first, past, block, (zero, zero)))

    def direction_shared(t, at, g_at, keep):
        (g, w, m, v), (u, _, new_m, new_v) = step_of(t, at, g_at)
        mbuf[at, :], vbuf[at, :] = jnp.where(keep, new_m, m), jnp.where(keep, new_v, v)
        gbuf[g_at, :] = jnp.where(keep, u, g)
        note(t, jnp.where(keep, u * u, 0.0), jnp.where(keep, w * w, 0.0))

    for k in range(LOADS):
        for c in loads[k]:
            c.wait()
        over(GB * k, GB * (k + 1) + (k == LOADS - 1), direction, direction_shared)
    share(sums, sum_send, sum_recv, 'start')
    share(sums, sum_send, sum_recv, 'get')
    total = jnp.sum(sum(sums[e] for e in range(N_DEV)), axis=1, keepdims=True)
    u_n, w_n = jnp.sqrt(total[:DOWN]), jnp.sqrt(total[DOWN:])
    both = (u_n > 0) & (w_n > 0)
    ratio = jnp.where(both, w_n / jnp.where(u_n > 0, u_n, 1.0), 1.0)
    rates[...] = jnp.broadcast_to(LEARN_RATE * ratio, rates.shape)

    def apply(t, first, past):
        rate = jnp.broadcast_to(rates[pl.ds(t, 1), :], (BLK, LANES))

        def block(b):
            at, g_at = block_rows(b)
            wbuf[at, :] = wbuf[at, :] - rate * gbuf[g_at, :]
        each(first, past, block)

    def apply_shared(t, at, g_at, keep):
        w = wbuf[at, :]
        wbuf[at, :] = jnp.where(keep, w - jnp.broadcast_to(rates[pl.ds(t, 1), :], w.shape) * gbuf[g_at, :], w)

    def cut(dev, j):
        return pl.ds(SHARD_ROWS * dev + CUTS[j], CUTS[j + 1] - CUTS[j])

    def twin(dev):
        return dev + other(2 * core)

    dg = N_DEV - 2 * (chip + 1) + core

    def own_part(j, e, sem, dev):
        return remote(wbuf.at[cut(0, j)], full.at[cut(me, j)], own_send.at[e, j], sem, dev)

    for j in range(PARTS):
        over(ENDS[j] // BLK, ENDS[j + 1] // BLK + (j == PARTS - 1), apply, apply_shared)
        for e, (sem, dev) in enumerate(((x_recv.at[j], xn), (y_recv.at[j], yn), (s_recv.at[0, j], sib))):
            own_part(j, e, sem, dev).start()
        local(wbuf.at[cut(0, j)], full.at[cut(me, j)], own_copy.at[j]).start()

    def wait_from(dev, j, sem):
        rows = full.at[cut(dev, j)]
        remote(rows, rows, cin_sem.at[0], sem, sib).wait_recv()

    def forward(dev, j, send_sem, recv_sem, to):
        rows = full.at[cut(dev, j)]
        remote(rows, rows, send_sem, recv_sem, to).start()

    def convert(*parts):
        todo = []
        for slot, (dev, j) in enumerate(parts):
            skip = DOWN if j == 0 else 0
            lo, size = pl.multiple_of(floor_of(dev) + skip + ENDS[j], DOWN), ENDS[j + 1] - ENDS[j] - skip
            cp = local(full.at[pl.ds(lo, size)], cin.at[slot, pl.ds(0, size)], cin_sem.at[slot])
            cp.start()
            todo.append((cp, slot, lo, size))
        for cp, slot, lo, size in todo:
            cp.wait()

            def body(b):
                params[pl.ds(pl.multiple_of(lo + b * DOWN, DOWN), DOWN), :] = cin[slot, tile(b, DOWN), :].astype(BF16)
            lax.fori_loop(0, size // DOWN, lambda b, c: (body(b), c)[1], 0, unroll=8)

    for j in range(PARTS):
        local(wbuf.at[cut(0, j)], full.at[cut(me, j)], own_copy.at[j]).wait()
        wait_from(sib, j, s_recv.at[0, j])
        convert((me, j), (sib, j))
        wait_from(xn, j, x_recv.at[j])
        forward(xn, j, sib_fwd.at[0, j], s_recv.at[1, j], sib)
        if j % 2 == 0:
            forward(xn, j, fwd_send.at[j], d_recv.at[j], yn)
        wait_from(yn, j, y_recv.at[j])
        forward(yn, j, sib_fwd.at[1, j], s_recv.at[2, j], sib)
        if j % 2 == 1:
            forward(yn, j, fwd_send.at[j], d_recv.at[j], xn)
        convert((xn, j), (yn, j))
        wait_from(twin(xn), j, s_recv.at[1, j])
        wait_from(twin(yn), j, s_recv.at[2, j])
        convert((twin(xn), j), (twin(yn), j))
    for j in range(0, PARTS, 2):
        both_parts = (j, j + 1)
        for e in both_parts:
            wait_from(dg, e, d_recv.at[e])
            forward(dg, e, sib_fwd.at[2, e], s_recv.at[3, e], sib)
        convert(*[(dg, e) for e in both_parts])
        for e in both_parts:
            wait_from(twin(dg), e, s_recv.at[3, e])
        if e == PARTS - 1:
            low = DOWN * (SHARD_ROWS * (N_DEV - 1) // DOWN) + SHARE
            pieces = ([(0, DOWN)] + [(DOWN * (SHARD_ROWS * s // DOWN) - DOWN, 2 * DOWN) for s in range(1, N_DEV)]
                      + [(low, TOTAL_ROWS - low)])
            ends = [local(full.at[pl.ds(lo, size)], cin.at[2, pl.ds(2 * DOWN * p, size)], cin_sem.at[2 + p])
                    for p, (lo, size) in enumerate(pieces)]
            for c in ends:
                c.start()
        convert(*[(twin(dg), e) for e in both_parts])
    for p, (c, (lo, size)) in enumerate(zip(ends, pieces)):
        c.wait()
        params[lo:lo + size, :] = cin[2, 2 * DOWN * p:2 * DOWN * p + size, :].astype(BF16)
    edges('sent')
    share(ssl, ss_send, ss_recv, 'sent')
    share(sums, sum_send, sum_recv, 'sent')
    for j in range(PARTS):
        sems = [fwd_send.at[j]] + [s.at[e, j] for s in (own_send, sib_fwd) for e in range(3)]
        for sem in sems:
            remote(wbuf.at[cut(0, j)], full.at[cut(me, j)], sem, x_recv.at[j], xn).wait_send()


def update_call(w, m, v, ga, gb, gc, vg, ss):
    shard = pltpu.VMEM((SHARD_ROWS, LANES), F32)
    outs = [shard, shard, shard, pltpu.VMEM((TOTAL_ROWS, LANES), BF16), shape(TOTAL_ROWS, LANES)]
    in_vmem = pl.BlockSpec(memory_space=pltpu.VMEM)
    return pl.pallas_call(
        update_kernel,
        out_shape=outs,
        in_specs=any_space(8),
        out_specs=[in_vmem] * 4 + any_space(1),
        scratch_shapes=[
            vmem(WIN, LANES), vmem(3, SEG, LANES),
            vmem(N_DEV, 8, LANES), vmem(N_DEV, 2 * DOWN, LANES), vmem(DOWN, LANES),
            *dmas((3, LOADS), 3, 2, 2, 7, N_DEV, 7, N_DEV, (3, PARTS), PARTS, PARTS, PARTS, PARTS, (4, PARTS),
                  PARTS, (3, PARTS), 11)],
        compiler_params=params_of(1, 14),
        name='lamb_gather',
    )(w, m, v, ga, gb, gc, vg, ss)


def cuts_of(rows):
    size, last = rows // CHUNKS // DOWN * DOWN, CHUNKS - 1
    return [(size * e, size) for e in range(last)] + [(size * last, rows - size * last)]


def write_kernel(*refs):
    *pairs, sem = refs
    half = len(pairs) // 2
    copies = [local(src.at[pl.ds(lo, size)], dst.at[pl.ds(lo, size)], sem.at[p, e])
              for p, (src, dst) in enumerate(zip(pairs[:half], pairs[half:]))
              for e, (lo, size) in enumerate(cuts_of(src.shape[0]))]
    for c in copies:
        c.start()
    for c in copies:
        c.wait()


def write_call(arrays):
    return pl.pallas_call(
        write_kernel,
        out_shape=[jax.ShapeDtypeStruct(a.shape, a.dtype) for a in arrays],
        in_specs=[pl.BlockSpec(memory_space=pltpu.VMEM)] * len(arrays),
        out_specs=any_space(len(arrays)),
        scratch_shapes=dmas((len(arrays), CHUNKS)),
        compiler_params=pltpu.CompilerParams(vmem_limit_bytes=MIB),
        name='write_out',
    )(*arrays)


def solution(mesh):
    def local_step(weights, moment_one, moment_two, *rest):
        *acts, ln_grad = rest
        ga, gb, gc, vg, ss, *_ = reduce_call(acts, ln_grad[0])
        rows = [a.reshape(SHARD_ROWS, LANES) for a in (weights, moment_one, moment_two)]
        out = update_call(*rows, *(g.reshape(-1, LANES) for g in (ga, gb, gc, vg)), ss)
        return tuple(a.reshape(-1) for a in write_call(out[:-1]))

    row_spec = P('dp', None)
    flat_spec = P('dp')
    in_specs = (flat_spec,) * 3 + (row_spec,) * 8 + (P('dp', None, None),)
    return jax.shard_map(local_step, mesh=mesh, in_specs=in_specs, out_specs=(flat_spec,) * 3 + (P(),), check_vma=False)
```

```python
import jax
import jax.numpy as jnp
from jax import lax
from jax.experimental import pallas as pl
from jax.experimental.pallas import tpu as pltpu
from jax.sharding import PartitionSpec as P

STEP = 10
LEARN_RATE = 0.5
BETA_ONE = 0.9
BETA_TWO = 0.999
EPSILON = 1e-6
DECAY = 0.01
CORR_ONE = 1.0 - BETA_ONE ** STEP
CORR_TWO = 1.0 - BETA_TWO ** STEP

D = 1024
N_DEV = 8
TOKENS = 4096
LANES = 128
SHARD_ROWS = 12301
TOTAL_ROWS = N_DEV * SHARD_ROWS
KC = 1024
CHUNKS = TOKENS // KC
BLOCK = 512
TASKS = 24
STEPS = TASKS * CHUNKS
UR = 128
UNITS = 12
HALF = UNITS // 2
F32 = jnp.float32
BF16 = jnp.bfloat16
MIB = 1024 * 1024

SIZES = [24576, 24, 8192, 8, 8, 8, 32768, 32, 32768, 8, 8, 8]
STARTS = [sum(SIZES[:pos]) for pos in range(len(SIZES) + 1)]
SHARE = UNITS * D
NOMINAL = [0, 12288, 24600, 36912, 49200, 61488, 73808, 86096]
FIRST_TENSOR = [max(t for t, at in enumerate(STARTS[:-1]) if at <= SHARD_ROWS * dev) for dev in range(N_DEV)]
PAST_TENSOR = [1 + max(t for t, at in enumerate(STARTS[:-1]) if at < SHARD_ROWS * (dev + 1)) for dev in range(N_DEV)]
EDGE = 48
WIN = 12416
UP, DOWN = 24, 16
FEW = [0, 1, 5, 6, 7, 11]
MANY = [0, 3, 3, 6, 9, 9]
WIDE = [0, 0, 1, 2, 0, 3]
B1, Y1, X1 = range(1, 4)


def pick(index, values):
    out = jnp.int32(values[-1])
    for pos in reversed(range(len(values) - 1)):
        out = jnp.where(index == pos, jnp.int32(values[pos]), out)
    return out


def tile(index, size):
    return pl.ds(pl.multiple_of(index * size, size), size)


def each(lo, hi, body):
    def step(pos, carry):
        body(pos)
        return carry
    lax.fori_loop(lo, hi, step, lo)


def other(bit):
    return 1 - bit


def device(y, x, core):
    return 4 * y + 2 * x + core


def neighbours():
    me = lax.axis_index('dp')
    chip, core = me // 2, me % 2
    x, y = chip % 2, chip // 2
    return me, chip, core, device(y, x, other(core)), device(y, other(x), core), device(other(y), x, core)


def local(src, dst, sem):
    return pltpu.make_async_copy(src, dst, sem)


def remote(src, dst, send_sem, recv_sem, dev):
    return pltpu.make_async_remote_copy(src_ref=src, dst_ref=dst, send_sem=send_sem, recv_sem=recv_sem,
                                        device_id=(dev,), device_id_type=pl.DeviceIdType.MESH)


def act_on(copy, act):
    if act == 'start':
        copy.start()
    elif act == 'sent':
        copy.wait_send()
    else:
        copy.wait()


def enter(devices):
    barrier = pltpu.get_barrier_semaphore()
    for dev in devices:
        pl.semaphore_signal(barrier, inc=1, device_id=(dev,), device_id_type=pl.DeviceIdType.MESH)
    pl.semaphore_wait(barrier, len(devices))


def task_of(n):
    six = HALF
    mid = n - six
    first, last = n < six, n >= 3 * six
    t = jnp.where(first, 0, jnp.where(last, X1, B1 + mid % 2))
    i = jnp.where(first, n, jnp.where(last, n - 3 * six, mid // 2))
    return t, i


def chip_of(t, chip):
    x, y = chip % 2, chip // 2
    return 2 * ((y + other(t % 2)) % 2) + (x + other(t // 2)) % 2


def is_square(i):
    return i % 3 == 1


def is_edge(q):
    return q % 3 == 0


def operands_of(q, i):
    square, odd, pair = is_square(i), i % 2, i // 2
    kind = jnp.where(is_edge(q), q, jnp.where(square, 2 * q - 1, 2))
    rb = jnp.where(q == 0, odd, jnp.where(is_edge(q), 2 + 3 * odd + pair, jnp.where(square, i // 4, q - 1)))
    cb = jnp.where(q == 0, pair, jnp.where(is_edge(q) | square, 0, pick(i, WIDE)))
    return kind, rb, cb


def units_of(q, i, par):
    square = is_square(i)
    few = q - 1 == par
    cnt = jnp.where(few, jnp.where(square, 4, 1), jnp.where(square, 0, 3))
    s0 = jnp.where(square | (par == 0), 0, 2 * q - 1)
    u0 = jnp.where(few, pick(i, FEW), pick(i, MANY))
    edge = is_edge(q)
    return (jnp.where(edge, 0, s0), jnp.where(edge, jnp.where(i % 2 == par, 4, 0), cnt),
            jnp.where(edge, 4 * (i // 2), u0))


def bias_of(q, i):
    square = is_square(i)
    need = jnp.where(q == 0, i % 2 > 0, jnp.where(q == 1, i == CHUNKS, jnp.where(q == 2, ~square, i == HALF - 1)))
    return need, jnp.where(q == 0, i // 2, jnp.where(q == 2, pick(i, WIDE), 0))


def reduce_kernel(xq, dyq, xp, dyp, xi, dyi, xo, dyo, ln,
                  g_a, g_b, g_c, v_out, ss_out, sib_land, relay,
                  xbuf, dybuf, acc, part, x_fin, y_fin, stage, stage_r, flat, vec, vsum, vflat, vland, lnbuf, ss, ss_small,
                  x_sem, dy_sem, sib_send, sib_recv, out_send, relay_recv, x_recv, y_recv,
                  v_send, v_recv, st_sem, sr_sem, fl_sem, misc_sem):
    me, chip, core, sib, xn, yn = neighbours()
    kinds = ((xq, dyq), (xp, dyp), (xi, dyi), (xo, dyo))
    here = X1

    def arrived(ref, sem):
        remote(ref, ref, misc_sem.at[0], sem, sib).wait_recv()

    def issue(j):
        n, slot = j // CHUNKS, j % CHUNKS
        t, i = task_of(n)
        kind, rb, cb = operands_of(chip_of(t, chip), i)
        for which, (x_ref, dy_ref) in enumerate(kinds):
            @pl.when(kind == which)
            def _():
                local(x_ref.at[tile(slot, KC), tile(rb, BLOCK)], xbuf.at[slot], x_sem.at[slot]).start()
                local(dy_ref.at[tile(slot, KC), tile(cb, D)], dybuf.at[slot], dy_sem.at[slot]).start()

    for j in range(CHUNKS - 1):
        issue(jnp.int32(j))
    ln_copy = local(ln, lnbuf, misc_sem.at[0])
    ln_copy.start()
    x_base, y_base = xn - core, yn - core
    enter((sib, xn, yn, x_base + other(core), y_base + other(core)))
    ln_copy.wait()
    ss[...] = jnp.zeros_like(ss)
    vec[...] = jnp.zeros_like(vec)
    for t in range(4):
        for q in (1, 3):
            @pl.when(chip_of(jnp.int32(t), chip) == q)
            def _():
                vec[t, 1:3, :] = lnbuf[q - 1:q + 1, :]

    def own_units(n, who, body):
        t, i = task_of(n)
        (s_a, _, u_a), (s_b, count_b, u_b) = [units_of(chip_of(t, chip), i, par) for par in range(2)]

        def sub_block(s):
            second = (s >= s_b) & (s < s_b + count_b)
            par = jnp.where(second, 1, 0)
            u = s + jnp.where(second, u_b - s_b, u_a - s_a)
            pair = 2 * (u // 2) + par
            owner = jnp.where(t == 0, u % 2, jnp.where(t == here, par, t - 1))
            e = jnp.where(t == 0, pair, jnp.where(t == here, here * UNITS + u, UNITS + 2 * u + par))

            @pl.when(owner == who)
            def _():
                body(t, par, u, s, e)
        each(0, CHUNKS, sub_block)

    def relayed(t, par, u, do):
        @pl.when(((t == B1) & (u % 2 == 1)) | ((t == Y1) & (u % 2 == 0)))
        def _():
            do(2 * (u // 2) + par)

    def prefetch(n):
        def body(t, par, u, s, e):
            arrived(sib_land.at[e], sib_recv.at[e])
            local(sib_land.at[e], stage.at[s], st_sem.at[s]).start()

            def more(at):
                arrived(relay.at[at], relay_recv.at[at])
                local(relay.at[at], stage_r.at[s], sr_sem.at[s]).start()
            relayed(t, par, u, more)
        own_units(n, core, body)

    def combine(n):
        def body(t, par, u, s, e):
            local(sib_land.at[e], stage.at[s], st_sem.at[s]).wait()
            part[e] = acc[n % 3, tile(s, UR), :] + stage[s]

            def more(at):
                local(relay.at[at], stage_r.at[s], sr_sem.at[s]).wait()
                part[e] = part[e] + stage_r[s]
            relayed(t, par, u, more)
        own_units(n, core, body)
        t, i = task_of(n)

        @pl.when(i == HALF - 1)
        def _():
            remote(vec.at[t], vland.at[t], v_send.at[t], v_recv.at[t], sib).wait()
            vsum[t] = vec[t] + vland[t]

            @pl.when(t == Y1)
            def _():
                arrived(vland.at[CHUNKS], v_recv.at[CHUNKS])
                vsum[t] = vsum[t] + vland[CHUNKS]

    def send_own(n):
        def body(t, par, u, s, e):
            def go(dst, recv, slot, dev):
                remote(part.at[e], dst, out_send.at[e], recv.at[slot], dev).start()

            @pl.when(t == 0)
            def _():
                go(relay.at[e], relay_recv, e, jnp.where(core == 0, x_base + 1, y_base))

            @pl.when(t == B1)
            def _():
                go(x_fin.at[u], x_recv, u, x_base + par)

            @pl.when(t == Y1)
            def _():
                go(y_fin.at[u], y_recv, u, y_base + par)
        own_units(n, core, body)
        t, i = task_of(n)
        for way, dev in enumerate((xn, xn, yn)):
            @pl.when((i == HALF - 1) & (t == way))
            def _():
                remote(vsum.at[t], vland.at[CHUNKS + way], v_send.at[CHUNKS + way], v_recv.at[CHUNKS + way], dev).start()

    def sib_units(n, act):
        def body(t, par, u, s, e):
            act_on(remote(acc.at[n % 3, tile(s, UR)], sib_land.at[e], sib_send.at[e], sib_recv.at[e], sib), act)
        own_units(n, other(core), body)

    def task(n):
        t, i = task_of(n)
        need, row = bias_of(chip_of(t, chip), i)
        a = n % 3

        @pl.when(n >= 3)
        def _():
            sib_units(n - 3, 'sent')

        def chunk(slot):
            j = n * CHUNKS + slot

            @pl.when(j + CHUNKS - 1 < STEPS)
            def _():
                issue(j + CHUNKS - 1)
            local(xq.at[tile(0, KC), tile(0, BLOCK)], xbuf.at[slot], x_sem.at[slot]).wait()
            local(dyq.at[tile(0, KC), tile(0, D)], dybuf.at[slot], dy_sem.at[slot]).wait()

            def dot():
                return lax.dot_general(xbuf[slot], dybuf[slot], (((0,), (0,)), ((), ())),
                                       preferred_element_type=F32)

            @pl.when(slot == 0)
            def _():
                acc[a] = dot()

            @pl.when(slot > 0)
            def _():
                acc[a] += dot()

            @pl.when(need)
            def _():
                def add(r, total):
                    block = dybuf[slot, tile(r, LANES), :].astype(F32)
                    return total + jnp.sum(block.reshape(-1, 8, D), axis=0)
                total = lax.fori_loop(0, KC // LANES, add, jnp.zeros_like(ss))
                vec[t, pl.ds(row, 1), :] += jnp.sum(total, axis=0, keepdims=True)

            @pl.when((slot == 0) & (n > 0))
            def _():
                prefetch(n - 1)

            @pl.when((slot == 1) & (n > 0))
            def _():
                combine(n - 1)
                send_own(n - 1)
        each(0, CHUNKS, chunk)
        sib_units(n, 'start')

        @pl.when(i == HALF - 1)
        def _():
            remote(vec.at[t], vland.at[t], v_send.at[t], v_recv.at[t], sib).start()

    each(0, TASKS, task)
    prefetch(jnp.int32(TASKS - 1))
    combine(jnp.int32(TASKS - 1))
    each(TASKS - 3, TASKS, lambda n: sib_units(n, 'sent'))

    few = chip - 1 == core
    mid = jnp.logical_not(is_edge(chip))
    past = chip == 2

    def write_unit(u, slot):
        def go(dst):
            local(flat.at[slot], dst, fl_sem.at[slot]).start()

        @pl.when(chip == 0)
        def _():
            go(g_a.at[tile(u % 4, UR), tile(u // 4, 8)])

        @pl.when(chip == 3)
        def _():
            go(g_c.at[tile(u, UR)])
        square = jnp.where((u >= FEW[1]) & (u < FEW[2]), u - FEW[1],
                           jnp.where((u >= FEW[4]) & (u < FEW[-1]), u - 3, -1))
        col = jnp.where(u < FEW[2], 0, jnp.where(u < FEW[4], u - 4, 3))

        @pl.when(mid & few & (square < 0))
        def _():
            go(g_b.at[tile(jnp.where(past, 0, 2), UR), tile(col, 8)])

        @pl.when(mid & few & (square >= 0))
        def _():
            go(g_c.at[tile(jnp.where(past, 4, 0) + square, UR)])

        @pl.when(mid & jnp.logical_not(few))
        def _():
            go(g_b.at[tile(u % 3, UR), tile(u // 3, 8)])

    def written(slot):
        local(flat.at[slot], g_c.at[tile(0, UR)], fl_sem.at[slot]).wait()

    def finish(u):
        slot = u % 2

        @pl.when(u >= 2)
        def _():
            written(slot)
        arrived(x_fin.at[u], x_recv.at[u])
        arrived(y_fin.at[u], y_recv.at[u])

        def add(r, total):
            rows = tile(r, 16)
            val = part[here * UNITS + u, rows, :] + x_fin[u, rows, :] + y_fin[u, rows, :]
            flat[slot, rows] = val.reshape(16, 8, LANES)
            return total + val[0:8] * val[0:8] + val[8:16] * val[8:16]
        ss[...] += lax.fori_loop(0, UR // 16, add, jnp.zeros_like(ss))
        write_unit(u, slot)

    each(0, UNITS, finish)
    arrived(vland.at[5], v_recv.at[5])
    arrived(vland.at[6], v_recv.at[6])
    val = vsum[here] + vland[5] + vland[6]
    vflat[...] = val.reshape(8, 8, LANES)
    total = ss[...] + jnp.where(core == 0, 1.0, 0.0).astype(F32) * (val * val)
    ss_small[...] = sum(total[:, LANES * c:LANES * (c + 1)] for c in range(8))
    tail = [local(vflat, v_out, misc_sem.at[0]), local(ss_small, ss_out, misc_sem.at[1])]
    for c in tail:
        c.start()
    written(0)
    written(1)
    for c in tail:
        c.wait()
    each(0, here * UNITS, lambda e: remote(part.at[e], x_fin.at[0], out_send.at[e], x_recv.at[0], xn).wait_send())
    for way in range(3):
        remote(vsum.at[way], vland.at[CHUNKS], v_send.at[CHUNKS + way], v_recv.at[CHUNKS], xn).wait_send()


def shape(*dims, dtype=F32):
    return jax.ShapeDtypeStruct(dims, dtype)


def vmem(*dims, dtype=F32):
    return pltpu.VMEM(dims, dtype)


def dmas(*counts):
    return [pltpu.SemaphoreType.DMA(c if isinstance(c, tuple) else (c,)) for c in counts]


def any_space(count):
    return [pl.BlockSpec(memory_space=pltpu.HBM)] * count


def params_of(collective_id, mib):
    return pltpu.CompilerParams(collective_id=collective_id, has_side_effects=True, vmem_limit_bytes=mib * MIB)


def reduce_call(acts, ln_rows):
    outs = [shape(512, 24, LANES), shape(384, 32, LANES), shape(1536, 8, LANES), shape(8, 8, LANES), shape(8, LANES),
            shape(CHUNKS * UNITS, UR, D), shape(UNITS, UR, D)]
    return pl.pallas_call(
        reduce_kernel,
        out_shape=outs,
        in_specs=any_space(len(acts) + 1),
        out_specs=any_space(len(outs)),
        scratch_shapes=[
            vmem(CHUNKS, KC, BLOCK, dtype=BF16), vmem(CHUNKS, KC, D, dtype=BF16), vmem(3, BLOCK, D),
            vmem(CHUNKS * UNITS, UR, D), vmem(UNITS, UR, D), vmem(UNITS, UR, D), vmem(CHUNKS, UR, D), vmem(CHUNKS, UR, D), vmem(2, UR, 8, LANES),
            vmem(CHUNKS, 8, D), vmem(CHUNKS, 8, D), vmem(8, 8, LANES), vmem(7, 8, D), vmem(CHUNKS, D), vmem(8, D), vmem(8, LANES),
            *dmas(CHUNKS, CHUNKS, CHUNKS * UNITS, CHUNKS * UNITS, X1 * UNITS, UNITS, UNITS, UNITS, 7, 7, CHUNKS, CHUNKS, 2, 2)],
        compiler_params=params_of(0, 63),
        name='grad_reduce',
    )(*acts, ln_rows)


BLK = 128
PART_BLOCKS = [7] * UNITS + [4, 4, 2, 2]
PARTS = len(PART_BLOCKS)
SEG = max(PART_BLOCKS) * BLK
ENDS = [BLK * sum(PART_BLOCKS[:j]) for j in range(PARTS + 1)]
CUTS = ENDS[:-1] + [SHARD_ROWS]
FULL = SHARE // BLK
LOADS = 4
LOAD = SHARE // LOADS
GB = FULL // LOADS


def update_kernel(w_in, m_in, v_in, ga, gb, gc, vg, ss_in,
                  wbuf, mbuf, vbuf, params, full,
                  gbuf, cin, ssl, sums, rates,
                  load_sem, g_sem, edge_send, edge_recv, ss_send, ss_recv, sum_send, sum_recv,
                  own_send, own_copy, x_recv, y_recv, d_recv, s_recv, fwd_send, sib_fwd, cin_sem):
    me, chip, core, sib, xn, yn = neighbours()

    def floor_of(dev):
        return DOWN * (SHARD_ROWS * dev // DOWN)

    def in_window(dev, row):
        return row - SHARD_ROWS * dev + EDGE

    def load_rows(k):
        return pl.ds(LOAD * k, LOAD if k < LOADS - 1 else SHARD_ROWS - LOAD * k)

    order = [*range(1, LOADS - 1), 0, LOADS - 1]
    loads = [[local(src.at[load_rows(k)], dst.at[load_rows(k)], load_sem.at[e, k])
              for e, (src, dst) in enumerate(((w_in, wbuf), (m_in, mbuf), (v_in, vbuf)))] for k in order]

    def when_in(lo, hi, do, *args):
        @pl.when((me >= lo) & (me <= hi))
        def _():
            do(*args)

    def g_loads(act):
        start = in_window(me, pick(me, NOMINAL))

        def go(*copies):
            for e, (src, lo, size, at) in enumerate(copies):
                act_on(local(src.at[pl.ds(lo, size)], gbuf.at[pl.ds(start + at, size)], g_sem.at[e]), act)
        two, one = SIZES[2], SHARE - SIZES[2]
        tail = (vg, 0, UP, SHARE)
        when_in(0, 0, go, (ga, 0, SHARE, 0))
        when_in(1, 1, go, (ga, 0, SHARE, 0), tail)
        when_in(2, 2, go, (gc, 0, two, 0), (vg, 0, UP, two), (gb, two, one, two + UP))
        when_in(3, 4, go, (gb, 0, SHARE, 0))
        when_in(5, 5, go, (gb, 0, one, 0), (vg, 0, SIZES[7], one), (gc, one, two, one + SIZES[7]))
        when_in(6, 6, go, (gc, 0, SHARE, 0))
        when_in(7, 7, go, (gc, 0, SHARE, 0), tail)

    ss_copy = local(ss_in, ssl.at[me], cin_sem.at[0])
    ss_copy.start()
    g_loads('start')
    for group in loads:
        for c in group:
            c.start()
    sums[...] = jnp.zeros_like(sums)
    others = [lax.rem(me + e, N_DEV) for e in range(1, N_DEV)]
    enter(others)
    ss_copy.wait()

    def share(buf, send, recv, act):
        for e, dev in enumerate(others):
            if act == 'get':
                remote(buf.at[dev], buf.at[dev], send.at[e], recv.at[dev], dev).wait_recv()
            else:
                act_on(remote(buf.at[me], buf.at[me], send.at[e], recv.at[me], dev), act)

    share(ssl, ss_send, ss_recv, 'start')

    def edges(act):
        def go(src, lo, size, dev, row, e):
            act_on(remote(src.at[pl.ds(lo, size)], gbuf.at[pl.ds(in_window(dev, row), size)],
                          edge_send.at[e], edge_recv.at[e], dev), act)

        def up(src):
            go(src, 0, UP, me - 1, pick(me, NOMINAL), 0)

        def down(src):
            go(src, SHARE - DOWN, DOWN, me + 1, pick(me + 1, NOMINAL) - DOWN, 1)
        when_in(1, 1, up, ga)
        when_in(2, 2, up, gc)
        when_in(3, 5, up, gb)
        when_in(6, 7, up, gc)
        when_in(0, 1, down, ga)
        when_in(2, 4, down, gb)
        when_in(5, 6, down, gc)

    edges('start')
    share(ssl, ss_send, ss_recv, 'get')
    grad_sq = jnp.sum(sum(ssl[e] for e in range(N_DEV)))
    grad_sq = grad_sq * (1.0 / (N_DEV * N_DEV))
    norm = jnp.sqrt(jnp.full((8, LANES), grad_sq, F32))
    scale = (1.0 / N_DEV) / jnp.maximum(1.0, norm)
    scale = jnp.concatenate([scale] * (BLK // 8), axis=0)
    g_loads('wait')
    first_t, past_t = pick(me, FIRST_TENSOR), pick(me, PAST_TENSOR)

    REST = SHARD_ROWS - FULL * BLK

    def over(first, past, whole, masked):
        top = min(past, FULL)

        def tensor(t):
            lo = pick(t, STARTS[:-1]) - SHARD_ROWS * me
            hi = pick(t, STARTS[1:]) - SHARD_ROWS * me
            head, tail = lo // BLK, hi // BLK
            from_b = jnp.maximum((lo + BLK - 1) // BLK, first)
            whole(t, from_b, jnp.maximum(from_b, jnp.minimum(tail, top)))

            def shared(b, size, at, g_at):
                ids = lax.broadcasted_iota(jnp.int32, (size, LANES), 0) + b * BLK
                masked(t, at, g_at, (ids >= lo) & (ids < hi))

            def end(e):
                b = jnp.where(e == 0, head, tail)
                cuts = jnp.where(e == 0, lo, hi) % BLK > 0
                again = (e > 0) & (head == tail) & (lo % BLK > 0)

                @pl.when(cuts & (b >= first) & (b < top) & jnp.logical_not(again))
                def _():
                    shared(b, BLK, *block_rows(b))
            each(0, 2, end)
            if past > FULL:
                shared(FULL, REST, pl.ds(FULL * BLK, REST), pl.ds(FULL * BLK + EDGE, REST))
        each(first_t, past_t, tensor)

    def block_rows(b):
        return tile(b, BLK), pl.ds(pl.multiple_of(b * BLK + EDGE, DOWN), BLK)

    def step_of(t, at, g_at):
        decay = jnp.where((t % 2 == 0) & (t != 4) & (t < 9), DECAY, 0.0).astype(F32)
        g, w, m, v = gbuf[g_at, :], wbuf[at, :], mbuf[at, :], vbuf[at, :]
        h = g * scale[:g.shape[0]]
        new_m = BETA_ONE * m + (1.0 - BETA_ONE) * h
        new_v = BETA_TWO * v + (1.0 - BETA_TWO) * (h * h)
        root = new_v * lax.rsqrt(jnp.maximum(new_v, jnp.finfo(F32).tiny))
        u = new_m / (root * (CORR_ONE / CORR_TWO ** 0.5) + EPSILON * CORR_ONE) + decay * w
        return (g, w, m, v), (u, w, new_m, new_v)

    def note(t, u_sq, w_sq):
        sums[me, pl.ds(t, 1), :] += jnp.sum(u_sq, axis=0, keepdims=True)
        sums[me, pl.ds(DOWN + t, 1), :] += jnp.sum(w_sq, axis=0, keepdims=True)

    def direction(t, first, past):
        def block(b, carry):
            at, g_at = block_rows(b)
            _, (u, w, new_m, new_v) = step_of(t, at, g_at)
            mbuf[at, :], vbuf[at, :], gbuf[g_at, :] = new_m, new_v, u
            return tuple(total + jnp.sum((x * x).reshape(-1, 8, LANES), axis=0) for total, x in zip(carry, (u, w)))
        zero = jnp.zeros((8, LANES), F32)
        note(t, *lax.fori_loop(first, past, block, (zero, zero)))

    def direction_shared(t, at, g_at, keep):
        (g, w, m, v), (u, _, new_m, new_v) = step_of(t, at, g_at)
        mbuf[at, :], vbuf[at, :] = jnp.where(keep, new_m, m), jnp.where(keep, new_v, v)
        gbuf[g_at, :] = jnp.where(keep, u, g)
        note(t, jnp.where(keep, u * u, 0.0), jnp.where(keep, w * w, 0.0))

    for k, group in zip(order, loads):
        if k == 0:
            for e, (has, size) in enumerate(((me < N_DEV - 1, UP), (me > 0, DOWN))):
                @pl.when(has)
                def _():
                    rows = gbuf.at[pl.ds(0, size)]
                    remote(rows, rows, edge_send.at[e], edge_recv.at[e], sib).wait_recv()
        for c in group:
            c.wait()
        over(GB * k, GB * (k + 1) + (k == LOADS - 1), direction, direction_shared)
    share(sums, sum_send, sum_recv, 'start')
    share(sums, sum_send, sum_recv, 'get')
    total = jnp.sum(sum(sums[e] for e in range(N_DEV)), axis=1, keepdims=True)
    u_n, w_n = jnp.sqrt(total[:DOWN]), jnp.sqrt(total[DOWN:])
    both = (u_n > 0) & (w_n > 0)
    ratio = jnp.where(both, w_n / jnp.where(u_n > 0, u_n, 1.0), 1.0)
    rates[...] = jnp.broadcast_to(LEARN_RATE * ratio, rates.shape)

    def apply(t, first, past):
        rate = jnp.broadcast_to(rates[pl.ds(t, 1), :], (BLK, LANES))

        def block(b):
            at, g_at = block_rows(b)
            wbuf[at, :] = wbuf[at, :] - rate * gbuf[g_at, :]
        each(first, past, block)

    def apply_shared(t, at, g_at, keep):
        w = wbuf[at, :]
        wbuf[at, :] = jnp.where(keep, w - jnp.broadcast_to(rates[pl.ds(t, 1), :], w.shape) * gbuf[g_at, :], w)

    def cut(dev, j):
        return pl.ds(SHARD_ROWS * dev + CUTS[j], CUTS[j + 1] - CUTS[j])

    def twin(dev):
        return dev + other(2 * core)

    dg = N_DEV - 2 * (chip + 1) + core

    def own_part(j, e, sem, dev):
        return remote(wbuf.at[cut(0, j)], full.at[cut(me, j)], own_send.at[e, j], sem, dev)

    for j in range(PARTS):
        over(ENDS[j] // BLK, ENDS[j + 1] // BLK + (j == PARTS - 1), apply, apply_shared)
        for e, (sem, dev) in enumerate(((x_recv.at[j], xn), (y_recv.at[j], yn), (s_recv.at[0, j], sib))):
            own_part(j, e, sem, dev).start()
        local(wbuf.at[cut(0, j)], full.at[cut(me, j)], own_copy.at[j]).start()

    def wait_from(dev, j, sem):
        rows = full.at[cut(dev, j)]
        remote(rows, rows, cin_sem.at[0], sem, sib).wait_recv()

    def forward(dev, j, send_sem, recv_sem, to):
        rows = full.at[cut(dev, j)]
        remote(rows, rows, send_sem, recv_sem, to).start()

    def convert(*parts):
        todo = []
        for slot, (dev, j) in enumerate(parts):
            skip = DOWN if j == 0 else 0
            lo, size = pl.multiple_of(floor_of(dev) + skip + ENDS[j], DOWN), ENDS[j + 1] - ENDS[j] - skip
            cp = local(full.at[pl.ds(lo, size)], cin.at[slot, pl.ds(0, size)], cin_sem.at[slot])
            cp.start()
            todo.append((cp, slot, lo, size))
        for cp, slot, lo, size in todo:
            cp.wait()

            def body(b):
                params[pl.ds(pl.multiple_of(lo + b * DOWN, DOWN), DOWN), :] = cin[slot, tile(b, DOWN), :].astype(BF16)
            lax.fori_loop(0, size // DOWN, lambda b, c: (body(b), c)[1], 0, unroll=8)

    for j in range(PARTS):
        local(wbuf.at[cut(0, j)], full.at[cut(me, j)], own_copy.at[j]).wait()
        wait_from(sib, j, s_recv.at[0, j])
        convert((me, j), (sib, j))
        wait_from(xn, j, x_recv.at[j])
        forward(xn, j, sib_fwd.at[0, j], s_recv.at[1, j], sib)
        if j % 2 == 0:
            forward(xn, j, fwd_send.at[j], d_recv.at[j], yn)
        wait_from(yn, j, y_recv.at[j])
        forward(yn, j, sib_fwd.at[1, j], s_recv.at[2, j], sib)
        if j % 2 == 1:
            forward(yn, j, fwd_send.at[j], d_recv.at[j], xn)
        convert((xn, j), (yn, j))
        wait_from(twin(xn), j, s_recv.at[1, j])
        wait_from(twin(yn), j, s_recv.at[2, j])
        convert((twin(xn), j), (twin(yn), j))
    for j in range(0, PARTS, 2):
        both_parts = (j, j + 1)
        for e in both_parts:
            wait_from(dg, e, d_recv.at[e])
            forward(dg, e, sib_fwd.at[2, e], s_recv.at[3, e], sib)
        convert(*[(dg, e) for e in both_parts])
        for e in both_parts:
            wait_from(twin(dg), e, s_recv.at[3, e])
        if e == PARTS - 1:
            low = DOWN * (SHARD_ROWS * (N_DEV - 1) // DOWN) + SHARE
            pieces = ([(0, DOWN)] + [(DOWN * (SHARD_ROWS * s // DOWN) - DOWN, 2 * DOWN) for s in range(1, N_DEV)]
                      + [(low, TOTAL_ROWS - low)])
            ends = [local(full.at[pl.ds(lo, size)], cin.at[2, pl.ds(2 * DOWN * p, size)], cin_sem.at[2 + p])
                    for p, (lo, size) in enumerate(pieces)]
            for c in ends:
                c.start()
        convert(*[(twin(dg), e) for e in both_parts])
    for p, (c, (lo, size)) in enumerate(zip(ends, pieces)):
        c.wait()
        params[lo:lo + size, :] = cin[2, 2 * DOWN * p:2 * DOWN * p + size, :].astype(BF16)
    edges('sent')
    share(ssl, ss_send, ss_recv, 'sent')
    share(sums, sum_send, sum_recv, 'sent')
    for j in range(PARTS):
        sems = [fwd_send.at[j]] + [s.at[e, j] for s in (own_send, sib_fwd) for e in range(3)]
        for sem in sems:
            remote(wbuf.at[cut(0, j)], full.at[cut(me, j)], sem, x_recv.at[j], xn).wait_send()


def update_call(w, m, v, ga, gb, gc, vg, ss):
    shard = pltpu.VMEM((SHARD_ROWS, LANES), F32)
    outs = [shard, shard, shard, pltpu.VMEM((TOTAL_ROWS, LANES), BF16), shape(TOTAL_ROWS, LANES)]
    in_vmem = pl.BlockSpec(memory_space=pltpu.VMEM)
    return pl.pallas_call(
        update_kernel,
        out_shape=outs,
        in_specs=any_space(8),
        out_specs=[in_vmem] * 4 + any_space(1),
        scratch_shapes=[
            vmem(WIN, LANES), vmem(3, SEG, LANES),
            vmem(N_DEV, 8, LANES), vmem(N_DEV, 2 * DOWN, LANES), vmem(DOWN, LANES),
            *dmas((3, LOADS), 3, 2, 2, 7, N_DEV, 7, N_DEV, (3, PARTS), PARTS, PARTS, PARTS, PARTS, (4, PARTS),
                  PARTS, (3, PARTS), 11)],
        compiler_params=params_of(1, 14),
        name='lamb_gather',
    )(w, m, v, ga, gb, gc, vg, ss)


def cuts_of(rows):
    size, last = rows // CHUNKS // DOWN * DOWN, CHUNKS - 1
    return [(size * e, size) for e in range(last)] + [(size * last, rows - size * last)]


def write_kernel(*refs):
    *pairs, sem = refs
    half = len(pairs) // 2
    copies = [local(src.at[pl.ds(lo, size)], dst.at[pl.ds(lo, size)], sem.at[p, e])
              for p, (src, dst) in enumerate(zip(pairs[:half], pairs[half:]))
              for e, (lo, size) in enumerate(cuts_of(src.shape[0]))]
    for c in copies:
        c.start()
    for c in copies:
        c.wait()


def write_call(arrays):
    return pl.pallas_call(
        write_kernel,
        out_shape=[jax.ShapeDtypeStruct(a.shape, a.dtype) for a in arrays],
        in_specs=[pl.BlockSpec(memory_space=pltpu.VMEM)] * len(arrays),
        out_specs=any_space(len(arrays)),
        scratch_shapes=dmas((len(arrays), CHUNKS)),
        compiler_params=pltpu.CompilerParams(vmem_limit_bytes=MIB),
        name='write_out',
    )(*arrays)


def solution(mesh):
    def local_step(weights, moment_one, moment_two, *rest):
        *acts, ln_grad = rest
        ga, gb, gc, vg, ss, *_ = reduce_call(acts, ln_grad[0])
        rows = [a.reshape(SHARD_ROWS, LANES) for a in (weights, moment_one, moment_two)]
        out = update_call(*rows, *(g.reshape(-1, LANES) for g in (ga, gb, gc, vg)), ss)
        return tuple(a.reshape(-1) for a in write_call(out[:-1]))

    row_spec = P('dp', None)
    flat_spec = P('dp')
    in_specs = (flat_spec,) * 3 + (row_spec,) * 8 + (P('dp', None, None),)
    return jax.shard_map(local_step, mesh=mesh, in_specs=in_specs, out_specs=(flat_spec,) * 3 + (P(),), check_vma=False)
```

```python
import jax
import jax.numpy as jnp
from jax import lax
from jax.experimental import pallas as pl
from jax.experimental.pallas import tpu as pltpu
from jax.sharding import PartitionSpec as P

STEP = 10
LEARN_RATE = 0.5
BETA_ONE = 0.9
BETA_TWO = 0.999
EPSILON = 1e-6
DECAY = 0.01
CORR_ONE = 1.0 - BETA_ONE ** STEP
CORR_TWO = 1.0 - BETA_TWO ** STEP

D = 1024
N_DEV = 8
TOKENS = 4096
LANES = 128
SUB = 8
SHARD_ROWS = 12301
TOTAL_ROWS = N_DEV * SHARD_ROWS
KC = 1024
CHUNKS = TOKENS // KC
BLOCK = 512
TASKS = 24
STEPS = TASKS * CHUNKS
UR = 128
UNITS = 12
HALF = UNITS // 2
F32 = jnp.float32
BF16 = jnp.bfloat16
MIB = 1024 * 1024

SIZES = [24576, 24, 8192, 8, 8, 8, 32768, 32, 32768, 8, 8, 8]
STARTS = [sum(SIZES[:pos]) for pos in range(len(SIZES) + 1)]
SHARE = UNITS * D
NOMINAL = [0, 12288, 24600, 36912, 49200, 61488, 73808, 86096]
FIRST_TENSOR = [max(t for t, at in enumerate(STARTS[:-1]) if at <= SHARD_ROWS * dev) for dev in range(N_DEV)]
PAST_TENSOR = [1 + max(t for t, at in enumerate(STARTS[:-1]) if at < SHARD_ROWS * (dev + 1)) for dev in range(N_DEV)]
EDGE = 48
WIN = 12416
UP, DOWN = 24, 16
FEW = [0, 1, 5, 6, 7, 11]
MANY = [0, 3, 3, 6, 9, 9]
WIDE = [0, 0, 1, 2, 0, 3]
B1, Y1, X1 = range(1, 4)


def pick(index, values):
    out = jnp.int32(values[-1])
    for pos in reversed(range(len(values) - 1)):
        out = jnp.where(index == pos, jnp.int32(values[pos]), out)
    return out


def tile(index, size):
    return pl.ds(pl.multiple_of(index * size, size), size)


def each(lo, hi, body):
    def step(pos, carry):
        body(pos)
        return carry
    lax.fori_loop(lo, hi, step, lo)


def other(bit):
    return 1 - bit


def device(y, x, core):
    return 4 * y + 2 * x + core


def neighbours():
    me = lax.axis_index('dp')
    chip, core = me // 2, me % 2
    x, y = chip % 2, chip // 2
    return me, chip, core, device(y, x, other(core)), device(y, other(x), core), device(other(y), x, core)


def local(src, dst, sem):
    return pltpu.make_async_copy(src, dst, sem)


def remote(src, dst, send_sem, recv_sem, dev):
    return pltpu.make_async_remote_copy(src_ref=src, dst_ref=dst, send_sem=send_sem, recv_sem=recv_sem,
                                        device_id=(dev,), device_id_type=pl.DeviceIdType.MESH)


def act_on(copy, act):
    if act == 'start':
        copy.start()
    elif act == 'sent':
        copy.wait_send()
    else:
        copy.wait()


def enter(devices):
    barrier = pltpu.get_barrier_semaphore()
    for dev in devices:
        pl.semaphore_signal(barrier, inc=1, device_id=(dev,), device_id_type=pl.DeviceIdType.MESH)
    pl.semaphore_wait(barrier, len(devices))


def task_of(n):
    six = HALF
    mid = n - six
    first, last = n < six, n >= 3 * six
    t = jnp.where(first, 0, jnp.where(last, X1, B1 + mid % 2))
    i = jnp.where(first, n, jnp.where(last, n - 3 * six, mid // 2))
    return t, i


def chip_of(t, chip):
    x, y = chip % 2, chip // 2
    return 2 * ((y + other(t % 2)) % 2) + (x + other(t // 2)) % 2


def is_square(i):
    return i % 3 == 1


def is_edge(q):
    return q % 3 == 0


def operands_of(q, i):
    square, odd, pair = is_square(i), i % 2, i // 2
    kind = jnp.where(is_edge(q), q, jnp.where(square, 2 * q - 1, 2))
    rb = jnp.where(q == 0, odd, jnp.where(is_edge(q), 2 + 3 * odd + pair, jnp.where(square, i // 4, q - 1)))
    cb = jnp.where(q == 0, pair, jnp.where(is_edge(q) | square, 0, pick(i, WIDE)))
    return kind, rb, cb


def units_of(q, i, par):
    square = is_square(i)
    few = q - 1 == par
    cnt = jnp.where(few, jnp.where(square, 4, 1), jnp.where(square, 0, 3))
    s0 = jnp.where(square | (par == 0), 0, 2 * q - 1)
    u0 = jnp.where(few, pick(i, FEW), pick(i, MANY))
    edge = is_edge(q)
    return (jnp.where(edge, 0, s0), jnp.where(edge, jnp.where(i % 2 == par, 4, 0), cnt),
            jnp.where(edge, 4 * (i // 2), u0))


def bias_of(q, i):
    square = is_square(i)
    need = jnp.where(q == 0, i % 2 > 0, jnp.where(q == 1, i == CHUNKS, jnp.where(q == 2, ~square, i == HALF - 1)))
    return need, jnp.where(q == 0, i // 2, jnp.where(q == 2, pick(i, WIDE), 0))


def reduce_kernel(xq, dyq, xp, dyp, xi, dyi, xo, dyo, ln,
                  g_a, g_b, g_c, v_out, ss_out, sib_land, relay,
                  xbuf, dybuf, acc, part, x_fin, y_fin, stage, stage_r, flat, vec, vsum, vflat, vland, lnbuf, ss, ss_small,
                  x_sem, dy_sem, sib_send, sib_recv, out_send, relay_recv, x_recv, y_recv,
                  v_send, v_recv, st_sem, sr_sem, fl_sem, misc_sem):
    me, chip, core, sib, xn, yn = neighbours()
    kinds = ((xq, dyq), (xp, dyp), (xi, dyi), (xo, dyo))
    here = X1

    def arrived(ref, sem):
        remote(ref, ref, misc_sem.at[0], sem, sib).wait_recv()

    def issue(j):
        n, slot = j // CHUNKS, j % CHUNKS
        t, i = task_of(n)
        kind, rb, cb = operands_of(chip_of(t, chip), i)
        for which, (x_ref, dy_ref) in enumerate(kinds):
            @pl.when(kind == which)
            def _():
                local(x_ref.at[tile(slot, KC), tile(rb, BLOCK)], xbuf.at[slot], x_sem.at[slot]).start()
                local(dy_ref.at[tile(slot, KC), tile(cb, D)], dybuf.at[slot], dy_sem.at[slot]).start()

    for j in range(CHUNKS - 1):
        issue(jnp.int32(j))
    ln_copy = local(ln, lnbuf, misc_sem.at[0])
    ln_copy.start()
    x_base, y_base = xn - core, yn - core
    enter((sib, xn, yn, x_base + other(core), y_base + other(core)))
    ln_copy.wait()
    ss[...] = jnp.zeros_like(ss)
    vec[...] = jnp.zeros_like(vec)
    for t in range(4):
        for q in (1, 3):
            @pl.when(chip_of(jnp.int32(t), chip) == q)
            def _():
                vec[t, 1:3, :] = lnbuf[q - 1:q + 1, :]

    def own_units(n, who, body):
        t, i = task_of(n)
        (s_a, _, u_a), (s_b, count_b, u_b) = [units_of(chip_of(t, chip), i, par) for par in range(2)]

        def sub_block(s):
            second = (s >= s_b) & (s < s_b + count_b)
            par = second.astype(jnp.int32)
            u = s + jnp.where(second, u_b - s_b, u_a - s_a)
            pair = 2 * (u // 2) + par
            owner = jnp.where(t == 0, u % 2, jnp.where(t == here, par, t - 1))
            e = jnp.where(t == 0, pair, jnp.where(t == here, here * UNITS + u, UNITS + 2 * u + par))

            @pl.when(owner == who)
            def _():
                body(t, par, u, s, e)
        each(0, CHUNKS, sub_block)

    def relayed(t, par, u, do):
        @pl.when(((t == B1) & (u % 2 == 1)) | ((t == Y1) & (u % 2 == 0)))
        def _():
            do(2 * (u // 2) + par)

    def prefetch(n):
        def body(t, par, u, s, e):
            arrived(sib_land.at[e], sib_recv.at[e])

            @pl.when(n > 0)
            def _():
                local(sib_land.at[e], stage.at[s], st_sem.at[s]).start()

            def more(at):
                arrived(relay.at[at], relay_recv.at[at])
                local(relay.at[at], stage_r.at[s], sr_sem.at[s]).start()
            relayed(t, par, u, more)
        own_units(n, core, body)

    def combine(n):
        def body(t, par, u, s, e):
            @pl.when(n > 0)
            def _():
                local(sib_land.at[e], stage.at[s], st_sem.at[s]).wait()
            part[e] = acc[n % 3, tile(s, UR), :] + stage[s]

            def more(at):
                local(relay.at[at], stage_r.at[s], sr_sem.at[s]).wait()
                part[e] = part[e] + stage_r[s]
            relayed(t, par, u, more)
        own_units(n, core, body)
        t, i = task_of(n)

        @pl.when(i == HALF - 1)
        def _():
            remote(vec.at[t], vland.at[t], v_send.at[t], v_recv.at[t], sib).wait()
            vsum[t] = vec[t] + vland[t]

            @pl.when(t == Y1)
            def _():
                arrived(vland.at[CHUNKS], v_recv.at[CHUNKS])
                vsum[t] = vsum[t] + vland[CHUNKS]

    def send_own(n):
        def body(t, par, u, s, e):
            def go(dst, recv, slot, dev):
                remote(part.at[e], dst, out_send.at[e], recv.at[slot], dev).start()

            @pl.when(t == 0)
            def _():
                go(relay.at[e], relay_recv, e, jnp.where(core == 0, x_base + 1, y_base))

            @pl.when(t == B1)
            def _():
                go(x_fin.at[u], x_recv, u, x_base + par)

            @pl.when(t == Y1)
            def _():
                go(y_fin.at[u], y_recv, u, y_base + par)
        own_units(n, core, body)
        t, i = task_of(n)
        for way, dev in enumerate((xn, xn, yn)):
            @pl.when((i == HALF - 1) & (t == way))
            def _():
                remote(vsum.at[t], vland.at[CHUNKS + way], v_send.at[CHUNKS + way], v_recv.at[CHUNKS + way], dev).start()

    def sib_units(n, act):
        def body(t, par, u, s, e):
            for first, dst in ((True, stage.at[s]), (False, sib_land.at[e])):
                @pl.when((n == 0) == first)
                def _():
                    act_on(remote(acc.at[n % 3, tile(s, UR)], dst, sib_send.at[e], sib_recv.at[e], sib), act)
        own_units(n, other(core), body)

    def task(n):
        t, i = task_of(n)
        need, row = bias_of(chip_of(t, chip), i)
        a = n % 3

        @pl.when(n >= 3)
        def _():
            sib_units(n - 3, 'sent')

        def chunk(slot):
            j = n * CHUNKS + slot

            @pl.when(j + CHUNKS - 1 < STEPS)
            def _():
                issue(j + CHUNKS - 1)
            local(xq.at[tile(0, KC), tile(0, BLOCK)], xbuf.at[slot], x_sem.at[slot]).wait()
            local(dyq.at[tile(0, KC), tile(0, D)], dybuf.at[slot], dy_sem.at[slot]).wait()

            def dot():
                return lax.dot_general(xbuf[slot], dybuf[slot], (((0,), (0,)), ((), ())),
                                       preferred_element_type=F32)

            @pl.when(slot == 0)
            def _():
                acc[a] = dot()

            @pl.when(slot > 0)
            def _():
                acc[a] += dot()

            @pl.when(need)
            def _():
                def add(r, total):
                    block = dybuf[slot, tile(r, LANES), :].astype(F32)
                    return total + jnp.sum(block.reshape(-1, SUB, D), axis=0)
                total = lax.fori_loop(0, KC // LANES, add, jnp.zeros_like(ss))
                vec[t, pl.ds(row, 1), :] += jnp.sum(total, axis=0, keepdims=True)

            @pl.when((slot == 0) & (n > 0))
            def _():
                prefetch(n - 1)

            @pl.when((slot == jnp.where(n == 1, 0, 1)) & (n > 0))
            def _():
                combine(n - 1)
                send_own(n - 1)
        each(0, CHUNKS, chunk)
        sib_units(n, 'start')

        @pl.when(i == HALF - 1)
        def _():
            remote(vec.at[t], vland.at[t], v_send.at[t], v_recv.at[t], sib).start()

    each(0, TASKS, task)
    prefetch(jnp.int32(TASKS - 1))
    combine(jnp.int32(TASKS - 1))
    each(TASKS - 3, TASKS, lambda n: sib_units(n, 'sent'))

    few = chip - 1 == core
    mid = jnp.logical_not(is_edge(chip))
    past = chip == 2

    def write_unit(u, slot):
        def go(dst):
            local(flat.at[slot], dst, fl_sem.at[slot]).start()

        @pl.when(chip == 0)
        def _():
            go(g_a.at[tile(u % 4, UR), tile(u // 4, SUB)])

        @pl.when(chip == 3)
        def _():
            go(g_c.at[tile(u, UR)])
        square = jnp.where((u >= FEW[1]) & (u < FEW[2]), u - FEW[1],
                           jnp.where((u >= FEW[4]) & (u < FEW[-1]), u - 3, -1))
        col = jnp.where(u < FEW[2], 0, jnp.where(u < FEW[4], u - 4, 3))

        @pl.when(mid & few & (square < 0))
        def _():
            go(g_b.at[tile(jnp.where(past, 0, 2), UR), tile(col, SUB)])

        @pl.when(mid & few & (square >= 0))
        def _():
            go(g_c.at[tile(jnp.where(past, 4, 0) + square, UR)])

        @pl.when(mid & jnp.logical_not(few))
        def _():
            go(g_b.at[tile(u % 3, UR), tile(u // 3, SUB)])

    def written(slot):
        local(flat.at[slot], g_c.at[tile(0, UR)], fl_sem.at[slot]).wait()

    def finish(u):
        slot = u % 2

        @pl.when(u >= 2)
        def _():
            written(slot)
        arrived(x_fin.at[u], x_recv.at[u])
        arrived(y_fin.at[u], y_recv.at[u])

        def add(r, total):
            rows = tile(r, 16)
            val = part[here * UNITS + u, rows, :] + x_fin[u, rows, :] + y_fin[u, rows, :]
            flat[slot, rows] = val.reshape(16, SUB, LANES)
            return total + val[0:8] * val[0:8] + val[8:16] * val[8:16]
        ss[...] += lax.fori_loop(0, UR // 16, add, jnp.zeros_like(ss))
        write_unit(u, slot)

    each(0, UNITS, finish)
    arrived(vland.at[5], v_recv.at[5])
    arrived(vland.at[6], v_recv.at[6])
    val = vsum[here] + vland[5] + vland[6]
    vflat[...] = val.reshape(8, SUB, LANES)
    total = ss[...] + jnp.where(core == 0, 1.0, 0.0).astype(F32) * (val * val)
    ss_small[...] = sum(total[:, LANES * c:LANES * (c + 1)] for c in range(8))
    tail = [local(vflat, v_out, misc_sem.at[0]), local(ss_small, ss_out, misc_sem.at[1])]
    for c in tail:
        c.start()
    written(0)
    written(1)
    for c in tail:
        c.wait()
    each(0, here * UNITS, lambda e: remote(part.at[e], x_fin.at[0], out_send.at[e], x_recv.at[0], xn).wait_send())
    for way in range(3):
        remote(vsum.at[way], vland.at[CHUNKS], v_send.at[CHUNKS + way], v_recv.at[CHUNKS], xn).wait_send()


def shape(*dims, dtype=F32):
    return jax.ShapeDtypeStruct(dims, dtype)


def vmem(*dims, dtype=F32):
    return pltpu.VMEM(dims, dtype)


def dmas(*counts):
    return [pltpu.SemaphoreType.DMA(c if isinstance(c, tuple) else (c,)) for c in counts]


def any_space(count):
    return [pl.BlockSpec(memory_space=pltpu.HBM)] * count


def params_of(collective_id, mib):
    return pltpu.CompilerParams(collective_id=collective_id, has_side_effects=True, vmem_limit_bytes=mib * MIB)


def reduce_call(acts, ln_rows):
    outs = [shape(512, 24, LANES), shape(384, 32, LANES), shape(1536, SUB, LANES), shape(8, SUB, LANES), shape(SUB, LANES),
            shape(CHUNKS * UNITS, UR, D), shape(UNITS, UR, D)]
    return pl.pallas_call(
        reduce_kernel,
        out_shape=outs,
        in_specs=any_space(len(acts) + 1),
        out_specs=any_space(len(outs)),
        scratch_shapes=[
            vmem(CHUNKS, KC, BLOCK, dtype=BF16), vmem(CHUNKS, KC, D, dtype=BF16), vmem(3, BLOCK, D),
            vmem(CHUNKS * UNITS, UR, D), vmem(UNITS, UR, D), vmem(UNITS, UR, D), vmem(CHUNKS, UR, D), vmem(CHUNKS, UR, D), vmem(2, UR, SUB, LANES),
            vmem(CHUNKS, 8, D), vmem(CHUNKS, 8, D), vmem(8, SUB, LANES), vmem(7, 8, D), vmem(CHUNKS, D), vmem(8, D), vmem(SUB, LANES),
            *dmas(CHUNKS, CHUNKS, CHUNKS * UNITS, CHUNKS * UNITS, X1 * UNITS, UNITS, UNITS, UNITS, 7, 7, CHUNKS, CHUNKS, 2, 2)],
        compiler_params=params_of(0, 63),
        name='grad_reduce',
    )(*acts, ln_rows)


BLK = 128
PART_BLOCKS = [7] * UNITS + [4, 4, 2, 2]
PARTS = len(PART_BLOCKS)
SEG = max(PART_BLOCKS) * BLK
ENDS = [BLK * sum(PART_BLOCKS[:j]) for j in range(PARTS + 1)]
CUTS = ENDS[:-1] + [SHARD_ROWS]
FULL = SHARE // BLK
LOADS = 4
LOAD = SHARE // LOADS
GB = FULL // LOADS


def update_kernel(w_in, m_in, v_in, ga, gb, gc, vg, ss_in,
                  wbuf, mbuf, vbuf, params, full,
                  gbuf, cin, ssl, sums, rates,
                  load_sem, g_sem, edge_send, edge_recv, ss_send, ss_recv, sum_send, sum_recv,
                  own_send, own_copy, x_recv, y_recv, d_recv, s_recv, fwd_send, sib_fwd, cin_sem):
    me, chip, core, sib, xn, yn = neighbours()

    def floor_of(dev):
        return DOWN * (SHARD_ROWS * dev // DOWN)

    def in_window(dev, row):
        return row - SHARD_ROWS * dev + EDGE

    def load_rows(k):
        return pl.ds(LOAD * k, LOAD if k < LOADS - 1 else SHARD_ROWS - LOAD * k)

    order = [*range(1, LOADS - 1), 0, LOADS - 1]
    loads = [[local(src.at[load_rows(k)], dst.at[load_rows(k)], load_sem.at[e, k])
              for e, (src, dst) in enumerate(((w_in, wbuf), (m_in, mbuf), (v_in, vbuf)))] for k in order]

    def when_in(lo, hi, do, *args):
        @pl.when((me >= lo) & (me <= hi))
        def _():
            do(*args)

    def g_loads(act):
        start = in_window(me, pick(me, NOMINAL))

        def go(*copies):
            for e, (src, lo, size, at) in enumerate(copies):
                act_on(local(src.at[pl.ds(lo, size)], gbuf.at[pl.ds(start + at, size)], g_sem.at[e]), act)
        two, one = SIZES[2], SHARE - SIZES[2]
        tail = (vg, 0, UP, SHARE)
        when_in(0, 0, go, (ga, 0, SHARE, 0))
        when_in(1, 1, go, (ga, 0, SHARE, 0), tail)
        when_in(2, 2, go, (gc, 0, two, 0), (vg, 0, UP, two), (gb, two, one, two + UP))
        when_in(3, 4, go, (gb, 0, SHARE, 0))
        when_in(5, 5, go, (gb, 0, one, 0), (vg, 0, SIZES[7], one), (gc, one, two, one + SIZES[7]))
        when_in(6, 6, go, (gc, 0, SHARE, 0))
        when_in(7, 7, go, (gc, 0, SHARE, 0), tail)

    ss_copy = local(ss_in, ssl.at[me], cin_sem.at[0])
    ss_copy.start()
    g_loads('start')
    for group in loads:
        for c in group:
            c.start()
    sums[...] = jnp.zeros_like(sums)
    others = [lax.rem(me + e, N_DEV) for e in range(1, N_DEV)]
    enter(others)
    ss_copy.wait()

    def share(buf, send, recv, act):
        for e, dev in enumerate(others):
            if act == 'get':
                remote(buf.at[dev], buf.at[dev], send.at[e], recv.at[dev], dev).wait_recv()
            else:
                act_on(remote(buf.at[me], buf.at[me], send.at[e], recv.at[me], dev), act)

    share(ssl, ss_send, ss_recv, 'start')

    def edges(act):
        def go(src, lo, size, dev, row, e):
            act_on(remote(src.at[pl.ds(lo, size)], gbuf.at[pl.ds(in_window(dev, row), size)],
                          edge_send.at[e], edge_recv.at[e], dev), act)

        def up(src):
            go(src, 0, UP, me - 1, pick(me, NOMINAL), 0)

        def down(src):
            go(src, SHARE - DOWN, DOWN, me + 1, pick(me + 1, NOMINAL) - DOWN, 1)
        when_in(1, 1, up, ga)
        when_in(2, 2, up, gc)
        when_in(3, 5, up, gb)
        when_in(6, 7, up, gc)
        when_in(0, 1, down, ga)
        when_in(2, 4, down, gb)
        when_in(5, 6, down, gc)

    edges('start')
    share(ssl, ss_send, ss_recv, 'get')
    grad_sq = jnp.sum(sum(ssl[e] for e in range(N_DEV)))
    grad_sq = grad_sq * (1.0 / (N_DEV * N_DEV))
    norm = jnp.sqrt(jnp.full((SUB, LANES), grad_sq, F32))
    scale = (1.0 / N_DEV) / jnp.maximum(1.0, norm)
    scale = jnp.concatenate([scale] * (BLK // 8), axis=0)
    g_loads('wait')
    first_t, past_t = pick(me, FIRST_TENSOR), pick(me, PAST_TENSOR)

    REST = SHARD_ROWS - FULL * BLK

    def over(first, past, whole, masked):
        top = min(past, FULL)

        def tensor(t):
            lo = pick(t, STARTS[:-1]) - SHARD_ROWS * me
            hi = pick(t, STARTS[1:]) - SHARD_ROWS * me
            head, tail = lo // BLK, hi // BLK
            from_b = jnp.maximum((lo + BLK - 1) // BLK, first)
            whole(t, from_b, jnp.maximum(from_b, jnp.minimum(tail, top)))

            def shared(b, size, at, g_at):
                ids = lax.broadcasted_iota(jnp.int32, (size, LANES), 0) + b * BLK
                masked(t, at, g_at, (ids >= lo) & (ids < hi))

            def end(e):
                b = jnp.where(e == 0, head, tail)
                cuts = jnp.where(e == 0, lo, hi) % BLK > 0
                again = (e > 0) & (head == tail) & (lo % BLK > 0)

                @pl.when(cuts & (b >= first) & (b < top) & jnp.logical_not(again))
                def _():
                    shared(b, BLK, *block_rows(b))
            each(0, 2, end)
            if past > FULL:
                shared(FULL, REST, pl.ds(FULL * BLK, REST), pl.ds(FULL * BLK + EDGE, REST))
        each(first_t, past_t, tensor)

    def block_rows(b):
        return tile(b, BLK), pl.ds(pl.multiple_of(b * BLK + EDGE, DOWN), BLK)

    def step_of(t, at, g_at):
        decay = jnp.where((t % 2 == 0) & (t != 4) & (t < 9), DECAY, 0.0).astype(F32)
        g, w, m, v = gbuf[g_at, :], wbuf[at, :], mbuf[at, :], vbuf[at, :]
        h = g * scale[:g.shape[0]]
        new_m = BETA_ONE * m + (1.0 - BETA_ONE) * h
        new_v = BETA_TWO * v + (1.0 - BETA_TWO) * (h * h)
        root = new_v * lax.rsqrt(jnp.maximum(new_v, jnp.finfo(F32).tiny))
        u = new_m / (root * (CORR_ONE / CORR_TWO ** 0.5) + EPSILON * CORR_ONE) + decay * w
        return (g, w, m, v), (u, w, new_m, new_v)

    def note(t, u_sq, w_sq):
        sums[me, pl.ds(t, 1), :] += jnp.sum(u_sq, axis=0, keepdims=True)
        sums[me, pl.ds(DOWN + t, 1), :] += jnp.sum(w_sq, axis=0, keepdims=True)

    def direction(t, first, past):
        def block(b, carry):
            at, g_at = block_rows(b)
            _, (u, w, new_m, new_v) = step_of(t, at, g_at)
            mbuf[at, :], vbuf[at, :], gbuf[g_at, :] = new_m, new_v, u
            return tuple(total + jnp.sum((x * x).reshape(-1, SUB, LANES), axis=0) for total, x in zip(carry, (u, w)))
        zero = jnp.zeros((SUB, LANES), F32)
        note(t, *lax.fori_loop(first, past, block, (zero, zero)))

    def direction_shared(t, at, g_at, keep):
        (g, w, m, v), (u, _, new_m, new_v) = step_of(t, at, g_at)
        mbuf[at, :], vbuf[at, :] = jnp.where(keep, new_m, m), jnp.where(keep, new_v, v)
        gbuf[g_at, :] = jnp.where(keep, u, g)
        note(t, jnp.where(keep, u * u, 0.0), jnp.where(keep, w * w, 0.0))

    for k, group in zip(order, loads):
        if k == 0:
            for e, (has, size) in enumerate(((me < N_DEV - 1, UP), (me > 0, DOWN))):
                @pl.when(has)
                def _():
                    rows = gbuf.at[pl.ds(0, size)]
                    remote(rows, rows, edge_send.at[e], edge_recv.at[e], sib).wait_recv()
        for c in group:
            c.wait()
        over(GB * k, GB * (k + 1) + (k == LOADS - 1), direction, direction_shared)
    share(sums, sum_send, sum_recv, 'start')
    share(sums, sum_send, sum_recv, 'get')
    total = jnp.sum(sum(sums[e] for e in range(N_DEV)), axis=1, keepdims=True)
    u_n, w_n = jnp.sqrt(total[:DOWN]), jnp.sqrt(total[DOWN:])
    both = (u_n > 0) & (w_n > 0)
    ratio = jnp.where(both, w_n / jnp.where(u_n > 0, u_n, 1.0), 1.0)
    rates[...] = jnp.broadcast_to(LEARN_RATE * ratio, rates.shape)

    def apply(t, first, past):
        rate = jnp.broadcast_to(rates[pl.ds(t, 1), :], (BLK, LANES))

        def block(b):
            at, g_at = block_rows(b)
            wbuf[at, :] = wbuf[at, :] - rate * gbuf[g_at, :]
        each(first, past, block)

    def apply_shared(t, at, g_at, keep):
        w = wbuf[at, :]
        wbuf[at, :] = jnp.where(keep, w - jnp.broadcast_to(rates[pl.ds(t, 1), :], w.shape) * gbuf[g_at, :], w)

    def cut(dev, j):
        return pl.ds(SHARD_ROWS * dev + CUTS[j], CUTS[j + 1] - CUTS[j])

    def twin(dev):
        return dev + other(2 * core)

    dg = N_DEV - 2 * (chip + 1) + core

    def own_part(j, e, sem, dev):
        return remote(wbuf.at[cut(0, j)], full.at[cut(me, j)], own_send.at[e, j], sem, dev)

    for j in range(PARTS):
        over(ENDS[j] // BLK, ENDS[j + 1] // BLK + (j == PARTS - 1), apply, apply_shared)
        for e, (sem, dev) in enumerate(((x_recv.at[j], xn), (y_recv.at[j], yn), (s_recv.at[0, j], sib))):
            own_part(j, e, sem, dev).start()
        local(wbuf.at[cut(0, j)], full.at[cut(me, j)], own_copy.at[j]).start()

    def wait_from(dev, j, sem):
        rows = full.at[cut(dev, j)]
        remote(rows, rows, cin_sem.at[0], sem, sib).wait_recv()

    def forward(dev, j, send_sem, recv_sem, to):
        rows = full.at[cut(dev, j)]
        remote(rows, rows, send_sem, recv_sem, to).start()

    def convert(*parts):
        todo = []
        for slot, (dev, j) in enumerate(parts):
            skip = DOWN if j == 0 else 0
            lo, size = pl.multiple_of(floor_of(dev) + skip + ENDS[j], DOWN), ENDS[j + 1] - ENDS[j] - skip
            cp = local(full.at[pl.ds(lo, size)], cin.at[slot, pl.ds(0, size)], cin_sem.at[slot])
            cp.start()
            todo.append((cp, slot, lo, size))
        for cp, slot, lo, size in todo:
            cp.wait()

            def body(b):
                params[pl.ds(pl.multiple_of(lo + b * DOWN, DOWN), DOWN), :] = cin[slot, tile(b, DOWN), :].astype(BF16)
            lax.fori_loop(0, size // DOWN, lambda b, c: (body(b), c)[1], 0, unroll=8)

    for j in range(PARTS):
        local(wbuf.at[cut(0, j)], full.at[cut(me, j)], own_copy.at[j]).wait()
        wait_from(sib, j, s_recv.at[0, j])
        convert((me, j), (sib, j))
        wait_from(xn, j, x_recv.at[j])
        forward(xn, j, sib_fwd.at[0, j], s_recv.at[1, j], sib)
        if j % 2 == 0:
            forward(xn, j, fwd_send.at[j], d_recv.at[j], yn)
        wait_from(yn, j, y_recv.at[j])
        forward(yn, j, sib_fwd.at[1, j], s_recv.at[2, j], sib)
        if j % 2 == 1:
            forward(yn, j, fwd_send.at[j], d_recv.at[j], xn)
        convert((xn, j), (yn, j))
        wait_from(twin(xn), j, s_recv.at[1, j])
        wait_from(twin(yn), j, s_recv.at[2, j])
        convert((twin(xn), j), (twin(yn), j))
    def drain(*sems):
        for j, sem in enumerate(sems):
            remote(wbuf.at[cut(0, j % PARTS)], full.at[cut(me, j % PARTS)], sem, x_recv.at[j % PARTS], xn).wait_send()

    for j in range(0, PARTS, 2):
        both_parts = (j, j + 1)
        if both_parts[-1] == PARTS - 1:
            edges('sent')
            share(ssl, ss_send, ss_recv, 'sent')
            share(sums, sum_send, sum_recv, 'sent')
            for sems in ([own_send.at[e] for e in range(3)] + [sib_fwd.at[e] for e in range(2)]):
                drain(*(sems.at[p] for p in range(PARTS)))
        for e in both_parts:
            wait_from(dg, e, d_recv.at[e])
            forward(dg, e, sib_fwd.at[2, e], s_recv.at[3, e], sib)
        convert(*[(dg, e) for e in both_parts])
        for e in both_parts:
            wait_from(twin(dg), e, s_recv.at[3, e])
        if e == PARTS - 1:
            low = DOWN * (SHARD_ROWS * (N_DEV - 1) // DOWN) + SHARE
            pieces = ([(0, DOWN)] + [(DOWN * (SHARD_ROWS * s // DOWN) - DOWN, 2 * DOWN) for s in range(1, N_DEV)]
                      + [(low, TOTAL_ROWS - low)])
            ends = [local(full.at[pl.ds(lo, size)], cin.at[2, pl.ds(2 * DOWN * p, size)], cin_sem.at[2 + p])
                    for p, (lo, size) in enumerate(pieces)]
            for c in ends:
                c.start()
        convert(*[(twin(dg), e) for e in both_parts])
    for p, (c, (lo, size)) in enumerate(zip(ends, pieces)):
        c.wait()
        params[lo:lo + size, :] = cin[2, 2 * DOWN * p:2 * DOWN * p + size, :].astype(BF16)
    drain(*(fwd_send.at[j] for j in range(PARTS)))
    drain(*(sib_fwd.at[2, j] for j in range(PARTS)))


def update_call(w, m, v, ga, gb, gc, vg, ss):
    shard = pltpu.VMEM((SHARD_ROWS, LANES), F32)
    outs = [shard, shard, shard, pltpu.VMEM((TOTAL_ROWS, LANES), BF16), shape(TOTAL_ROWS, LANES)]
    in_vmem = pl.BlockSpec(memory_space=pltpu.VMEM)
    return pl.pallas_call(
        update_kernel,
        out_shape=outs,
        in_specs=any_space(8),
        out_specs=[in_vmem] * 4 + any_space(1),
        scratch_shapes=[
            vmem(WIN, LANES), vmem(3, SEG, LANES),
            vmem(N_DEV, SUB, LANES), vmem(N_DEV, 2 * DOWN, LANES), vmem(DOWN, LANES),
            *dmas((3, LOADS), 3, 2, 2, 7, N_DEV, 7, N_DEV, (3, PARTS), PARTS, PARTS, PARTS, PARTS, (4, PARTS),
                  PARTS, (3, PARTS), 11)],
        compiler_params=params_of(1, 14),
        name='lamb_gather',
    )(w, m, v, ga, gb, gc, vg, ss)


def cuts_of(rows):
    size, last = rows // CHUNKS // DOWN * DOWN, CHUNKS - 1
    return [(size * e, size) for e in range(last)] + [(size * last, rows - size * last)]


def write_kernel(*refs):
    *pairs, sem = refs
    half = len(pairs) // 2
    copies = [local(src.at[pl.ds(lo, size)], dst.at[pl.ds(lo, size)], sem.at[p, e])
              for p, (src, dst) in enumerate(zip(pairs[:half], pairs[half:]))
              for e, (lo, size) in enumerate(cuts_of(src.shape[0]))]
    for c in copies:
        c.start()
    for c in copies:
        c.wait()


def write_call(arrays):
    return pl.pallas_call(
        write_kernel,
        out_shape=[jax.ShapeDtypeStruct(a.shape, a.dtype) for a in arrays],
        in_specs=[pl.BlockSpec(memory_space=pltpu.VMEM)] * len(arrays),
        out_specs=any_space(len(arrays)),
        scratch_shapes=dmas((len(arrays), CHUNKS)),
        compiler_params=pltpu.CompilerParams(vmem_limit_bytes=MIB),
        name='write_out',
    )(*arrays)


def solution(mesh):
    def local_step(weights, moment_one, moment_two, *rest):
        *acts, ln_grad = rest
        ga, gb, gc, vg, ss, *_ = reduce_call(acts, ln_grad[0])
        rows = [a.reshape(SHARD_ROWS, LANES) for a in (weights, moment_one, moment_two)]
        out = update_call(*rows, *(g.reshape(-1, LANES) for g in (ga, gb, gc, vg)), ss)
        return tuple(a.reshape(-1) for a in write_call(out[:-1]))

    row_spec = P('dp', None)
    flat_spec = P('dp')
    in_specs = (flat_spec,) * 3 + (row_spec,) * 8 + (P('dp', None, None),)
    return jax.shard_map(local_step, mesh=mesh, in_specs=in_specs, out_specs=(flat_spec,) * 3 + (P(),), check_vma=False)
```

```python
import jax
import jax.numpy as jnp
from jax import lax
from jax.experimental import pallas as pl
from jax.experimental.pallas import tpu as pltpu
from jax.sharding import PartitionSpec as P

STEP = 10
LEARN_RATE = 0.5
BETA_ONE = 0.9
BETA_TWO = 0.999
EPSILON = 1e-6
DECAY = 0.01
CORR_ONE = 1.0 - BETA_ONE ** STEP
CORR_TWO = 1.0 - BETA_TWO ** STEP

D = 1024
N_DEV = 8
TOKENS = 4096
LANES = 128
SUB = 8
SHARD_ROWS = 12301
TOTAL_ROWS = N_DEV * SHARD_ROWS
KC = 1024
CHUNKS = TOKENS // KC
BLOCK = 512
TASKS = 24
STEPS = TASKS * CHUNKS
UR = 128
UNITS = 12
HALF = UNITS // 2
F32 = jnp.float32
BF16 = jnp.bfloat16
MIB = 1024 * 1024

SIZES = [24576, 24, 8192, 8, 8, 8, 32768, 32, 32768, 8, 8, 8]
STARTS = [sum(SIZES[:pos]) for pos in range(len(SIZES) + 1)]
SHARE = UNITS * D
NOMINAL = [0, 12288, 24600, 36912, 49200, 61488, 73808, 86096]
FIRST_TENSOR = [max(t for t, at in enumerate(STARTS[:-1]) if at <= SHARD_ROWS * dev) for dev in range(N_DEV)]
PAST_TENSOR = [1 + max(t for t, at in enumerate(STARTS[:-1]) if at < SHARD_ROWS * (dev + 1)) for dev in range(N_DEV)]
EDGE = 48
WIN = 12416
UP, DOWN = 24, 16
FEW = [0, 1, 5, 6, 7, 11]
MANY = [0, 3, 3, 6, 9, 9]
WIDE = [0, 0, 1, 2, 0, 3]
B1, Y1, X1 = range(1, 4)


def pick(index, values):
    out = jnp.int32(values[-1])
    for pos in reversed(range(len(values) - 1)):
        out = jnp.where(index == pos, jnp.int32(values[pos]), out)
    return out


def tile(index, size):
    return pl.ds(pl.multiple_of(index * size, size), size)


def each(lo, hi, body):
    def step(pos, carry):
        body(pos)
        return carry
    lax.fori_loop(lo, hi, step, lo)


def other(bit):
    return 1 - bit


def device(y, x, core):
    return 4 * y + 2 * x + core


def neighbours():
    me = lax.axis_index('dp')
    chip, core = me // 2, me % 2
    x, y = chip % 2, chip // 2
    return me, chip, core, device(y, x, other(core)), device(y, other(x), core), device(other(y), x, core)


def local(src, dst, sem):
    return pltpu.make_async_copy(src, dst, sem)


def remote(src, dst, send_sem, recv_sem, dev):
    return pltpu.make_async_remote_copy(src_ref=src, dst_ref=dst, send_sem=send_sem, recv_sem=recv_sem,
                                        device_id=(dev,), device_id_type=pl.DeviceIdType.MESH)


def act_on(copy, act):
    if act == 'start':
        copy.start()
    elif act == 'sent':
        copy.wait_send()
    else:
        copy.wait()


def enter(devices):
    barrier = pltpu.get_barrier_semaphore()
    for dev in devices:
        pl.semaphore_signal(barrier, inc=1, device_id=(dev,), device_id_type=pl.DeviceIdType.MESH)
    pl.semaphore_wait(barrier, len(devices))


def task_of(n):
    six = HALF
    mid = n - six
    first, last = n < six, n >= 3 * six
    t = jnp.where(first, 0, jnp.where(last, X1, B1 + mid % 2))
    i = jnp.where(first, n, jnp.where(last, n - 3 * six, mid // 2))
    return t, i


def chip_of(t, chip):
    x, y = chip % 2, chip // 2
    return 2 * ((y + other(t % 2)) % 2) + (x + other(t // 2)) % 2


def is_square(i):
    return i % 3 == 1


def is_edge(q):
    return q % 3 == 0


def operands_of(q, i):
    square, odd, pair = is_square(i), i % 2, i // 2
    kind = jnp.where(is_edge(q), q, jnp.where(square, 2 * q - 1, 2))
    rb = jnp.where(q == 0, odd, jnp.where(is_edge(q), 2 + 3 * odd + pair, jnp.where(square, i // 4, q - 1)))
    cb = jnp.where(q == 0, pair, jnp.where(is_edge(q) | square, 0, pick(i, WIDE)))
    return kind, rb, cb


def units_of(q, i, par):
    square = is_square(i)
    few = q - 1 == par
    cnt = jnp.where(few, jnp.where(square, 4, 1), jnp.where(square, 0, 3))
    s0 = jnp.where(square | (par == 0), 0, 2 * q - 1)
    u0 = jnp.where(few, pick(i, FEW), pick(i, MANY))
    edge = is_edge(q)
    return (jnp.where(edge, 0, s0), jnp.where(edge, jnp.where(i % 2 == par, 4, 0), cnt),
            jnp.where(edge, 4 * (i // 2), u0))


def bias_of(q, i):
    square = is_square(i)
    need = jnp.where(q == 0, i % 2 > 0, jnp.where(q == 1, i == CHUNKS, jnp.where(q == 2, ~square, i == HALF - 1)))
    return need, jnp.where(q == 0, i // 2, jnp.where(q == 2, pick(i, WIDE), 0))


def reduce_kernel(xq, dyq, xp, dyp, xi, dyi, xo, dyo, ln,
                  g_a, g_b, g_c, v_out, ss_out, sib_land, relay,
                  xbuf, dybuf, acc, part, x_fin, y_fin, stage, stage_r, flat, vec, vsum, vflat, vland, lnbuf, ss, ss_small,
                  x_sem, dy_sem, sib_send, sib_recv, out_send, relay_recv, x_recv, y_recv,
                  v_send, v_recv, st_sem, sr_sem, fl_sem, misc_sem):
    me, chip, core, sib, xn, yn = neighbours()
    kinds = ((xq, dyq), (xp, dyp), (xi, dyi), (xo, dyo))
    here = X1

    def arrived(ref, sem):
        remote(ref, ref, misc_sem.at[0], sem, sib).wait_recv()

    def issue(j):
        n, slot = j // CHUNKS, j % CHUNKS
        t, i = task_of(n)
        kind, rb, cb = operands_of(chip_of(t, chip), i)
        for which, (x_ref, dy_ref) in enumerate(kinds):
            @pl.when(kind == which)
            def _():
                local(x_ref.at[tile(slot, KC), tile(rb, BLOCK)], xbuf.at[slot], x_sem.at[slot]).start()
                local(dy_ref.at[tile(slot, KC), tile(cb, D)], dybuf.at[slot], dy_sem.at[slot]).start()

    for j in range(CHUNKS - 1):
        issue(jnp.int32(j))
    ln_copy = local(ln, lnbuf, misc_sem.at[0])
    ln_copy.start()
    x_base, y_base = xn - core, yn - core
    enter((sib, xn, yn, x_base + other(core), y_base + other(core)))
    ln_copy.wait()
    ss[...] = jnp.zeros_like(ss)
    vec[...] = jnp.zeros_like(vec)
    for t in range(4):
        for q in (1, 3):
            @pl.when(chip_of(jnp.int32(t), chip) == q)
            def _():
                vec[t, 1:3, :] = lnbuf[q - 1:q + 1, :]

    def own_units(n, who, body):
        t, i = task_of(n)
        (s_a, _, u_a), (s_b, count_b, u_b) = [units_of(chip_of(t, chip), i, par) for par in range(2)]

        def sub_block(s):
            second = (s >= s_b) & (s < s_b + count_b)
            par = second.astype(jnp.int32)
            u = s + jnp.where(second, u_b - s_b, u_a - s_a)
            pair = 2 * (u // 2) + par
            owner = jnp.where(t == 0, u % 2, jnp.where(t == here, par, t - 1))
            e = jnp.where(t == 0, pair, jnp.where(t == here, here * UNITS + u, UNITS + 2 * u + par))

            @pl.when(owner == who)
            def _():
                body(t, par, u, s, e)
        each(0, CHUNKS, sub_block)

    def relayed(t, par, u, do):
        @pl.when(((t == B1) & (u % 2 == 1)) | ((t == Y1) & (u % 2 == 0)))
        def _():
            do(2 * (u // 2) + par)

    def prefetch(n):
        def body(t, par, u, s, e):
            arrived(sib_land.at[e], sib_recv.at[e])

            @pl.when(n > 0)
            def _():
                local(sib_land.at[e], stage.at[s], st_sem.at[s]).start()

            def more(at):
                arrived(relay.at[at], relay_recv.at[at])
                local(relay.at[at], stage_r.at[s], sr_sem.at[s]).start()
            relayed(t, par, u, more)
        own_units(n, core, body)

    def combine(n):
        def body(t, par, u, s, e):
            @pl.when(n > 0)
            def _():
                local(sib_land.at[e], stage.at[s], st_sem.at[s]).wait()
            part[e] = acc[n % 3, tile(s, UR), :] + stage[s]

            def more(at):
                local(relay.at[at], stage_r.at[s], sr_sem.at[s]).wait()
                part[e] = part[e] + stage_r[s]
            relayed(t, par, u, more)
        own_units(n, core, body)
        t, i = task_of(n)

        @pl.when(i == HALF - 1)
        def _():
            remote(vec.at[t], vland.at[t], v_send.at[t], v_recv.at[t], sib).wait()
            vsum[t] = vec[t] + vland[t]

            @pl.when(t == Y1)
            def _():
                arrived(vland.at[CHUNKS], v_recv.at[CHUNKS])
                vsum[t] = vsum[t] + vland[CHUNKS]

    def send_own(n):
        def body(t, par, u, s, e):
            def go(dst, recv, slot, dev):
                remote(part.at[e], dst, out_send.at[e], recv.at[slot], dev).start()

            @pl.when(t == 0)
            def _():
                go(relay.at[e], relay_recv, e, jnp.where(core == 0, x_base + 1, y_base))

            @pl.when(t == B1)
            def _():
                go(x_fin.at[u], x_recv, u, x_base + par)

            @pl.when(t == Y1)
            def _():
                go(y_fin.at[u], y_recv, u, y_base + par)
        own_units(n, core, body)
        t, i = task_of(n)
        for way, dev in enumerate((xn, xn, yn)):
            @pl.when((i == HALF - 1) & (t == way))
            def _():
                remote(vsum.at[t], vland.at[CHUNKS + way], v_send.at[CHUNKS + way], v_recv.at[CHUNKS + way], dev).start()

    def sib_units(n, act):
        def body(t, par, u, s, e):
            for first, dst in ((True, stage.at[s]), (False, sib_land.at[e])):
                @pl.when((n == 0) == first)
                def _():
                    act_on(remote(acc.at[n % 3, tile(s, UR)], dst, sib_send.at[e], sib_recv.at[e], sib), act)
        own_units(n, other(core), body)

    def task(n):
        t, i = task_of(n)
        need, row = bias_of(chip_of(t, chip), i)
        a = n % 3

        @pl.when(n >= 3)
        def _():
            sib_units(n - 3, 'sent')

        def chunk(slot):
            j = n * CHUNKS + slot

            @pl.when(j + CHUNKS - 1 < STEPS)
            def _():
                issue(j + CHUNKS - 1)
            local(xq.at[tile(0, KC), tile(0, BLOCK)], xbuf.at[slot], x_sem.at[slot]).wait()
            local(dyq.at[tile(0, KC), tile(0, D)], dybuf.at[slot], dy_sem.at[slot]).wait()

            def dot():
                return lax.dot_general(xbuf[slot], dybuf[slot], (((0,), (0,)), ((), ())),
                                       preferred_element_type=F32)

            @pl.when(slot == 0)
            def _():
                acc[a] = dot()

            @pl.when(slot > 0)
            def _():
                acc[a] += dot()

            @pl.when(need)
            def _():
                def add(r, total):
                    block = dybuf[slot, tile(r, LANES), :].astype(F32)
                    return total + jnp.sum(block.reshape(-1, SUB, D), axis=0)
                total = lax.fori_loop(0, KC // LANES, add, jnp.zeros_like(ss))
                vec[t, pl.ds(row, 1), :] += jnp.sum(total, axis=0, keepdims=True)

            @pl.when((slot == 0) & (n > 0))
            def _():
                prefetch(n - 1)

            @pl.when((slot == jnp.where(n == 1, 0, 1)) & (n > 0))
            def _():
                combine(n - 1)
                send_own(n - 1)
        each(0, CHUNKS, chunk)
        sib_units(n, 'start')

        @pl.when(i == HALF - 1)
        def _():
            remote(vec.at[t], vland.at[t], v_send.at[t], v_recv.at[t], sib).start()

    each(0, TASKS, task)
    prefetch(jnp.int32(TASKS - 1))
    combine(jnp.int32(TASKS - 1))
    each(TASKS - 3, TASKS, lambda n: sib_units(n, 'sent'))

    few = chip - 1 == core
    mid = jnp.logical_not(is_edge(chip))
    past = chip == 2

    def write_unit(u, slot):
        def go(dst):
            local(flat.at[slot], dst, fl_sem.at[slot]).start()

        @pl.when(chip == 0)
        def _():
            go(g_a.at[tile(u % 4, UR), tile(u // 4, SUB)])

        @pl.when(chip == 3)
        def _():
            go(g_c.at[tile(u, UR)])
        square = jnp.where((u >= FEW[1]) & (u < FEW[2]), u - FEW[1],
                           jnp.where((u >= FEW[4]) & (u < FEW[-1]), u - 3, -1))
        col = jnp.where(u < FEW[2], 0, jnp.where(u < FEW[4], u - 4, 3))

        @pl.when(mid & few & (square < 0))
        def _():
            go(g_b.at[tile(jnp.where(past, 0, 2), UR), tile(col, SUB)])

        @pl.when(mid & few & (square >= 0))
        def _():
            go(g_c.at[tile(jnp.where(past, 4, 0) + square, UR)])

        @pl.when(mid & jnp.logical_not(few))
        def _():
            go(g_b.at[tile(u % 3, UR), tile(u // 3, SUB)])

    def written(slot):
        local(flat.at[slot], g_c.at[tile(0, UR)], fl_sem.at[slot]).wait()

    def finish(u):
        slot = u % 2

        @pl.when(u >= 2)
        def _():
            written(slot)
        arrived(x_fin.at[u], x_recv.at[u])
        arrived(y_fin.at[u], y_recv.at[u])

        def add(r, total):
            rows = tile(r, 16)
            val = part[here * UNITS + u, rows, :] + x_fin[u, rows, :] + y_fin[u, rows, :]
            flat[slot, rows] = val.reshape(16, SUB, LANES)
            return total + val[0:8] * val[0:8] + val[8:16] * val[8:16]
        ss[...] += lax.fori_loop(0, UR // 16, add, jnp.zeros_like(ss))
        write_unit(u, slot)

    each(0, UNITS, finish)
    arrived(vland.at[5], v_recv.at[5])
    arrived(vland.at[6], v_recv.at[6])
    val = vsum[here] + vland[5] + vland[6]
    vflat[...] = val.reshape(8, SUB, LANES)
    total = ss[...] + jnp.where(core == 0, 1.0, 0.0).astype(F32) * (val * val)
    ss_small[...] = sum(total[:, LANES * c:LANES * (c + 1)] for c in range(8))
    tail = [local(vflat, v_out, misc_sem.at[0]), local(ss_small, ss_out, misc_sem.at[1])]
    for c in tail:
        c.start()
    written(0)
    written(1)
    for c in tail:
        c.wait()
    each(0, here * UNITS, lambda e: remote(part.at[e], x_fin.at[0], out_send.at[e], x_recv.at[0], xn).wait_send())
    for way in range(3):
        remote(vsum.at[way], vland.at[CHUNKS], v_send.at[CHUNKS + way], v_recv.at[CHUNKS], xn).wait_send()


def shape(*dims, dtype=F32):
    return jax.ShapeDtypeStruct(dims, dtype)


def vmem(*dims, dtype=F32):
    return pltpu.VMEM(dims, dtype)


def dmas(*counts):
    return [pltpu.SemaphoreType.DMA(c if isinstance(c, tuple) else (c,)) for c in counts]


def any_space(count):
    return [pl.BlockSpec(memory_space=pltpu.HBM)] * count


def params_of(collective_id, mib):
    return pltpu.CompilerParams(collective_id=collective_id, has_side_effects=True, vmem_limit_bytes=mib * MIB)


def reduce_call(acts, ln_rows):
    outs = [shape(512, 24, LANES), shape(384, 32, LANES), shape(1536, SUB, LANES), shape(8, SUB, LANES), shape(SUB, LANES),
            shape(CHUNKS * UNITS, UR, D), shape(UNITS, UR, D)]
    return pl.pallas_call(
        reduce_kernel,
        out_shape=outs,
        in_specs=any_space(len(acts) + 1),
        out_specs=any_space(len(outs)),
        scratch_shapes=[
            vmem(CHUNKS, KC, BLOCK, dtype=BF16), vmem(CHUNKS, KC, D, dtype=BF16), vmem(3, BLOCK, D),
            vmem(CHUNKS * UNITS, UR, D), vmem(UNITS, UR, D), vmem(UNITS, UR, D), vmem(CHUNKS, UR, D), vmem(CHUNKS, UR, D), vmem(2, UR, SUB, LANES),
            vmem(CHUNKS, 8, D), vmem(CHUNKS, 8, D), vmem(8, SUB, LANES), vmem(7, 8, D), vmem(CHUNKS, D), vmem(8, D), vmem(SUB, LANES),
            *dmas(CHUNKS, CHUNKS, CHUNKS * UNITS, CHUNKS * UNITS, X1 * UNITS, UNITS, UNITS, UNITS, 7, 7, CHUNKS, CHUNKS, 2, 2)],
        compiler_params=params_of(0, 63),
        name='grad_reduce',
    )(*acts, ln_rows)


BLK = 128
PART_BLOCKS = [7] * UNITS + [4, 4, 2, 2]
PARTS = len(PART_BLOCKS)
SEG = max(PART_BLOCKS) * BLK
ENDS = [BLK * sum(PART_BLOCKS[:j]) for j in range(PARTS + 1)]
CUTS = ENDS[:-1] + [SHARD_ROWS]
FULL = SHARE // BLK
LOADS = 4
LOAD = SHARE // LOADS
GB = FULL // LOADS


def update_kernel(w_in, m_in, v_in, ga, gb, gc, vg, ss_in,
                  wbuf, mbuf, vbuf, params, full,
                  gbuf, cin, ssl, sums, rates,
                  load_sem, g_sem, edge_send, edge_recv, ss_send, ss_recv, sum_send, sum_recv,
                  own_send, own_copy, x_recv, y_recv, d_recv, s_recv, fwd_send, sib_fwd, cin_sem):
    me, chip, core, sib, xn, yn = neighbours()

    def floor_of(dev):
        return DOWN * (SHARD_ROWS * dev // DOWN)

    def in_window(dev, row):
        return row - SHARD_ROWS * dev + EDGE

    def load_rows(k):
        return pl.ds(LOAD * k, LOAD if k < LOADS - 1 else SHARD_ROWS - LOAD * k)

    order = [*range(1, LOADS - 1), 0, LOADS - 1]
    loads = [[local(src.at[load_rows(k)], dst.at[load_rows(k)], load_sem.at[e, k])
              for e, (src, dst) in enumerate(((w_in, wbuf), (m_in, mbuf), (v_in, vbuf)))] for k in order]

    def when_in(lo, hi, do, *args):
        @pl.when((me >= lo) & (me <= hi))
        def _():
            do(*args)

    def g_loads(act):
        start = in_window(me, pick(me, NOMINAL))

        def go(*copies):
            for e, (src, lo, size, at) in enumerate(copies):
                act_on(local(src.at[pl.ds(lo, size)], gbuf.at[pl.ds(start + at, size)], g_sem.at[e]), act)
        two, one = SIZES[2], SHARE - SIZES[2]
        tail = (vg, 0, UP, SHARE)
        when_in(0, 0, go, (ga, 0, SHARE, 0))
        when_in(1, 1, go, (ga, 0, SHARE, 0), tail)
        when_in(2, 2, go, (gc, 0, two, 0), (vg, 0, UP, two), (gb, two, one, two + UP))
        when_in(3, 4, go, (gb, 0, SHARE, 0))
        when_in(5, 5, go, (gb, 0, one, 0), (vg, 0, SIZES[7], one), (gc, one, two, one + SIZES[7]))
        when_in(6, 6, go, (gc, 0, SHARE, 0))
        when_in(7, 7, go, (gc, 0, SHARE, 0), tail)

    ss_copy = local(ss_in, ssl.at[me], cin_sem.at[0])
    ss_copy.start()
    g_loads('start')
    for group in loads:
        for c in group:
            c.start()
    sums[...] = jnp.zeros_like(sums)
    others = [lax.rem(me + e, N_DEV) for e in range(1, N_DEV)]
    enter(others)
    ss_copy.wait()

    def share(buf, send, recv, act):
        for e, dev in enumerate(others):
            if act == 'get':
                remote(buf.at[dev], buf.at[dev], send.at[e], recv.at[dev], dev).wait_recv()
            else:
                act_on(remote(buf.at[me], buf.at[me], send.at[e], recv.at[me], dev), act)

    share(ssl, ss_send, ss_recv, 'start')

    def edges(act):
        def go(src, lo, size, dev, row, e):
            act_on(remote(src.at[pl.ds(lo, size)], gbuf.at[pl.ds(in_window(dev, row), size)],
                          edge_send.at[e], edge_recv.at[e], dev), act)

        def up(src):
            go(src, 0, UP, me - 1, pick(me, NOMINAL), 0)

        def down(src):
            go(src, SHARE - DOWN, DOWN, me + 1, pick(me + 1, NOMINAL) - DOWN, 1)
        when_in(1, 1, up, ga)
        when_in(2, 2, up, gc)
        when_in(3, 5, up, gb)
        when_in(6, 7, up, gc)
        when_in(0, 1, down, ga)
        when_in(2, 4, down, gb)
        when_in(5, 6, down, gc)

    edges('start')
    share(ssl, ss_send, ss_recv, 'get')
    grad_sq = jnp.sum(sum(ssl[e] for e in range(N_DEV)))
    grad_sq = grad_sq * (1.0 / (N_DEV * N_DEV))
    norm = jnp.sqrt(jnp.full((SUB, LANES), grad_sq, F32))
    scale = (1.0 / N_DEV) / jnp.maximum(1.0, norm)
    scale = jnp.concatenate([scale] * (BLK // 8), axis=0)
    g_loads('wait')
    first_t, past_t = pick(me, FIRST_TENSOR), pick(me, PAST_TENSOR)

    REST = SHARD_ROWS - FULL * BLK

    def over(first, past, whole, masked):
        top = min(past, FULL)

        def tensor(t):
            lo = pick(t, STARTS[:-1]) - SHARD_ROWS * me
            hi = pick(t, STARTS[1:]) - SHARD_ROWS * me

            @pl.when((hi > first * BLK) & (lo < past * BLK))
            def _():
                head, tail = lo // BLK, hi // BLK
                from_b = jnp.maximum((lo + BLK - 1) // BLK, first)
                whole(t, from_b, jnp.maximum(from_b, jnp.minimum(tail, top)))

                def shared(b, size, at, g_at):
                    ids = lax.broadcasted_iota(jnp.int32, (size, LANES), 0) + b * BLK
                    masked(t, at, g_at, (ids >= lo) & (ids < hi))

                def end(e):
                    b = jnp.where(e == 0, head, tail)
                    cuts = jnp.where(e == 0, lo, hi) % BLK > 0
                    again = (e > 0) & (head == tail) & (lo % BLK > 0)

                    @pl.when(cuts & (b >= first) & (b < top) & jnp.logical_not(again))
                    def _():
                        shared(b, BLK, *block_rows(b))
                each(0, 2, end)
                if past > FULL:
                    shared(FULL, REST, pl.ds(FULL * BLK, REST), pl.ds(FULL * BLK + EDGE, REST))
        each(first_t, past_t, tensor)

    def block_rows(b):
        return tile(b, BLK), pl.ds(pl.multiple_of(b * BLK + EDGE, DOWN), BLK)

    def step_of(t, at, g_at):
        decay = jnp.where((t % 2 == 0) & (t != 4) & (t < 9), DECAY, 0.0).astype(F32)
        g, w, m, v = gbuf[g_at, :], wbuf[at, :], mbuf[at, :], vbuf[at, :]
        h = g * scale[:g.shape[0]]
        new_m = BETA_ONE * m + (1.0 - BETA_ONE) * h
        new_v = BETA_TWO * v + (1.0 - BETA_TWO) * (h * h)
        root = new_v * lax.rsqrt(jnp.maximum(new_v, jnp.finfo(F32).tiny))
        u = new_m / (root * (CORR_ONE / CORR_TWO ** 0.5) + EPSILON * CORR_ONE) + decay * w
        return (g, w, m, v), (u, w, new_m, new_v)

    def note(t, u_sq, w_sq):
        sums[me, pl.ds(t, 1), :] += jnp.sum(u_sq, axis=0, keepdims=True)
        sums[me, pl.ds(DOWN + t, 1), :] += jnp.sum(w_sq, axis=0, keepdims=True)

    def direction(t, first, past):
        def block(b, carry):
            at, g_at = block_rows(b)
            _, (u, w, new_m, new_v) = step_of(t, at, g_at)
            mbuf[at, :], vbuf[at, :], gbuf[g_at, :] = new_m, new_v, u
            return tuple(total + jnp.sum((x * x).reshape(-1, SUB, LANES), axis=0) for total, x in zip(carry, (u, w)))
        zero = jnp.zeros((SUB, LANES), F32)
        note(t, *lax.fori_loop(first, past, block, (zero, zero)))

    def direction_shared(t, at, g_at, keep):
        (g, w, m, v), (u, _, new_m, new_v) = step_of(t, at, g_at)
        mbuf[at, :], vbuf[at, :] = jnp.where(keep, new_m, m), jnp.where(keep, new_v, v)
        gbuf[g_at, :] = jnp.where(keep, u, g)
        note(t, jnp.where(keep, u * u, 0.0), jnp.where(keep, w * w, 0.0))

    for k, group in zip(order, loads):
        if k == 0:
            for e, (has, size) in enumerate(((me < N_DEV - 1, UP), (me > 0, DOWN))):
                @pl.when(has)
                def _():
                    rows = gbuf.at[pl.ds(0, size)]
                    remote(rows, rows, edge_send.at[e], edge_recv.at[e], sib).wait_recv()
        for c in group:
            c.wait()
        over(GB * k, GB * (k + 1) + (k == LOADS - 1), direction, direction_shared)
    share(sums, sum_send, sum_recv, 'start')
    share(sums, sum_send, sum_recv, 'get')
    total = jnp.sum(sum(sums[e] for e in range(N_DEV)), axis=1, keepdims=True)
    u_n, w_n = jnp.sqrt(total[:DOWN]), jnp.sqrt(total[DOWN:])
    both = (u_n > 0) & (w_n > 0)
    ratio = jnp.where(both, w_n / jnp.where(u_n > 0, u_n, 1.0), 1.0)
    rates[...] = jnp.broadcast_to(LEARN_RATE * ratio, rates.shape)

    def apply(t, first, past):
        rate = jnp.broadcast_to(rates[pl.ds(t, 1), :], (BLK, LANES))

        def block(b):
            at, g_at = block_rows(b)
            wbuf[at, :] = wbuf[at, :] - rate * gbuf[g_at, :]
        each(first, past, block)

    def apply_shared(t, at, g_at, keep):
        w = wbuf[at, :]
        wbuf[at, :] = jnp.where(keep, w - jnp.broadcast_to(rates[pl.ds(t, 1), :], w.shape) * gbuf[g_at, :], w)

    def cut(dev, j):
        return pl.ds(SHARD_ROWS * dev + CUTS[j], CUTS[j + 1] - CUTS[j])

    def twin(dev):
        return dev + other(2 * core)

    dg = N_DEV - 2 * (chip + 1) + core

    def own_part(j, e, sem, dev):
        return remote(wbuf.at[cut(0, j)], full.at[cut(me, j)], own_send.at[e, j], sem, dev)

    for j in range(PARTS):
        over(ENDS[j] // BLK, ENDS[j + 1] // BLK + (j == PARTS - 1), apply, apply_shared)
        for e, (sem, dev) in enumerate(((x_recv.at[j], xn), (y_recv.at[j], yn), (s_recv.at[0, j], sib))):
            own_part(j, e, sem, dev).start()
        local(wbuf.at[cut(0, j)], full.at[cut(me, j)], own_copy.at[j]).start()

    def wait_from(dev, j, sem):
        rows = full.at[cut(dev, j)]
        remote(rows, rows, cin_sem.at[0], sem, sib).wait_recv()

    def forward(dev, j, send_sem, recv_sem, to):
        rows = full.at[cut(dev, j)]
        remote(rows, rows, send_sem, recv_sem, to).start()

    def convert(*parts):
        todo = []
        for slot, (dev, j) in enumerate(parts):
            skip = DOWN if j == 0 else 0
            lo, size = pl.multiple_of(floor_of(dev) + skip + ENDS[j], DOWN), ENDS[j + 1] - ENDS[j] - skip
            cp = local(full.at[pl.ds(lo, size)], cin.at[slot, pl.ds(0, size)], cin_sem.at[slot])
            cp.start()
            todo.append((cp, slot, lo, size))
        for cp, slot, lo, size in todo:
            cp.wait()

            def body(b):
                params[pl.ds(pl.multiple_of(lo + b * DOWN, DOWN), DOWN), :] = cin[slot, tile(b, DOWN), :].astype(BF16)
            lax.fori_loop(0, size // DOWN, lambda b, c: (body(b), c)[1], 0, unroll=8)

    for j in range(PARTS):
        local(wbuf.at[cut(0, j)], full.at[cut(me, j)], own_copy.at[j]).wait()
        wait_from(sib, j, s_recv.at[0, j])
        convert((me, j), (sib, j))
        wait_from(xn, j, x_recv.at[j])
        forward(xn, j, sib_fwd.at[0, j], s_recv.at[1, j], sib)
        if j % 2 == 0:
            forward(xn, j, fwd_send.at[j], d_recv.at[j], yn)
        wait_from(yn, j, y_recv.at[j])
        forward(yn, j, sib_fwd.at[1, j], s_recv.at[2, j], sib)
        if j % 2 == 1:
            forward(yn, j, fwd_send.at[j], d_recv.at[j], xn)
        convert((xn, j), (yn, j))
        wait_from(twin(xn), j, s_recv.at[1, j])
        wait_from(twin(yn), j, s_recv.at[2, j])
        convert((twin(xn), j), (twin(yn), j))
    def drain(sems, parts):
        for p in parts:
            remote(wbuf.at[cut(0, p)], full.at[cut(me, p)], sems.at[p], x_recv.at[p], xn).wait_send()

    for j in range(0, PARTS, 2):
        both_parts = (j, j + 1)
        if both_parts[-1] == PARTS - 1:
            edges('sent')
            share(ssl, ss_send, ss_recv, 'sent')
            share(sums, sum_send, sum_recv, 'sent')
            for sems in ([own_send.at[e] for e in range(3)] + [sib_fwd.at[e] for e in range(2)]):
                drain(sems, range(PARTS))
            for sems in (fwd_send, sib_fwd.at[2]):
                drain(sems, range(j))
        for e in both_parts:
            wait_from(dg, e, d_recv.at[e])
            forward(dg, e, sib_fwd.at[2, e], s_recv.at[3, e], sib)
        convert(*[(dg, e) for e in both_parts])
        for e in both_parts:
            wait_from(twin(dg), e, s_recv.at[3, e])
        if e == PARTS - 1:
            low = DOWN * (SHARD_ROWS * (N_DEV - 1) // DOWN) + SHARE
            pieces = ([(0, DOWN)] + [(DOWN * (SHARD_ROWS * s // DOWN) - DOWN, 2 * DOWN) for s in range(1, N_DEV)]
                      + [(low, TOTAL_ROWS - low)])
            ends = [local(full.at[pl.ds(lo, size)], cin.at[2, pl.ds(2 * DOWN * p, size)], cin_sem.at[2 + p])
                    for p, (lo, size) in enumerate(pieces)]
            for c in ends:
                c.start()
        convert(*[(twin(dg), e) for e in both_parts])
    for p, (c, (lo, size)) in enumerate(zip(ends, pieces)):
        c.wait()
        params[lo:lo + size, :] = cin[2, 2 * DOWN * p:2 * DOWN * p + size, :].astype(BF16)
    for sems in (fwd_send, sib_fwd.at[2]):
        drain(sems, both_parts)


def update_call(w, m, v, ga, gb, gc, vg, ss):
    shard = pltpu.VMEM((SHARD_ROWS, LANES), F32)
    outs = [shard, shard, shard, pltpu.VMEM((TOTAL_ROWS, LANES), BF16), shape(TOTAL_ROWS, LANES)]
    in_vmem = pl.BlockSpec(memory_space=pltpu.VMEM)
    return pl.pallas_call(
        update_kernel,
        out_shape=outs,
        in_specs=any_space(8),
        out_specs=[in_vmem] * 4 + any_space(1),
        scratch_shapes=[
            vmem(WIN, LANES), vmem(3, SEG, LANES),
            vmem(N_DEV, SUB, LANES), vmem(N_DEV, 2 * DOWN, LANES), vmem(DOWN, LANES),
            *dmas((3, LOADS), 3, 2, 2, 7, N_DEV, 7, N_DEV, (3, PARTS), PARTS, PARTS, PARTS, PARTS, (4, PARTS),
                  PARTS, (3, PARTS), 11)],
        compiler_params=params_of(1, 14),
        name='lamb_gather',
    )(w, m, v, ga, gb, gc, vg, ss)


def cuts_of(rows):
    size, last = rows // CHUNKS // DOWN * DOWN, CHUNKS - 1
    return [(size * e, size) for e in range(last)] + [(size * last, rows - size * last)]


def write_kernel(*refs):
    *pairs, sem = refs
    half = len(pairs) // 2
    copies = [local(src.at[pl.ds(lo, size)], dst.at[pl.ds(lo, size)], sem.at[p, e])
              for p, (src, dst) in enumerate(zip(pairs[:half], pairs[half:]))
              for e, (lo, size) in enumerate(cuts_of(src.shape[0]))]
    for c in copies:
        c.start()
    for c in copies:
        c.wait()


def write_call(arrays):
    return pl.pallas_call(
        write_kernel,
        out_shape=[jax.ShapeDtypeStruct(a.shape, a.dtype) for a in arrays],
        in_specs=[pl.BlockSpec(memory_space=pltpu.VMEM)] * len(arrays),
        out_specs=any_space(len(arrays)),
        scratch_shapes=dmas((len(arrays), CHUNKS)),
        compiler_params=pltpu.CompilerParams(vmem_limit_bytes=MIB),
        name='write_out',
    )(*arrays)


def solution(mesh):
    def local_step(weights, moment_one, moment_two, *rest):
        *acts, ln_grad = rest
        ga, gb, gc, vg, ss, *_ = reduce_call(acts, ln_grad[0])
        rows = [a.reshape(SHARD_ROWS, LANES) for a in (weights, moment_one, moment_two)]
        out = update_call(*rows, *(g.reshape(-1, LANES) for g in (ga, gb, gc, vg)), ss)
        return tuple(a.reshape(-1) for a in write_call(out[:-1]))

    row_spec = P('dp', None)
    flat_spec = P('dp')
    in_specs = (flat_spec,) * 3 + (row_spec,) * 8 + (P('dp', None, None),)
    return jax.shard_map(local_step, mesh=mesh, in_specs=in_specs, out_specs=(flat_spec,) * 3 + (P(),), check_vma=False)
```
